32 devices in a mesh: dp: 2 (over x), row: 4 (over z), col: 4 (over y, core).
Axes of the slice: x: 2, y: 2, z: 4, core: 2. Of those that a mesh axis runs over, the one named last changes fastest.
Arguments:
- inputs: bfloat16 [768, 8192], P('row', ('dp', 'col')), may hold values from -6 to 6
- w_query: bfloat16 [4, 4, 36864], P('row', 'col'), may hold values from -0.21875 to 0.21875
- w_key: bfloat16 [4, 4, 36864], P('row', 'col'), may hold values from -0.21875 to 0.21875
- w_value: bfloat16 [4, 4, 36864], P('row', 'col'), may hold values from -0.21875 to 0.21875
- w_out: bfloat16 [4, 4, 36864], P('col', 'row'), may hold values from -0.875 to 0.875
- w_up: bfloat16 [768, 3072], P('row', 'col'), may hold values from -0.21875 to 0.21875
- w_down: bfloat16 [768, 3072], P('row', 'col'), may hold values from -0.109375 to 0.109375
- ln1_gain: float32 [768], P('row'), may hold values from 0.5 to 1.5
- ln1_bias: float32 [768], P('row'), may hold values from -1.75 to 1.75
- ln2_gain: float32 [768], P('row'), may hold values from 0.5 to 1.5
- ln2_bias: float32 [768], P('row'), may hold values from -1.75 to 1.75
- segment_ids: int32 [8192], P('dp'), may hold values from 0 to 20, as said below
- pad_mask: int32 [8192], P('dp'), may hold values from 0 to 1, as said below
- rand_blocks: int32 [2, 12, 64, 3], P('dp', 'col'), may hold values from 1 to 62, as said below
- grad_out: bfloat16 [768, 8192], P('row', ('dp', 'col')), may hold values from -6 to 6
Outputs:
- output: bfloat16 [768, 8192], P('row', ('dp', 'col'))
- grad_inputs: float32 [768, 8192], P('row', ('dp', 'col'))
- grad_w_query: float32 [4, 4, 36864], P('row', 'col')
- grad_w_key: float32 [4, 4, 36864], P('row', 'col')
- grad_w_value: float32 [4, 4, 36864], P('row', 'col')
- grad_w_out: float32 [4, 4, 36864], P('col', 'row')
- grad_w_up: float32 [768, 3072], P('row', 'col')
- grad_w_down: float32 [768, 3072], P('row', 'col')
- grad_ln1_gain: float32 [768], P('row')
- grad_ln1_bias: float32 [768], P('row')
- grad_ln2_gain: float32 [768], P('row')
- grad_ln2_bias: float32 [768], P('row')
The draws below stay inside these ranges and needn't reach their ends.
Inputs may be any that keep to these rules, and one draw needn't show every extreme that they name: `segment_ids`: within each sequence of 4096 tokens the ids never fall, the last token's id is 4096 // 204, and every run of one id except the one that the sequence's end cuts spans 204 to 2048 tokens. `pad_mask`: in each sequence the last 1 to 204 tokens are 0 and all others 1. `rand_blocks`: for each sequence, head and query block i: three different block numbers, none of them 0, 63, i - 1, i or i + 1.
All inputs are finite; a program needn't handle non-finite values.
Results may differ from the reference program's by a relative error of at most 0.015.
Values may be sent and summed in bfloat16 or wider, within the bound.
A program may use at most 192 MiB of HBM per device.

```python
import jax
import jax.numpy as jnp
from jax import lax

D = 768
H = 12
HD = 64
FF = 3072
BLOCK = 64
LEN = 4096
NB = 64
SEQUENCES = 2
TOKENS = 8192
DOC_MIN = 204
DOC_MAX = 2048
N_ROW = 4
N_COL = 4


def doc_layout(key):
    doc_count = LEN // DOC_MIN + 1
    lengths = jax.random.randint(jax.random.fold_in(key, 11), (SEQUENCES, doc_count), DOC_MIN, DOC_MAX + 1)
    doc_ends = jnp.cumsum(lengths, axis=1)
    position = jnp.arange(LEN, dtype=jnp.int32)
    segments = jnp.sum((position[None, :, None] >= doc_ends[:, None, :]).astype(jnp.int32), axis=2)
    segments = segments - segments[:, LEN - 1:LEN] + LEN // DOC_MIN
    pad_len = jax.random.randint(jax.random.fold_in(key, 12), (SEQUENCES, 1), 1, DOC_MIN + 1)
    real_tok = (position[None, :] < LEN - pad_len).astype(jnp.int32)
    return (segments.reshape(-1).astype(jnp.int32), real_tok.reshape(-1))


def draw_segment_ids(key, part):
    return doc_layout(key)[0]


def draw_pad_mask(key, part):
    return doc_layout(key)[1]


def draw_rand_blocks(key, part):
    noise = jax.random.randint(jax.random.fold_in(key, 21), (SEQUENCES, H, NB, NB), 0, 1 << 20)
    block_ids = jnp.arange(NB, dtype=jnp.int32)
    query_blk = block_ids[:, None]
    banned = (block_ids[None, :] == 0) | (block_ids[None, :] == NB - 1) | (jnp.abs(block_ids[None, :] - query_blk) <= 1)
    scores = jnp.where(banned[None, None], -1, noise * NB + block_ids)
    top_vals, picked = lax.top_k(scores, 3)
    return picked.astype(jnp.int32)


def shard_levels(rng, extent, shards, least, top_value):
    def one(axis_at, parts):
        heights = jax.random.uniform(jax.random.fold_in(jax.random.fold_in(rng, 6), axis_at), (parts,), jnp.float32, least / len(shards), top_value / len(shards))
        return jnp.repeat(jnp.exp(heights), extent[axis_at] // parts).reshape((-1,) + (1,) * (len(extent) - axis_at - 1))

    factor_of = one(*shards[0])
    for cut in shards[1:]:
        factor_of = factor_of * one(*cut)
    return factor_of


def centred(key, shape, width, reach, split=(), kind=jnp.bfloat16):
    factor_of = shard_levels(key, shape, split, -0.22, 0.18) if split else 1.0
    result = jax.random.normal(key, shape, jnp.float32) * width * factor_of
    return jnp.minimum(jnp.maximum(result, -reach), reach).astype(kind)


def setup_inputs(seed: int = 0) -> dict:
    splits = jax.random.split(jax.random.key(seed), 16)
    return {
        "inputs": centred(splits[0], (D, TOKENS), 1.0, 6.0, ((0, 4), (1, 8))),
        "w_query": centred(splits[1], (N_ROW, N_COL, D * D // (N_ROW * N_COL)), D ** -0.5, 0.21875, ((0, 4), (1, 4))),
        "w_key": centred(splits[2], (N_ROW, N_COL, D * D // (N_ROW * N_COL)), D ** -0.5, 0.21875, ((0, 4), (1, 4))),
        "w_value": centred(splits[3], (N_ROW, N_COL, D * D // (N_ROW * N_COL)), D ** -0.5, 0.21875, ((0, 4), (1, 4))),
        "w_out": centred(splits[4], (N_COL, N_ROW, D * D // (N_ROW * N_COL)), (D // 16) ** -0.5, 0.875, ((0, 4), (1, 4))),
        "w_up": centred(splits[5], (D, FF), D ** -0.5, 0.21875, ((0, 4), (1, 4))),
        "w_down": centred(splits[6], (D, FF), FF ** -0.5, 0.109375, ((0, 4), (1, 4))),
        "ln1_gain": jnp.clip(1.0 + 0.1 * jax.random.normal(splits[7], (D,), jnp.float32), 0.5, 1.5),
        "ln1_bias": centred(splits[8], (D,), 0.3, 1.75, ((0, 4),), jnp.float32),
        "ln2_gain": jnp.clip(1.0 + 0.1 * jax.random.normal(splits[9], (D,), jnp.float32), 0.5, 1.5),
        "ln2_bias": centred(splits[10], (D,), 0.3, 1.75, ((0, 4),), jnp.float32),
        "segment_ids": draw_segment_ids(jax.random.fold_in(splits[15], 71), 0),
        "pad_mask": draw_pad_mask(jax.random.fold_in(splits[15], 71), 0),
        "rand_blocks": draw_rand_blocks(jax.random.fold_in(splits[15], 71), 0),
        "grad_out": centred(splits[14], (D, TOKENS), 1.0, 6.0, ((0, 4), (1, 8))),
    }


@jax.custom_vjp
def low(v):
    return lax.optimization_barrier(v.astype(jnp.bfloat16)).astype(jnp.float32)

@jax.custom_vjp
def low_back(v):
    return v

def low_keep(v):
    return (low(v), None)

def low_pass(kept, grad):
    return (grad,)

def back_keep(v):
    return (v, None)

def back_low(kept, grad):
    return (low(grad),)
low.defvjp(low_keep, low_pass)
low_back.defvjp(back_keep, back_low)
NEG = -1000000000.0
EPS = 1e-06

def low_both(value):
    return low_back(low(value))

def matmul(left, right):
    return jnp.dot(left, right, precision=lax.Precision.HIGHEST, preferred_element_type=jnp.float32)

def unblock(blocks, first_parts, second_parts):
    return blocks.reshape(first_parts, second_parts, D // first_parts, D // second_parts).transpose(0, 2, 1, 3).reshape(D, D)

def layer_norm(resid, gain, bias):
    mean_row = lax.optimization_barrier(jnp.mean(resid, axis=1, keepdims=True))
    var_row = lax.optimization_barrier(jnp.mean(resid * resid, axis=1, keepdims=True)) - mean_row * mean_row
    return (resid - mean_row) * lax.rsqrt(var_row + EPS) * gain + bias

def head_attention(packed):
    query, keys, values, rand_rows, seg_row, pad_row = packed
    block_ids = jnp.arange(NB)
    query_blk = block_ids[:, None]
    key_blk = block_ids[None, :]
    chosen = jnp.any(rand_rows[:, :, None] == block_ids[None, None, :], axis=1)
    block_ok = (jnp.abs(query_blk - key_blk) <= 1) | (key_blk == 0) | (key_blk == NB - 1)
    block_ok = block_ok | (query_blk == 0) | (query_blk == NB - 1) | chosen
    token_ok = jnp.repeat(jnp.repeat(block_ok, BLOCK, axis=0), BLOCK, axis=1)
    position = jnp.arange(LEN)
    same_doc = (seg_row[:, None] == seg_row[None, :]) & (pad_row[None, :] == 1)
    allowed = token_ok & (same_doc | (position[:, None] == position[None, :]))
    scores = low_back(jnp.einsum('qd,kd->qk', query, keys, precision=lax.Precision.HIGHEST) * HD ** (-0.5))
    scores = jnp.where(allowed, scores, NEG)
    row_top = lax.optimization_barrier(jnp.max(scores, axis=1, keepdims=True))
    log_total = row_top + jnp.log(lax.optimization_barrier(jnp.sum(jnp.exp(scores - row_top), axis=1, keepdims=True)))
    softmax_w = jnp.exp(scores - log_total)
    return matmul(low(softmax_w), values)

def split_heads(value):
    return value.reshape(SEQUENCES, LEN, H, HD).transpose(0, 2, 1, 3).reshape(SEQUENCES * H, LEN, HD)

def attention(query, keys, values, rand_blocks, segment_ids, pad_mask):
    rand_flat = rand_blocks.reshape(SEQUENCES * H, NB, 3)
    seg_flat = jnp.repeat(segment_ids.reshape(SEQUENCES, LEN), H, axis=0)
    pad_flat = jnp.repeat(pad_mask.reshape(SEQUENCES, LEN), H, axis=0)
    heads_out = lax.map(jax.checkpoint(head_attention), (split_heads(query), split_heads(keys), split_heads(values), rand_flat, seg_flat, pad_flat))
    return heads_out.reshape(SEQUENCES, H, LEN, HD).transpose(0, 2, 1, 3).reshape(TOKENS, D)

def reference(inputs, w_query, w_key, w_value, w_out, w_up, w_down, ln1_gain, ln1_bias, ln2_gain, ln2_bias, segment_ids, pad_mask, rand_blocks, grad_out):

    def forward(x_cols, query_b, key_b, value_b, out_b, up_w, down_t, gain_one, bias_one, gain_two, bias_two):
        x_in = x_cols.T
        query_w = unblock(query_b, N_ROW, N_COL)
        key_w = unblock(key_b, N_ROW, N_COL)
        value_w = unblock(value_b, N_ROW, N_COL)
        out_w = unblock(out_b, N_COL, N_ROW)
        query = low_both(matmul(x_in, query_w))
        keys = low_both(matmul(x_in, key_w))
        values = low_both(matmul(x_in, value_w))
        heads_out = low_both(attention(query, keys, values, rand_blocks, segment_ids, pad_mask))
        attn = low_back(matmul(heads_out, out_w))
        hidden = layer_norm(x_in + attn, gain_one, bias_one)
        up_val = low_back(matmul(low(hidden), up_w))
        act = low(jax.nn.gelu(up_val, approximate=True))
        down_val = low_back(matmul(act, down_t.T))
        return layer_norm(hidden + down_val, gain_two, bias_two).T
    output, pullback = jax.vjp(forward, inputs.astype(jnp.float32), w_query.astype(jnp.float32), w_key.astype(jnp.float32), w_value.astype(jnp.float32), w_out.astype(jnp.float32), w_up.astype(jnp.float32), w_down.astype(jnp.float32), ln1_gain.astype(jnp.float32), ln1_bias.astype(jnp.float32), ln2_gain.astype(jnp.float32), ln2_bias.astype(jnp.float32))
    grads = pullback(grad_out.astype(jnp.float32))
    return (output.astype(jnp.bfloat16), grads[0], grads[1], grads[2], grads[3], grads[4], grads[5], grads[6], grads[7], grads[8], grads[9], grads[10])
```

```python
import functools

import jax
import jax.numpy as jnp
from jax import lax
from jax.experimental import pallas as pl
from jax.experimental.pallas import tpu as pltpu
from jax.sharding import PartitionSpec as P

BLOCK = 64
HW = 64
LANES = 128
NEG = -1000000000.0
EPS = 1e-06
BF = jnp.bfloat16
F32 = jnp.float32


def mm(left, right):
    return lax.dot_general(left, right, (((1,), (0,)), ((), ())), preferred_element_type=F32)


def mm_nt(left, right):
    return lax.dot_general(left, right, (((1,), (1,)), ((), ())), preferred_element_type=F32)


def mm_tn(left, right):
    return lax.dot_general(left, right, (((0,), (0,)), ((), ())), preferred_element_type=F32)


def block_of(j, row, per, rows):
    return (j // per) * (per * rows) + row * per + j % per


def rows_at(ref, block, head):
    start = pl.multiple_of(block * BLOCK, BLOCK)
    return ref[pl.ds(start, BLOCK), head * LANES : (head + 1) * LANES]


def sparse_lists(rand_ref, head, pos, nb):
    picks = [rand_ref[(head * nb + pos) * 3 + i] for i in range(3)]
    before = jnp.maximum(pos - 1, 0)
    after = jnp.minimum(pos + 1, nb - 1)
    blocks = [0, nb - 1, before, pos, after] + picks
    masks = [
        0,
        nb - 1,
        jnp.where(pos >= 2, before, 2 * nb),
        nb + pos,
        jnp.where(pos <= nb - 3, after, 2 * nb),
    ] + picks
    return blocks, masks


def dense_lists(group, pos, nb):
    blocks = [group * 8 + i for i in range(8)]
    masks = [jnp.where(b == pos, nb + b, b) for b in blocks]
    return blocks, masks


def gather(ref, blocks, head):
    return jnp.concatenate([rows_at(ref, b, head) for b in blocks], axis=0)


def scores_of(query, query_mask, keys, key_mask):
    return jnp.where(mm_nt(query_mask, key_mask) > 0.5, mm_nt(query, keys), NEG)


def forward_kernel(heads, nb, per, rows, row_ref, rand_ref, q_ref, qm_ref, kv_ref, km_ref, o_ref, lse_ref):
    row = row_ref[0]

    def place(j, head):
        start = pl.multiple_of(j * BLOCK, BLOCK)
        return pl.ds(start, BLOCK), slice(head * LANES, (head + 1) * LANES)

    def step(j, carry):
        pos = block_of(j, row, per, rows)
        is_global = (pos == 0) | (pos == nb - 1)
        query_mask = qm_ref[pl.ds(pl.multiple_of(j * BLOCK, BLOCK), BLOCK), :]

        @pl.when(jnp.logical_not(is_global))
        def _():
            for head in range(heads):
                at = place(j, head)
                blocks, masks = sparse_lists(rand_ref, head, pos, nb)
                keys = gather(kv_ref, blocks, head)
                score = scores_of(q_ref[at], query_mask, keys, gather(km_ref, masks, 0))
                top = jnp.max(score, axis=1, keepdims=True)
                weight = jnp.exp(score - top)
                total = jnp.sum(weight, axis=1, keepdims=True)
                probs = (weight * (1.0 / total)).astype(BF)
                o_ref[at] = mm(probs, keys).astype(BF)
                lse_ref[at] = jnp.broadcast_to(top + jnp.log(total), (BLOCK, LANES))

        @pl.when(is_global)
        def _():
            def score_at(group, head):
                blocks, masks = dense_lists(group, pos, nb)
                keys = gather(kv_ref, blocks, head)
                score = scores_of(
                    q_ref[place(j, head)], query_mask, keys, gather(km_ref, masks, 0)
                )
                return score, keys

            def stats(group, kept):
                new = []
                for head in range(heads):
                    top, total = kept[head]
                    score, _ = score_at(group, head)
                    above = jnp.maximum(top, jnp.max(score, axis=1, keepdims=True))
                    total = total * jnp.exp(top - above) + jnp.sum(
                        jnp.exp(score - above), axis=1, keepdims=True
                    )
                    new.append((above, total))
                return tuple(new)

            first = tuple(
                (jnp.full((BLOCK, 1), 2 * NEG, F32), jnp.zeros((BLOCK, 1), F32))
                for _ in range(heads)
            )
            found = lax.fori_loop(0, nb // 8, stats, first)
            lses = [top + jnp.log(total) for top, total in found]

            def outs(group, kept):
                new = []
                for head in range(heads):
                    score, keys = score_at(group, head)
                    new.append(kept[head] + mm(jnp.exp(score - lses[head]).astype(BF), keys))
                return tuple(new)

            done = lax.fori_loop(
                0, nb // 8, outs, tuple(jnp.zeros((BLOCK, LANES), F32) for _ in range(heads))
            )
            for head in range(heads):
                at = place(j, head)
                o_ref[at] = done[head].astype(BF)
                lse_ref[at] = jnp.broadcast_to(lses[head], (BLOCK, LANES))

        return carry

    lax.fori_loop(0, q_ref.shape[0] // BLOCK, step, 0)


def backward_kernel(
    heads, nb, per, rows, row_ref, rand_ref, q_ref, qm_ref, kv_ref, km_ref, do_ref, lse_ref,
    dq_ref, dkv_ref, acc_ref,
):
    row = row_ref[0]
    acc_ref[...] = jnp.zeros_like(acc_ref)

    def place(j, head):
        start = pl.multiple_of(j * BLOCK, BLOCK)
        return pl.ds(start, BLOCK), slice(head * LANES, (head + 1) * LANES)

    def parts(j, head, query_mask, blocks, masks):
        at = place(j, head)
        keys = gather(kv_ref, blocks, head)
        score = scores_of(q_ref[at], query_mask, keys, gather(km_ref, masks, 0))
        lse = lse_ref[at][:, :1]
        probs = jnp.exp(score - lse)
        return keys, probs, mm_nt(do_ref[at], keys)

    def finish(j, head, blocks, keys, probs, grad_probs, dot_row):
        at = place(j, head)
        low = (probs * (grad_probs - dot_row)).astype(BF)
        both = jnp.concatenate([low, probs.astype(BF)], axis=0)
        sides = jnp.concatenate([q_ref[at], do_ref[at]], axis=0)
        grad = mm_tn(both, sides)
        for i, block in enumerate(blocks):
            start = pl.multiple_of(block * BLOCK, BLOCK)
            acc_ref[pl.ds(start, BLOCK), at[1]] += grad[i * BLOCK : (i + 1) * BLOCK, :]
        return mm(low, keys)

    def step(j, carry):
        pos = block_of(j, row, per, rows)
        is_global = (pos == 0) | (pos == nb - 1)
        query_mask = qm_ref[pl.ds(pl.multiple_of(j * BLOCK, BLOCK), BLOCK), :]

        @pl.when(jnp.logical_not(is_global))
        def _():
            for head in range(heads):
                blocks, masks = sparse_lists(rand_ref, head, pos, nb)
                keys, probs, grad_probs = parts(j, head, query_mask, blocks, masks)
                dot_row = jnp.sum(probs * grad_probs, axis=1, keepdims=True)
                grad_q = finish(j, head, blocks, keys, probs, grad_probs, dot_row)
                dq_ref[place(j, head)] = (grad_q * 0.125).astype(BF)

        @pl.when(is_global)
        def _():
            def dots(group, kept):
                blocks, masks = dense_lists(group, pos, nb)
                new = []
                for head in range(heads):
                    _, probs, grad_probs = parts(j, head, query_mask, blocks, masks)
                    new.append(kept[head] + jnp.sum(probs * grad_probs, axis=1, keepdims=True))
                return tuple(new)

            dot_rows = lax.fori_loop(
                0, nb // 8, dots, tuple(jnp.zeros((BLOCK, 1), F32) for _ in range(heads))
            )

            def grads(group, kept):
                blocks, masks = dense_lists(group, pos, nb)
                new = []
                for head in range(heads):
                    keys, probs, grad_probs = parts(j, head, query_mask, blocks, masks)
                    new.append(
                        kept[head]
                        + finish(j, head, blocks, keys, probs, grad_probs, dot_rows[head])
                    )
                return tuple(new)

            done = lax.fori_loop(
                0, nb // 8, grads, tuple(jnp.zeros((BLOCK, LANES), F32) for _ in range(heads))
            )
            for head in range(heads):
                dq_ref[place(j, head)] = (done[head] * 0.125).astype(BF)

        return carry

    lax.fori_loop(0, q_ref.shape[0] // BLOCK, step, 0)
    span = per * BLOCK

    def out(i, carry):
        source = (i % rows) * (rows * span) + (i // rows) * span
        dkv_ref[pl.ds(pl.multiple_of(i * span, span), span), :] = acc_ref[
            pl.ds(pl.multiple_of(source, span), span), :
        ].astype(BF)
        return carry

    lax.fori_loop(0, kv_ref.shape[0] // span, out, 0)


def specs(count):
    return [pl.BlockSpec(memory_space=pltpu.SMEM)] * 2 + [
        pl.BlockSpec(memory_space=pltpu.VMEM)
    ] * count


def attention_forward(dims, row, rand, q, q_mask, kv, k_mask):
    own, wide = q.shape
    vmem = pl.BlockSpec(memory_space=pltpu.VMEM)
    return pl.pallas_call(
        functools.partial(forward_kernel, *dims),
        name="attn_fwd",
        out_shape=(
            jax.ShapeDtypeStruct((own, wide), BF),
            jax.ShapeDtypeStruct((own, wide), F32),
        ),
        in_specs=specs(4),
        out_specs=(vmem, vmem),
        cost_estimate=pl.CostEstimate(
            flops=own * 512 * wide * 6, bytes_accessed=12 << 20, transcendentals=own * 512 * 3
        ),
        compiler_params=pltpu.CompilerParams(vmem_limit_bytes=48 << 20),
    )(row, rand, q, q_mask, kv, k_mask)


def attention_backward(dims, row, rand, q, q_mask, kv, k_mask, d_o, lse):
    own, wide = q.shape
    vmem = pl.BlockSpec(memory_space=pltpu.VMEM)
    return pl.pallas_call(
        functools.partial(backward_kernel, *dims),
        name="attn_bwd",
        out_shape=(
            jax.ShapeDtypeStruct((own, wide), BF),
            jax.ShapeDtypeStruct(kv.shape, BF),
        ),
        in_specs=specs(6),
        out_specs=(vmem, vmem),
        scratch_shapes=[pltpu.VMEM(kv.shape, F32)],
        cost_estimate=pl.CostEstimate(
            flops=own * 512 * wide * 12, bytes_accessed=20 << 20, transcendentals=own * 512 * 3
        ),
        compiler_params=pltpu.CompilerParams(vmem_limit_bytes=48 << 20),
    )(row, rand, q, q_mask, kv, k_mask, d_o, lse)


def norm(resid, gain, bias):
    mean = jnp.mean(resid, axis=1, keepdims=True)
    var = jnp.mean(resid * resid, axis=1, keepdims=True) - mean * mean
    rstd = lax.rsqrt(var + EPS)
    normed = (resid - mean) * rstd
    return normed * gain + bias, normed, rstd


def norm_grad(grad, normed, rstd, gain):
    scaled = grad * gain
    first = jnp.mean(scaled, axis=1, keepdims=True)
    second = jnp.mean(scaled * normed, axis=1, keepdims=True)
    return rstd * (scaled - first - normed * second)


def gelu(value):
    return jax.nn.gelu(value, approximate=True)


def on_device(
    inputs, w_query, w_key, w_value, w_out, w_up, w_down,
    ln1_gain, ln1_bias, ln2_gain, ln2_bias, segment_ids, pad_mask, rand_blocks, grad_out,
):
    rows, cols = lax.axis_size("row"), lax.axis_size("col")
    row, col = lax.axis_index("row"), lax.axis_index("col")
    feat, local = inputs.shape
    model = feat * rows
    hid = model // cols
    heads = hid // HW
    length = local * cols
    nb = length // BLOCK
    span = local // rows
    per = span // BLOCK
    dims = (heads, nb, per, rows)
    own = cols * span

    blk_q = w_query.reshape(feat, hid)
    blk_k = w_key.reshape(feat, hid)
    blk_v = w_value.reshape(feat, hid)
    blk_o = w_out.reshape(hid, feat)
    w_qkv = jnp.concatenate([blk_q, blk_k, blk_v], axis=1)
    w_own = lax.all_gather(w_qkv, "row", axis=0, tiled=True)
    x_parts = lax.all_gather(inputs, ("row", "col"), axis=0).reshape(rows, cols, feat, local)
    gains = lax.all_gather(
        jnp.stack([ln1_gain, ln1_bias, ln2_gain, ln2_bias]), "row", axis=0
    ).transpose(1, 0, 2).reshape(4, 1, model)
    grad_rows = lax.all_to_all(grad_out, "row", 1, 0, tiled=True).T.astype(F32)

    w_heads = w_own.reshape(model, 3, heads, HW)
    w_kv = jnp.concatenate([w_heads[:, 1], w_heads[:, 2]], axis=2).reshape(model, heads * LANES)
    w_q = jnp.pad(w_heads[:, 0], ((0, 0), (0, 0), (0, HW))).reshape(model, heads * LANES)
    x_all = x_parts.transpose(0, 2, 1, 3).reshape(model, length)
    x_own = lax.dynamic_index_in_dim(
        x_parts.reshape(rows, cols, feat, rows, span), row, axis=3, keepdims=False
    )
    x_res = lax.dynamic_index_in_dim(x_own, col, axis=1, keepdims=False)
    x_res = x_res.reshape(model, span).T.astype(F32)
    x_own = x_own.transpose(0, 2, 1, 3).reshape(model, own)
    kv = mm_tn(x_all, w_kv).astype(BF)
    q = (mm_tn(x_own, w_q).astype(BF) * 0.125).astype(BF)

    kinds = jnp.arange(BLOCK, dtype=jnp.int32)
    seg_hot = segment_ids[:, None] == kinds[None, :]
    key_hot = (seg_hot & (pad_mask[:, None] == 1)).astype(BF)
    place_hot = ((jnp.arange(length, dtype=jnp.int32) % BLOCK)[:, None] == kinds[None, :]).astype(BF)
    zeros = jnp.zeros_like(key_hot)
    k_mask = jnp.concatenate(
        [
            jnp.concatenate([key_hot, zeros], axis=1),
            jnp.concatenate([key_hot, place_hot], axis=1),
            jnp.zeros((BLOCK, LANES), BF),
        ],
        axis=0,
    )
    q_mask = jnp.concatenate([seg_hot.astype(BF), place_hot], axis=1)
    q_mask = lax.dynamic_index_in_dim(
        q_mask.reshape(cols, rows, span, LANES), row, axis=1, keepdims=False
    ).reshape(own, LANES)
    rand = rand_blocks.reshape(-1)
    row_arr = jnp.reshape(row, (1,)).astype(jnp.int32)

    o_wide, lse = attention_forward(dims, row_arr, rand, q, q_mask, kv, k_mask)
    o_own = o_wide.reshape(own, heads, 2, HW)[:, :, 1].reshape(own, hid)
    o = lax.all_to_all(o_own, "col", 0, 1, tiled=True)

    small = lax.all_gather(jnp.concatenate([w_qkv, blk_o.T], axis=1), ("row", "col"), axis=0)
    small = small.reshape(rows, cols, feat, 3 * hid + hid)
    w_o = small[..., 3 * hid :].transpose(0, 2, 1, 3).reshape(model, model)
    w_back = small[..., : 3 * hid].transpose(0, 2, 1, 3).reshape(model, 3 * model)
    up = lax.all_gather(w_up, ("row", "col"), axis=0).reshape(rows, cols, feat, -1)
    up = up.transpose(0, 2, 1, 3).reshape(model, -1)
    down = lax.all_gather(w_down, ("row", "col"), axis=0).reshape(rows, cols, feat, -1)
    down = down.transpose(0, 2, 1, 3).reshape(model, -1)

    gain1, bias1, gain2, bias2 = gains[0], gains[1], gains[2], gains[3]
    hidden, normed1, rstd1 = norm(x_res + mm_nt(o, w_o), gain1, bias1)
    hidden_low = hidden.astype(BF)
    up_val = mm(hidden_low, up)
    act, gelu_back = jax.vjp(gelu, up_val)
    act = act.astype(BF)
    result, normed2, rstd2 = norm(hidden + mm_nt(act, down), gain2, bias2)
    output = lax.all_to_all(result.T.astype(BF), "row", 0, 1, tiled=True)

    g_gain2 = jnp.sum(grad_rows * normed2, axis=0)
    g_bias2 = jnp.sum(grad_rows, axis=0)
    grad2 = norm_grad(grad_rows, normed2, rstd2, gain2)
    df = grad2.astype(BF)
    g_down = mm_tn(df, act).astype(BF)
    du = gelu_back(mm(df, down))[0].astype(BF)
    g_up = mm_tn(hidden_low, du).astype(BF)
    dh = mm_nt(du, up) + grad2
    g_gain1 = jnp.sum(dh * normed1, axis=0)
    g_bias1 = jnp.sum(dh, axis=0)
    grad1 = norm_grad(dh, normed1, rstd1, gain1)
    dattn = grad1.astype(BF)
    g_out = mm_tn(dattn, o).astype(BF)
    d_o = mm(dattn, w_o).astype(BF)
    d_o = lax.all_to_all(d_o, "col", 1, 0, tiled=True)
    d_o = jnp.pad(d_o.reshape(own, heads, HW), ((0, 0), (0, 0), (HW, 0))).reshape(own, -1)

    dq, dkv = attention_backward(dims, row_arr, rand, q, q_mask, kv, k_mask, d_o, lse)
    dkv = lax.psum_scatter(dkv, "row", scatter_dimension=0, tiled=True)

    def grid(grad):
        return grad.reshape(rows, feat, cols, -1).transpose(0, 2, 1, 3).reshape(rows * cols, feat, -1)

    g_ffn = jnp.concatenate([grid(g_up), grid(g_down), grid(g_out)], axis=2)
    g_ffn = lax.psum_scatter(g_ffn, ("row", "col"), scatter_dimension=0, tiled=True)
    g_ffn = lax.psum(g_ffn.reshape(feat, -1), "dp").astype(F32)

    dq = dq.reshape(own, heads, 2, HW)[:, :, 0].reshape(own, hid)
    dkv = dkv.reshape(own, heads, 2, HW)
    dqkv = jnp.concatenate(
        [dq, dkv[:, :, 0].reshape(own, hid), dkv[:, :, 1].reshape(own, hid)], axis=1
    )
    g_qkv = mm(x_own, dqkv).astype(BF)
    g_qkv = lax.psum_scatter(g_qkv, "row", scatter_dimension=0, tiled=True)
    g_qkv = lax.psum(g_qkv, "dp").astype(F32)
    dqkv = lax.all_to_all(dqkv, "col", 0, 1, tiled=True)
    grad_in = mm_nt(dqkv, w_back) + grad1
    grad_in = lax.all_to_all(grad_in.T, "row", 0, 1, tiled=True)

    sums = lax.psum(jnp.stack([g_gain1, g_bias1, g_gain2, g_bias2]), ("dp", "row", "col"))
    sums = lax.dynamic_slice_in_dim(sums, row * feat, feat, axis=1)
    ff = w_up.shape[1]
    return (
        output,
        grad_in,
        g_qkv[:, :hid].reshape(1, 1, -1),
        g_qkv[:, hid : 2 * hid].reshape(1, 1, -1),
        g_qkv[:, 2 * hid :].reshape(1, 1, -1),
        g_ffn[:, 2 * ff :].T.reshape(1, 1, -1),
        g_ffn[:, :ff],
        g_ffn[:, ff : 2 * ff],
        sums[0],
        sums[1],
        sums[2],
        sums[3],
    )


def solution(mesh):
    tokens = P("row", ("dp", "col"))
    grid = P("row", "col", None)
    return jax.shard_map(
        on_device,
        mesh=mesh,
        in_specs=(
            tokens,
            grid,
            grid,
            grid,
            P("col", "row", None),
            P("row", "col"),
            P("row", "col"),
            P("row"),
            P("row"),
            P("row"),
            P("row"),
            P("dp"),
            P("dp"),
            P("dp", "col", None, None),
            tokens,
        ),
        out_specs=(
            tokens,
            tokens,
            grid,
            grid,
            grid,
            P("col", "row", None),
            P("row", "col"),
            P("row", "col"),
            P("row"),
            P("row"),
            P("row"),
            P("row"),
        ),
        check_vma=False,
    )
```

```python
import functools

import jax
import jax.numpy as jnp
from jax import lax
from jax.experimental import pallas as pl
from jax.experimental.pallas import tpu as pltpu
from jax.sharding import PartitionSpec as P

BLOCK = 64
HW = 64
LANES = 128
NEG = -1000000000.0
EPS = 1e-06
BF = jnp.bfloat16
F32 = jnp.float32


def mm(left, right):
    return lax.dot_general(left, right, (((1,), (0,)), ((), ())), preferred_element_type=F32)


def mm_nt(left, right):
    return lax.dot_general(left, right, (((1,), (1,)), ((), ())), preferred_element_type=F32)


def mm_tn(left, right):
    return lax.dot_general(left, right, (((0,), (0,)), ((), ())), preferred_element_type=F32)


def block_of(j, row, per, rows):
    return (j // per) * (per * rows) + row * per + j % per


def rows_at(ref, block, head):
    start = pl.multiple_of(block * BLOCK, BLOCK)
    return ref[pl.ds(start, BLOCK), head * LANES : (head + 1) * LANES]


def sparse_lists(rand_ref, head, pos, nb):
    picks = [rand_ref[(head * nb + pos) * 3 + i] for i in range(3)]
    before = jnp.maximum(pos - 1, 0)
    after = jnp.minimum(pos + 1, nb - 1)
    blocks = [0, nb - 1, before, pos, after] + picks
    masks = [
        0,
        nb - 1,
        jnp.where(pos >= 2, before, 2 * nb),
        nb + pos,
        jnp.where(pos <= nb - 3, after, 2 * nb),
    ] + picks
    return blocks, masks


def dense_lists(group, pos, nb):
    blocks = [group * 8 + i for i in range(8)]
    masks = [jnp.where(b == pos, nb + b, b) for b in blocks]
    return blocks, masks


def gather(ref, blocks, head):
    return jnp.concatenate([rows_at(ref, b, head) for b in blocks], axis=0)


def scores_of(query, query_mask, keys, key_mask):
    return jnp.where(mm_nt(query_mask, key_mask) > 0.5, mm_nt(query, keys), NEG)


def forward_kernel(heads, nb, per, rows, row_ref, rand_ref, q_ref, qm_ref, kv_ref, km_ref, o_ref, lse_ref):
    row = row_ref[0]

    def place(j, head):
        start = pl.multiple_of(j * BLOCK, BLOCK)
        return pl.ds(start, BLOCK), slice(head * LANES, (head + 1) * LANES)

    def step(j, carry):
        pos = block_of(j, row, per, rows)
        is_global = (pos == 0) | (pos == nb - 1)
        query_mask = qm_ref[pl.ds(pl.multiple_of(j * BLOCK, BLOCK), BLOCK), :]

        @pl.when(jnp.logical_not(is_global))
        def _():
            for head in range(heads):
                at = place(j, head)
                blocks, masks = sparse_lists(rand_ref, head, pos, nb)
                keys = gather(kv_ref, blocks, head)
                score = scores_of(q_ref[at], query_mask, keys, gather(km_ref, masks, 0))
                top = jnp.max(score, axis=1, keepdims=True)
                weight = jnp.exp(score - top)
                total = jnp.sum(weight, axis=1, keepdims=True)
                probs = (weight * (1.0 / total)).astype(BF)
                o_ref[at] = mm(probs, keys).astype(BF)
                lse_ref[at] = jnp.broadcast_to(top + jnp.log(total), (BLOCK, LANES))

        @pl.when(is_global)
        def _():
            def score_at(group, head):
                blocks, masks = dense_lists(group, pos, nb)
                keys = gather(kv_ref, blocks, head)
                score = scores_of(
                    q_ref[place(j, head)], query_mask, keys, gather(km_ref, masks, 0)
                )
                return score, keys

            def stats(group, kept):
                new = []
                for head in range(heads):
                    top, total = kept[head]
                    score, _ = score_at(group, head)
                    above = jnp.maximum(top, jnp.max(score, axis=1, keepdims=True))
                    total = total * jnp.exp(top - above) + jnp.sum(
                        jnp.exp(score - above), axis=1, keepdims=True
                    )
                    new.append((above, total))
                return tuple(new)

            first = tuple(
                (jnp.full((BLOCK, 1), 2 * NEG, F32), jnp.zeros((BLOCK, 1), F32))
                for _ in range(heads)
            )
            found = lax.fori_loop(0, nb // 8, stats, first)
            lses = [top + jnp.log(total) for top, total in found]

            def outs(group, kept):
                new = []
                for head in range(heads):
                    score, keys = score_at(group, head)
                    new.append(kept[head] + mm(jnp.exp(score - lses[head]).astype(BF), keys))
                return tuple(new)

            done = lax.fori_loop(
                0, nb // 8, outs, tuple(jnp.zeros((BLOCK, LANES), F32) for _ in range(heads))
            )
            for head in range(heads):
                at = place(j, head)
                o_ref[at] = done[head].astype(BF)
                lse_ref[at] = jnp.broadcast_to(lses[head], (BLOCK, LANES))

        return carry

    lax.fori_loop(0, q_ref.shape[0] // BLOCK, step, 0)


def backward_kernel(
    heads, nb, per, rows, row_ref, rand_ref, q_ref, qm_ref, kv_ref, km_ref, do_ref, lse_ref,
    dq_ref, dkv_ref, acc_ref,
):
    row = row_ref[0]
    acc_ref[...] = jnp.zeros_like(acc_ref)

    def place(j, head):
        start = pl.multiple_of(j * BLOCK, BLOCK)
        return pl.ds(start, BLOCK), slice(head * LANES, (head + 1) * LANES)

    def parts(j, head, query_mask, blocks, masks):
        at = place(j, head)
        keys = gather(kv_ref, blocks, head)
        score = scores_of(q_ref[at], query_mask, keys, gather(km_ref, masks, 0))
        lse = lse_ref[at][:, :1]
        probs = jnp.exp(score - lse)
        return keys, probs, mm_nt(do_ref[at], keys)

    def finish(j, head, blocks, keys, probs, grad_probs, dot_row):
        at = place(j, head)
        low = (probs * (grad_probs - dot_row)).astype(BF)
        both = jnp.concatenate([low, probs.astype(BF)], axis=0)
        sides = jnp.concatenate([q_ref[at], do_ref[at]], axis=0)
        grad = mm_tn(both, sides)
        for i, block in enumerate(blocks):
            start = pl.multiple_of(block * BLOCK, BLOCK)
            acc_ref[pl.ds(start, BLOCK), at[1]] += grad[i * BLOCK : (i + 1) * BLOCK, :]
        return mm(low, keys)

    def step(j, carry):
        pos = block_of(j, row, per, rows)
        is_global = (pos == 0) | (pos == nb - 1)
        query_mask = qm_ref[pl.ds(pl.multiple_of(j * BLOCK, BLOCK), BLOCK), :]

        @pl.when(jnp.logical_not(is_global))
        def _():
            for head in range(heads):
                blocks, masks = sparse_lists(rand_ref, head, pos, nb)
                keys, probs, grad_probs = parts(j, head, query_mask, blocks, masks)
                dot_row = jnp.sum(probs * grad_probs, axis=1, keepdims=True)
                grad_q = finish(j, head, blocks, keys, probs, grad_probs, dot_row)
                dq_ref[place(j, head)] = (grad_q * 0.125).astype(BF)

        @pl.when(is_global)
        def _():
            def dots(group, kept):
                blocks, masks = dense_lists(group, pos, nb)
                new = []
                for head in range(heads):
                    _, probs, grad_probs = parts(j, head, query_mask, blocks, masks)
                    new.append(kept[head] + jnp.sum(probs * grad_probs, axis=1, keepdims=True))
                return tuple(new)

            dot_rows = lax.fori_loop(
                0, nb // 8, dots, tuple(jnp.zeros((BLOCK, 1), F32) for _ in range(heads))
            )

            def grads(group, kept):
                blocks, masks = dense_lists(group, pos, nb)
                new = []
                for head in range(heads):
                    keys, probs, grad_probs = parts(j, head, query_mask, blocks, masks)
                    new.append(
                        kept[head]
                        + finish(j, head, blocks, keys, probs, grad_probs, dot_rows[head])
                    )
                return tuple(new)

            done = lax.fori_loop(
                0, nb // 8, grads, tuple(jnp.zeros((BLOCK, LANES), F32) for _ in range(heads))
            )
            for head in range(heads):
                dq_ref[place(j, head)] = (done[head] * 0.125).astype(BF)

        return carry

    lax.fori_loop(0, q_ref.shape[0] // BLOCK, step, 0)
    span = per * BLOCK

    def out(i, carry):
        source = (i % rows) * (rows * span) + (i // rows) * span
        dkv_ref[pl.ds(pl.multiple_of(i * span, span), span), :] = acc_ref[
            pl.ds(pl.multiple_of(source, span), span), :
        ].astype(BF)
        return carry

    lax.fori_loop(0, kv_ref.shape[0] // span, out, 0)


def specs(count):
    return [pl.BlockSpec(memory_space=pltpu.SMEM)] * 2 + [
        pl.BlockSpec(memory_space=pltpu.VMEM)
    ] * count


def attention_forward(dims, row, rand, q, q_mask, kv, k_mask):
    own, wide = q.shape
    vmem = pl.BlockSpec(memory_space=pltpu.VMEM)
    return pl.pallas_call(
        functools.partial(forward_kernel, *dims),
        name="attn_fwd",
        out_shape=(
            jax.ShapeDtypeStruct((own, wide), BF),
            jax.ShapeDtypeStruct((own, wide), F32),
        ),
        in_specs=specs(4),
        out_specs=(vmem, vmem),
        cost_estimate=pl.CostEstimate(
            flops=own * 512 * wide * 6, bytes_accessed=12 << 20, transcendentals=own * 512 * 3
        ),
        compiler_params=pltpu.CompilerParams(vmem_limit_bytes=48 << 20),
    )(row, rand, q, q_mask, kv, k_mask)


def attention_backward(dims, row, rand, q, q_mask, kv, k_mask, d_o, lse):
    own, wide = q.shape
    vmem = pl.BlockSpec(memory_space=pltpu.VMEM)
    return pl.pallas_call(
        functools.partial(backward_kernel, *dims),
        name="attn_bwd",
        out_shape=(
            jax.ShapeDtypeStruct((own, wide), BF),
            jax.ShapeDtypeStruct(kv.shape, BF),
        ),
        in_specs=specs(6),
        out_specs=(vmem, vmem),
        scratch_shapes=[pltpu.VMEM(kv.shape, F32)],
        cost_estimate=pl.CostEstimate(
            flops=own * 512 * wide * 12, bytes_accessed=20 << 20, transcendentals=own * 512 * 3
        ),
        compiler_params=pltpu.CompilerParams(vmem_limit_bytes=48 << 20),
    )(row, rand, q, q_mask, kv, k_mask, d_o, lse)


def project_kernel(rows, span, row_ref, x_ref, wq_ref, wkv_ref, q_ref, kv_ref, own_ref):
    feat = x_ref.shape[2]
    start = pl.multiple_of(row_ref[0] * span, span)
    kv = q = None
    for part in range(rows):
        at = slice(part * feat, (part + 1) * feat)
        mine = x_ref[part, 0, :, pl.ds(start, span)]
        own_ref[at, :] = mine
        kv_part = mm_tn(x_ref[part, 0], wkv_ref[at, :])
        q_part = mm_tn(mine, wq_ref[at, :])
        kv = kv_part if kv is None else kv + kv_part
        q = q_part if q is None else q + q_part
    kv_ref[...] = kv.astype(BF)
    q_ref[...] = (q.astype(BF) * 0.125).astype(BF)


def project(row, x_parts, w_q, w_kv, span):
    rows, cols, feat, local = x_parts.shape
    model, wide = w_q.shape
    return pl.pallas_call(
        functools.partial(project_kernel, rows, span),
        name="project",
        grid=(cols,),
        out_shape=(
            jax.ShapeDtypeStruct((cols * span, wide), BF),
            jax.ShapeDtypeStruct((cols * local, wide), BF),
            jax.ShapeDtypeStruct((model, cols * span), BF),
        ),
        in_specs=[
            pl.BlockSpec(memory_space=pltpu.SMEM),
            pl.BlockSpec((rows, 1, feat, local), lambda c: (0, c, 0, 0)),
            pl.BlockSpec((model, wide), lambda c: (0, 0)),
            pl.BlockSpec((model, wide), lambda c: (0, 0)),
        ],
        out_specs=(
            pl.BlockSpec((span, wide), lambda c: (c, 0)),
            pl.BlockSpec((local, wide), lambda c: (c, 0)),
            pl.BlockSpec((model, span), lambda c: (0, c)),
        ),
        cost_estimate=pl.CostEstimate(
            flops=cols * local * model * wide * 3, bytes_accessed=16 << 20, transcendentals=0
        ),
        compiler_params=pltpu.CompilerParams(vmem_limit_bytes=48 << 20),
    )(row, x_parts, w_q, w_kv)


PIECES = 2


def col_places():
    me = lax.axis_index("col")
    partner = me + 1 - 2 * lax.rem(me, 2)
    cross = lax.rem(me + 2, 4)
    diag = lax.rem(partner + 2, 4)
    barrier = pltpu.get_barrier_semaphore()
    for peer in (partner, cross):
        pl.semaphore_signal(
            barrier, inc=1, device_id={"col": peer}, device_id_type=pl.DeviceIdType.MESH
        )
    pl.semaphore_wait(barrier, 2)
    return me, partner, cross, diag


def send_to(source, target, sems, kind, piece, peer):
    copy = pltpu.make_async_remote_copy(
        src_ref=source,
        dst_ref=target,
        send_sem=sems[0].at[kind, piece],
        recv_sem=sems[1].at[kind, piece],
        device_id={"col": peer},
        device_id_type=pl.DeviceIdType.MESH,
    )
    copy.start()
    return copy


def gather_kernel(x_ref, out_ref, send_sem, recv_sem):
    me, partner, cross, _ = col_places()
    sems = (send_sem, recv_sem)
    size = x_ref.shape[0] // PIECES
    cuts = [pl.ds(i * size, size) for i in range(PIECES)]
    over = [
        send_to(x_ref.at[cut], out_ref.at[me, cut], sems, 0, i, cross)
        for i, cut in enumerate(cuts)
    ]
    near = [
        send_to(x_ref.at[cut], out_ref.at[me, cut], sems, 1, i, partner)
        for i, cut in enumerate(cuts)
    ]
    out_ref[me] = x_ref[...]
    relay = []
    for i, cut in enumerate(cuts):
        over[i].wait_recv()
        relay.append(
            send_to(out_ref.at[cross, cut], out_ref.at[cross, cut], sems, 2, i, partner)
        )
    for i in range(PIECES):
        over[i].wait_send()
        near[i].wait()
        relay[i].wait()


def scatter_kernel(x_ref, out_ref, near_buf, sum_buf, over_buf, send_sem, recv_sem):
    me, partner, cross, diag = col_places()
    sems = (send_sem, recv_sem)
    size = x_ref.shape[1] // PIECES
    cuts = [pl.ds(i * size, size) for i in range(PIECES)]
    first = [
        send_to(x_ref.at[diag, cut], near_buf.at[1, cut], sems, 0, i, partner)
        for i, cut in enumerate(cuts)
    ]
    second = [
        send_to(x_ref.at[partner, cut], near_buf.at[0, cut], sems, 1, i, partner)
        for i, cut in enumerate(cuts)
    ]
    over = []
    for i, cut in enumerate(cuts):
        first[i].wait_recv()
        sum_buf[cut, :] = (
            x_ref[cross, cut, :].astype(F32) + near_buf[1, cut, :].astype(F32)
        ).astype(BF)
        over.append(send_to(sum_buf.at[cut], over_buf.at[cut], sems, 2, i, cross))
    for i, cut in enumerate(cuts):
        second[i].wait_recv()
        out_ref[cut, :] = x_ref[me, cut, :].astype(F32) + near_buf[0, cut, :].astype(F32)
    for i, cut in enumerate(cuts):
        over[i].wait_recv()
        out_ref[cut, :] += over_buf[cut, :].astype(F32)
    for i in range(PIECES):
        first[i].wait_send()
        second[i].wait_send()
        over[i].wait_send()


def comm_params(ident):
    return pltpu.CompilerParams(
        collective_id=ident, has_side_effects=True, vmem_limit_bytes=32 << 20
    )


def comm_sems(kinds):
    return [pltpu.SemaphoreType.DMA((kinds, PIECES)), pltpu.SemaphoreType.DMA((kinds, PIECES))]


def gather_col(value, ident):
    count, wide = value.shape
    vmem = pl.BlockSpec(memory_space=pltpu.VMEM)
    return pl.pallas_call(
        gather_kernel,
        name="gather_col",
        out_shape=jax.ShapeDtypeStruct((4, count, wide), BF),
        in_specs=[vmem],
        out_specs=vmem,
        scratch_shapes=comm_sems(3),
        compiler_params=comm_params(ident),
    )(value)


def scatter_col(value):
    count, wide = value.shape[0] // 4, value.shape[1]
    vmem = pl.BlockSpec(memory_space=pltpu.VMEM)
    return pl.pallas_call(
        scatter_kernel,
        name="scatter_col",
        out_shape=jax.ShapeDtypeStruct((count, wide), F32),
        in_specs=[vmem],
        out_specs=vmem,
        scratch_shapes=[
            pltpu.VMEM((2, count, wide), BF),
            pltpu.VMEM((count, wide), BF),
            pltpu.VMEM((count, wide), BF),
        ]
        + comm_sems(3),
        compiler_params=comm_params(2),
    )(value.reshape(4, count, wide))


def norm(resid, gain, bias):
    mean = jnp.mean(resid, axis=1, keepdims=True)
    var = jnp.mean(resid * resid, axis=1, keepdims=True) - mean * mean
    rstd = lax.rsqrt(var + EPS)
    normed = (resid - mean) * rstd
    return normed * gain + bias, normed, rstd


def norm_grad(grad, normed, rstd, gain):
    scaled = grad * gain
    first = jnp.mean(scaled, axis=1, keepdims=True)
    second = jnp.mean(scaled * normed, axis=1, keepdims=True)
    return rstd * (scaled - first - normed * second)


def gelu(value):
    return jax.nn.gelu(value, approximate=True)


def on_device(
    inputs, w_query, w_key, w_value, w_out, w_up, w_down,
    ln1_gain, ln1_bias, ln2_gain, ln2_bias, segment_ids, pad_mask, rand_blocks, grad_out,
):
    rows, cols = lax.axis_size("row"), lax.axis_size("col")
    row, col = lax.axis_index("row"), lax.axis_index("col")
    feat, local = inputs.shape
    model = feat * rows
    hid = model // cols
    heads = hid // HW
    length = local * cols
    nb = length // BLOCK
    span = local // rows
    per = span // BLOCK
    dims = (heads, nb, per, rows)
    own = cols * span

    blk_q = w_query.reshape(feat, hid)
    blk_k = w_key.reshape(feat, hid)
    blk_v = w_value.reshape(feat, hid)
    blk_o = w_out.reshape(hid, feat)
    params = jnp.stack([ln1_gain, ln1_bias, ln2_gain, ln2_bias], axis=1)
    high = params.astype(BF)
    rest = params - high.astype(F32)
    middle = rest.astype(BF)
    low = (rest - middle.astype(F32)).astype(BF)
    w_qkv = jnp.concatenate([blk_q, blk_k, blk_v, high, middle, low], axis=1)
    w_own = lax.all_gather(w_qkv, "row", axis=0, tiled=True)
    x_parts = lax.all_gather(inputs, ("row", "col"), axis=0)
    w_rest = jnp.concatenate([w_up, w_down, blk_o.T], axis=1)
    x_parts, w_rest, grad_out = lax.optimization_barrier((x_parts, w_rest, grad_out))
    x_parts = x_parts.reshape(rows, cols, feat, local)
    w_rest = lax.all_gather(w_rest, "row", axis=0, tiled=True)
    ff = w_up.shape[1]
    up, down, w_o = w_rest[:, :ff], w_rest[:, ff : 2 * ff], w_rest[:, 2 * ff :]
    gains = w_own[:, 3 * hid :].astype(F32)
    gains = (gains[:, :4] + gains[:, 4:8]) + gains[:, 8:12]
    gains = gains.T.reshape(4, 1, model)
    w_own = w_own[:, : 3 * hid]
    grad_rows = lax.all_to_all(grad_out, "row", 1, 0, tiled=True).T.astype(F32)

    w_heads = w_own.reshape(model, 3, heads, HW)
    w_kv = jnp.concatenate([w_heads[:, 1], w_heads[:, 2]], axis=2).reshape(model, heads * LANES)
    w_q = jnp.pad(w_heads[:, 0], ((0, 0), (0, 0), (0, HW))).reshape(model, heads * LANES)
    row_arr = jnp.reshape(row, (1,)).astype(jnp.int32)
    q, kv, x_own = project(row_arr, x_parts, w_q, w_kv, span)
    x_res = lax.dynamic_slice_in_dim(x_own, col * span, span, axis=1).T.astype(F32)

    kinds = jnp.arange(BLOCK, dtype=jnp.int32)
    seg_hot = segment_ids[:, None] == kinds[None, :]
    key_hot = (seg_hot & (pad_mask[:, None] == 1)).astype(BF)
    place_hot = ((jnp.arange(length, dtype=jnp.int32) % BLOCK)[:, None] == kinds[None, :]).astype(BF)
    zeros = jnp.zeros_like(key_hot)
    k_mask = jnp.concatenate(
        [
            jnp.concatenate([key_hot, zeros], axis=1),
            jnp.concatenate([key_hot, place_hot], axis=1),
            jnp.zeros((BLOCK, LANES), BF),
        ],
        axis=0,
    )
    q_mask = jnp.concatenate([seg_hot.astype(BF), place_hot], axis=1)
    q_mask = lax.dynamic_index_in_dim(
        q_mask.reshape(cols, rows, span, LANES), row, axis=1, keepdims=False
    ).reshape(own, LANES)
    rand = rand_blocks.reshape(-1)

    o_wide, lse = attention_forward(dims, row_arr, rand, q, q_mask, kv, k_mask)
    o = o_wide.reshape(own, heads, 2, HW)[:, :, 1].reshape(own, hid)
    attn = scatter_col(mm_nt(o, w_o).astype(BF))

    gain1, bias1, gain2, bias2 = gains[0], gains[1], gains[2], gains[3]
    hidden, normed1, rstd1 = norm(x_res + attn, gain1, bias1)
    hidden_all = gather_col(hidden.astype(BF), 1).reshape(own, model)
    up_val = mm(hidden_all, up)
    act, gelu_back = jax.vjp(gelu, up_val)
    act = act.astype(BF)
    ffn = scatter_col(mm_nt(act, down).astype(BF))
    result, normed2, rstd2 = norm(hidden + ffn, gain2, bias2)
    output = lax.all_to_all(result.T.astype(BF), "row", 0, 1, tiled=True)

    grad2 = norm_grad(grad_rows, normed2, rstd2, gain2)
    df = gather_col(grad2.astype(BF), 1).reshape(own, model)
    g_down = mm_tn(df, act).astype(BF)
    du = gelu_back(mm(df, down))[0].astype(BF)
    g_up = mm_tn(hidden_all, du).astype(BF)
    dh = scatter_col(mm_nt(du, up).astype(BF)) + grad2
    grad1 = norm_grad(dh, normed1, rstd1, gain1)
    sums = jnp.stack(
        [
            jnp.sum(dh * normed1, axis=0),
            jnp.sum(dh, axis=0),
            jnp.sum(grad_rows * normed2, axis=0),
            jnp.sum(grad_rows, axis=0),
        ]
    )
    extra = jnp.pad(sums, ((0, 28), (0, 0))).astype(BF)
    dattn = gather_col(jnp.concatenate([grad1.astype(BF), extra], axis=0), 3)
    sums = jnp.sum(dattn[:, span : span + 4].astype(F32), axis=0)
    dattn = dattn[:, :span].reshape(own, model)
    g_out = mm_tn(dattn, o).astype(BF)
    d_o = mm(dattn, w_o).astype(BF)
    d_o = jnp.pad(d_o.reshape(own, heads, HW), ((0, 0), (0, 0), (HW, 0))).reshape(own, -1)

    g_ffn = jnp.concatenate([g_up, g_down, g_out, sums.T.astype(BF)], axis=1)
    g_ffn = lax.psum_scatter(g_ffn, "row", scatter_dimension=0, tiled=True)
    g_sums = g_ffn[:, 2 * ff + hid :]
    g_ffn = lax.psum(g_ffn[:, : 2 * ff + hid], "dp").astype(F32)
    g_sums = lax.psum(g_sums, ("dp",)).astype(F32).T

    dq, dkv = attention_backward(dims, row_arr, rand, q, q_mask, kv, k_mask, d_o, lse)
    dkv = lax.psum_scatter(dkv, "row", scatter_dimension=0, tiled=True)
    dq = dq.reshape(own, heads, 2, HW)[:, :, 0].reshape(own, hid)
    dkv = dkv.reshape(own, heads, 2, HW)
    dqkv = jnp.concatenate(
        [dq, dkv[:, :, 0].reshape(own, hid), dkv[:, :, 1].reshape(own, hid)], axis=1
    )
    g_qkv = mm(x_own, dqkv).astype(BF)
    g_qkv = lax.psum_scatter(g_qkv, "row", scatter_dimension=0, tiled=True)
    g_qkv = lax.psum(g_qkv, "dp").astype(F32)
    grad_in = scatter_col(mm_nt(dqkv, w_own).astype(BF)) + grad1
    grad_in = lax.all_to_all(grad_in.T.astype(BF), "row", 0, 1, tiled=True).astype(F32)

    return (
        output,
        grad_in,
        g_qkv[:, :hid].reshape(1, 1, -1),
        g_qkv[:, hid : 2 * hid].reshape(1, 1, -1),
        g_qkv[:, 2 * hid :].reshape(1, 1, -1),
        g_ffn[:, 2 * ff :].T.reshape(1, 1, -1),
        g_ffn[:, :ff],
        g_ffn[:, ff : 2 * ff],
        g_sums[0],
        g_sums[1],
        g_sums[2],
        g_sums[3],
    )


def solution(mesh):
    tokens = P("row", ("dp", "col"))
    grid = P("row", "col", None)
    return jax.shard_map(
        on_device,
        mesh=mesh,
        in_specs=(
            tokens,
            grid,
            grid,
            grid,
            P("col", "row", None),
            P("row", "col"),
            P("row", "col"),
            P("row"),
            P("row"),
            P("row"),
            P("row"),
            P("dp"),
            P("dp"),
            P("dp", "col", None, None),
            tokens,
        ),
        out_specs=(
            tokens,
            tokens,
            grid,
            grid,
            grid,
            P("col", "row", None),
            P("row", "col"),
            P("row", "col"),
            P("row"),
            P("row"),
            P("row"),
            P("row"),
        ),
        check_vma=False,
    )
```

```python
import functools

import jax
import jax.numpy as jnp
from jax import lax
from jax.experimental import pallas as pl
from jax.experimental.pallas import tpu as pltpu
from jax.sharding import PartitionSpec as P


BLOCK = 64
HW = 64
LANES = 128
NEG = -1000000000.0
EPS = 1e-06
BF = jnp.bfloat16
F32 = jnp.float32


def mm(left, right):
    return lax.dot_general(left, right, (((1,), (0,)), ((), ())), preferred_element_type=F32)


def mm_nt(left, right):
    return lax.dot_general(left, right, (((1,), (1,)), ((), ())), preferred_element_type=F32)


def mm_tn(left, right):
    return lax.dot_general(left, right, (((0,), (0,)), ((), ())), preferred_element_type=F32)


def block_of(j, row, per, rows):
    return (j // per) * (per * rows) + row * per + j % per


def rows_at(ref, block, head):
    start = pl.multiple_of(block * BLOCK, BLOCK)
    return ref[pl.ds(start, BLOCK), head * LANES : (head + 1) * LANES]


def sparse_lists(rand_ref, head, pos, nb):
    before = jnp.maximum(pos - 1, 0)
    after = jnp.minimum(pos + 1, nb - 1)
    picks = [rand_ref[(head * nb + pos) * 3 + i] for i in range(3)]
    return [0, nb - 1, before, pos, after] + picks


def dense_list(group):
    return [group * 8 + i for i in range(8)]


def sparse_bar(pos, nb):
    entry = lax.broadcasted_iota(jnp.int32, (1, 8 * BLOCK), 1) // BLOCK
    no_before = jnp.where(pos < 2, 8.0, 0.0)
    no_after = jnp.where(pos > nb - 3, 8.0, 0.0)
    return 0.5 + jnp.where(entry == 2, no_before, 0.0) + jnp.where(entry == 4, no_after, 0.0)


def gather(ref, blocks, head):
    return jnp.concatenate([rows_at(ref, b, head) for b in blocks], axis=0)


def scores_of(query, query_mask, keys, key_mask, own, bar):
    shape = (query.shape[0], keys.shape[0])
    apart = lax.broadcasted_iota(jnp.int32, shape, 1) - lax.broadcasted_iota(jnp.int32, shape, 0)
    allowed = (mm_nt(query_mask, key_mask) > bar) | (apart == own * BLOCK)
    return jnp.where(allowed, mm_nt(query, keys), NEG)


def forward_kernel(heads, nb, per, rows, row_ref, rand_ref, q_ref, qm_ref, kv_ref, km_ref, o_ref, lse_ref):
    row = row_ref[0]

    def place(j, head):
        start = pl.multiple_of(j * BLOCK, BLOCK)
        return pl.ds(start, BLOCK), slice(head * LANES, (head + 1) * LANES)

    def step(j, carry):
        pos = block_of(j, row, per, rows)
        is_global = (pos == 0) | (pos == nb - 1)
        query_mask = qm_ref[pl.ds(pl.multiple_of(j * BLOCK, BLOCK), BLOCK), :]

        @pl.when(jnp.logical_not(is_global))
        def _():
            for head in range(heads):
                at = place(j, head)
                blocks = sparse_lists(rand_ref, head, pos, nb)
                keys = gather(kv_ref, blocks, head)
                score = scores_of(
                    q_ref[at], query_mask, keys, gather(km_ref, blocks, 0), 3, sparse_bar(pos, nb)
                )
                top = jnp.max(score, axis=1, keepdims=True)
                weight = jnp.exp(score - top)
                total = jnp.sum(weight, axis=1, keepdims=True)
                probs = (weight * (1.0 / total)).astype(BF)
                o_ref[at] = mm(probs, keys).astype(BF)
                lse_ref[at] = jnp.broadcast_to(top + jnp.log(total), (BLOCK, LANES))

        @pl.when(is_global)
        def _():
            def score_at(group, head):
                blocks = dense_list(group)
                keys = gather(kv_ref, blocks, head)
                score = scores_of(
                    q_ref[place(j, head)], query_mask, keys, gather(km_ref, blocks, 0),
                    pos - group * 8, 0.5,
                )
                return score, keys

            def stats(group, kept):
                new = []
                for head in range(heads):
                    top, total = kept[head]
                    score, _ = score_at(group, head)
                    above = jnp.maximum(top, jnp.max(score, axis=1, keepdims=True))
                    total = total * jnp.exp(top - above) + jnp.sum(
                        jnp.exp(score - above), axis=1, keepdims=True
                    )
                    new.append((above, total))
                return tuple(new)

            first = tuple(
                (jnp.full((BLOCK, 1), 2 * NEG, F32), jnp.zeros((BLOCK, 1), F32))
                for _ in range(heads)
            )
            found = lax.fori_loop(0, nb // 8, stats, first)
            lses = [top + jnp.log(total) for top, total in found]

            def outs(group, kept):
                new = []
                for head in range(heads):
                    score, keys = score_at(group, head)
                    new.append(kept[head] + mm(jnp.exp(score - lses[head]).astype(BF), keys))
                return tuple(new)

            done = lax.fori_loop(
                0, nb // 8, outs, tuple(jnp.zeros((BLOCK, LANES), F32) for _ in range(heads))
            )
            for head in range(heads):
                at = place(j, head)
                o_ref[at] = done[head].astype(BF)
                lse_ref[at] = jnp.broadcast_to(lses[head], (BLOCK, LANES))

        return carry

    lax.fori_loop(0, q_ref.shape[0] // BLOCK, step, 0)


def backward_kernel(
    heads, nb, per, rows, row_ref, rand_ref, q_ref, qm_ref, kv_ref, km_ref, do_ref, lse_ref,
    dq_ref, dkv_ref, acc_ref,
):
    row = row_ref[0]
    acc_ref[...] = jnp.zeros_like(acc_ref)

    def place(j, head):
        start = pl.multiple_of(j * BLOCK, BLOCK)
        return pl.ds(start, BLOCK), slice(head * LANES, (head + 1) * LANES)

    def parts(j, head, query_mask, blocks, mine, bar):
        at = place(j, head)
        keys = gather(kv_ref, blocks, head)
        score = scores_of(q_ref[at], query_mask, keys, gather(km_ref, blocks, 0), mine, bar)
        lse = lse_ref[at][:, :1]
        probs = jnp.exp(score - lse)
        return keys, probs, mm_nt(do_ref[at], keys)

    def finish(j, head, blocks, keys, probs, grad_probs, dot_row):
        at = place(j, head)
        low = (probs * (grad_probs - dot_row)).astype(BF)
        both = jnp.concatenate([low, probs.astype(BF)], axis=0)
        sides = jnp.concatenate([q_ref[at], do_ref[at]], axis=0)
        grad = mm_tn(both, sides)
        for i, block in enumerate(blocks):
            start = pl.multiple_of(block * BLOCK, BLOCK)
            acc_ref[pl.ds(start, BLOCK), at[1]] += grad[i * BLOCK : (i + 1) * BLOCK, :]
        return mm(low, keys)

    def step(j, carry):
        pos = block_of(j, row, per, rows)
        is_global = (pos == 0) | (pos == nb - 1)
        query_mask = qm_ref[pl.ds(pl.multiple_of(j * BLOCK, BLOCK), BLOCK), :]

        @pl.when(jnp.logical_not(is_global))
        def _():
            for head in range(heads):
                blocks = sparse_lists(rand_ref, head, pos, nb)
                keys, probs, grad_probs = parts(
                    j, head, query_mask, blocks, 3, sparse_bar(pos, nb)
                )
                dot_row = jnp.sum(probs * grad_probs, axis=1, keepdims=True)
                grad_q = finish(j, head, blocks, keys, probs, grad_probs, dot_row)
                dq_ref[place(j, head)] = (grad_q * 0.125).astype(BF)

        @pl.when(is_global)
        def _():
            def dots(group, kept):
                blocks = dense_list(group)
                mine = pos - group * 8
                new = []
                for head in range(heads):
                    _, probs, grad_probs = parts(j, head, query_mask, blocks, mine, 0.5)
                    new.append(kept[head] + jnp.sum(probs * grad_probs, axis=1, keepdims=True))
                return tuple(new)

            dot_rows = lax.fori_loop(
                0, nb // 8, dots, tuple(jnp.zeros((BLOCK, 1), F32) for _ in range(heads))
            )

            def grads(group, kept):
                blocks = dense_list(group)
                mine = pos - group * 8
                new = []
                for head in range(heads):
                    keys, probs, grad_probs = parts(j, head, query_mask, blocks, mine, 0.5)
                    new.append(
                        kept[head]
                        + finish(j, head, blocks, keys, probs, grad_probs, dot_rows[head])
                    )
                return tuple(new)

            done = lax.fori_loop(
                0, nb // 8, grads, tuple(jnp.zeros((BLOCK, LANES), F32) for _ in range(heads))
            )
            for head in range(heads):
                dq_ref[place(j, head)] = (done[head] * 0.125).astype(BF)

        return carry

    lax.fori_loop(0, q_ref.shape[0] // BLOCK, step, 0)
    span = per * BLOCK

    def out(i, carry):
        source = (i % rows) * (rows * span) + (i // rows) * span
        dkv_ref[pl.ds(pl.multiple_of(i * span, span), span), :] = acc_ref[
            pl.ds(pl.multiple_of(source, span), span), :
        ].astype(BF)
        return carry

    lax.fori_loop(0, kv_ref.shape[0] // span, out, 0)


def specs(count):
    return [pl.BlockSpec(memory_space=pltpu.SMEM)] * 2 + [
        pl.BlockSpec(memory_space=pltpu.VMEM)
    ] * count


def attention_forward(dims, row, rand, q, q_mask, kv, k_mask):
    own, wide = q.shape
    vmem = pl.BlockSpec(memory_space=pltpu.VMEM)
    return pl.pallas_call(
        functools.partial(forward_kernel, *dims),
        name="attn_fwd",
        out_shape=(
            jax.ShapeDtypeStruct((own, wide), BF),
            jax.ShapeDtypeStruct((own, wide), F32),
        ),
        in_specs=specs(4),
        out_specs=(vmem, vmem),
        cost_estimate=pl.CostEstimate(
            flops=own * 512 * wide * 6, bytes_accessed=12 << 20, transcendentals=own * 512 * 3
        ),
        compiler_params=pltpu.CompilerParams(vmem_limit_bytes=48 << 20),
    )(row, rand, q, q_mask, kv, k_mask)


def attention_backward(dims, row, rand, q, q_mask, kv, k_mask, d_o, lse):
    own, wide = q.shape
    vmem = pl.BlockSpec(memory_space=pltpu.VMEM)
    return pl.pallas_call(
        functools.partial(backward_kernel, *dims),
        name="attn_bwd",
        out_shape=(
            jax.ShapeDtypeStruct((own, wide), BF),
            jax.ShapeDtypeStruct(kv.shape, BF),
        ),
        in_specs=specs(6),
        out_specs=(vmem, vmem),
        scratch_shapes=[pltpu.VMEM(kv.shape, F32)],
        cost_estimate=pl.CostEstimate(
            flops=own * 512 * wide * 12, bytes_accessed=20 << 20, transcendentals=own * 512 * 3
        ),
        compiler_params=pltpu.CompilerParams(vmem_limit_bytes=48 << 20),
    )(row, rand, q, q_mask, kv, k_mask, d_o, lse)


def one_hot_rows(hot):
    kinds = hot.shape[0]
    shape = (kinds, LANES)
    eye = lax.broadcasted_iota(jnp.int32, shape, 0) == lax.broadcasted_iota(jnp.int32, shape, 1)
    return mm_tn(jnp.where(hot, 1.0, 0.0).astype(BF), jnp.where(eye, 1.0, 0.0).astype(BF)).astype(BF)


def project_kernel(
    rows, span, row_ref, x_ref, wq_ref, wkv_ref, seg_ref, pad_ref,
    q_ref, kv_ref, own_ref, qm_ref, km_ref,
):
    feat = x_ref.shape[2]
    start = pl.multiple_of(row_ref[0] * span, span)
    kv = q = None
    for part in range(rows):
        at = slice(part * feat, (part + 1) * feat)
        mine = x_ref[part, 0, :, pl.ds(start, span)]
        own_ref[at, :] = mine
        kv_part = mm_tn(x_ref[part, 0], wkv_ref[at, :])
        q_part = mm_tn(mine, wq_ref[at, :])
        kv = kv_part if kv is None else kv + kv_part
        q = q_part if q is None else q + q_part
    kv_ref[...] = kv.astype(BF)
    q_ref[...] = (q.astype(BF) * 0.125).astype(BF)
    segs = seg_ref[...]
    kinds = lax.broadcasted_iota(jnp.int32, (BLOCK, segs.shape[1]), 0)
    km_ref[...] = one_hot_rows((kinds == segs) & (pad_ref[...] == 1))
    mine = seg_ref[:, pl.ds(start, span)]
    kinds = lax.broadcasted_iota(jnp.int32, (BLOCK, span), 0)
    qm_ref[...] = one_hot_rows(kinds == mine)


def project(row, x_parts, w_q, w_kv, span, segs, pads):
    rows, cols, feat, local = x_parts.shape
    model, wide = w_q.shape
    return pl.pallas_call(
        functools.partial(project_kernel, rows, span),
        name="project",
        grid=(cols,),
        out_shape=(
            jax.ShapeDtypeStruct((cols * span, wide), BF),
            jax.ShapeDtypeStruct((cols * local, wide), BF),
            jax.ShapeDtypeStruct((model, cols * span), BF),
            jax.ShapeDtypeStruct((cols * span, LANES), BF),
            jax.ShapeDtypeStruct((cols * local, LANES), BF),
        ),
        in_specs=[
            pl.BlockSpec(memory_space=pltpu.SMEM),
            pl.BlockSpec((rows, 1, feat, local), lambda c: (0, c, 0, 0)),
            pl.BlockSpec((model, wide), lambda c: (0, 0)),
            pl.BlockSpec((model, wide), lambda c: (0, 0)),
            pl.BlockSpec((1, local), lambda c: (0, c)),
            pl.BlockSpec((1, local), lambda c: (0, c)),
        ],
        out_specs=(
            pl.BlockSpec((span, wide), lambda c: (c, 0)),
            pl.BlockSpec((local, wide), lambda c: (c, 0)),
            pl.BlockSpec((model, span), lambda c: (0, c)),
            pl.BlockSpec((span, LANES), lambda c: (c, 0)),
            pl.BlockSpec((local, LANES), lambda c: (c, 0)),
        ),
        cost_estimate=pl.CostEstimate(
            flops=cols * local * model * wide * 3, bytes_accessed=16 << 20, transcendentals=0
        ),
        compiler_params=pltpu.CompilerParams(vmem_limit_bytes=48 << 20),
    )(row, x_parts, w_q, w_kv, segs.reshape(1, -1), pads.reshape(1, -1))


PIECES = 2


def col_places():
    me = lax.axis_index("col")
    partner = me + 1 - 2 * lax.rem(me, 2)
    cross = lax.rem(me + 2, 4)
    diag = lax.rem(partner + 2, 4)
    barrier = pltpu.get_barrier_semaphore()
    for peer in (partner, cross):
        pl.semaphore_signal(
            barrier, inc=1, device_id={"col": peer}, device_id_type=pl.DeviceIdType.MESH
        )
    pl.semaphore_wait(barrier, 2)
    return me, partner, cross, diag


def send_to(source, target, sems, kind, piece, peer):
    copy = pltpu.make_async_remote_copy(
        src_ref=source,
        dst_ref=target,
        send_sem=sems[0].at[kind, piece],
        recv_sem=sems[1].at[kind, piece],
        device_id={"col": peer},
        device_id_type=pl.DeviceIdType.MESH,
    )
    copy.start()
    return copy


def gather_kernel(x_ref, out_ref, send_sem, recv_sem):
    me, partner, cross, _ = col_places()
    sems = (send_sem, recv_sem)
    size = x_ref.shape[0] // PIECES
    cuts = [pl.ds(i * size, size) for i in range(PIECES)]
    over = [
        send_to(x_ref.at[cut], out_ref.at[me, cut], sems, 0, i, cross)
        for i, cut in enumerate(cuts)
    ]
    near = [
        send_to(x_ref.at[cut], out_ref.at[me, cut], sems, 1, i, partner)
        for i, cut in enumerate(cuts)
    ]
    out_ref[me] = x_ref[...]
    relay = []
    for i, cut in enumerate(cuts):
        over[i].wait_recv()
        relay.append(
            send_to(out_ref.at[cross, cut], out_ref.at[cross, cut], sems, 2, i, partner)
        )
    for i in range(PIECES):
        over[i].wait_send()
        near[i].wait()
        relay[i].wait()


def scatter_kernel(x_ref, out_ref, near_buf, sum_buf, over_buf, send_sem, recv_sem):
    me, partner, cross, diag = col_places()
    sems = (send_sem, recv_sem)
    size = x_ref.shape[1] // PIECES
    cuts = [pl.ds(i * size, size) for i in range(PIECES)]
    first = [
        send_to(x_ref.at[diag, cut], near_buf.at[1, cut], sems, 0, i, partner)
        for i, cut in enumerate(cuts)
    ]
    second = [
        send_to(x_ref.at[partner, cut], near_buf.at[0, cut], sems, 1, i, partner)
        for i, cut in enumerate(cuts)
    ]
    over = []
    for i, cut in enumerate(cuts):
        first[i].wait_recv()
        sum_buf[cut, :] = (
            x_ref[cross, cut, :].astype(F32) + near_buf[1, cut, :].astype(F32)
        ).astype(BF)
        over.append(send_to(sum_buf.at[cut], over_buf.at[cut], sems, 2, i, cross))
    for i, cut in enumerate(cuts):
        second[i].wait_recv()
        out_ref[cut, :] = x_ref[me, cut, :].astype(F32) + near_buf[0, cut, :].astype(F32)
    for i, cut in enumerate(cuts):
        over[i].wait_recv()
        out_ref[cut, :] += over_buf[cut, :].astype(F32)
    for i in range(PIECES):
        first[i].wait_send()
        second[i].wait_send()
        over[i].wait_send()


def scatter_row_kernel(
    rows, swap, x_ref, out_ref, from_left, from_right, to_right, to_left, own_buf, peer_buf,
    send_sem, recv_sem, swap_sem,
):
    me = lax.axis_index("row")
    right, left = lax.rem(me + 1, rows), lax.rem(me + rows - 1, rows)
    has_left, has_right = me > 0, me < rows - 1
    mesh_id = pl.DeviceIdType.MESH
    barrier = pltpu.get_barrier_semaphore()

    @pl.when(has_left)
    def _():
        pl.semaphore_signal(barrier, inc=1, device_id={"row": left}, device_id_type=mesh_id)

    @pl.when(has_right)
    def _():
        pl.semaphore_signal(barrier, inc=1, device_id={"row": right}, device_id_type=mesh_id)

    if swap:
        peer = 1 - lax.axis_index("dp")
        pl.semaphore_signal(barrier, inc=1, device_id={"dp": peer}, device_id_type=mesh_id)

    peers = jnp.where(has_left, 1, 0) + jnp.where(has_right, 1, 0) + (1 if swap else 0)
    pl.semaphore_wait(barrier, peers)

    size = x_ref.shape[1] // PIECES
    cuts = [pl.ds(i * size, size) for i in range(PIECES)]

    def hop(way, dest, i):
        stage, target, to = ((to_right, from_left, right), (to_left, from_right, left))[way]
        return pltpu.make_async_remote_copy(
            src_ref=stage.at[dest, cuts[i]],
            dst_ref=target.at[dest, cuts[i]],
            send_sem=send_sem.at[way, dest, i],
            recv_sem=recv_sem.at[way, dest, i],
            device_id={"row": to},
            device_id_type=mesh_id,
        )

    flows = []
    for step in range(rows - 1):
        flows.append((0, rows - 1 - step, me < rows - 1 - step, has_left))
        flows.append((1, step, me > step, has_right))
    for way, dest, active, relays in flows:
        stage, came = ((to_right, from_left), (to_left, from_right))[way]
        for i, cut in enumerate(cuts):

            @pl.when(active & relays)
            def _():
                hop(way, dest, i).wait_recv()
                stage[dest, cut, :] = (
                    x_ref[dest, cut, :].astype(F32) + came[dest, cut, :].astype(F32)
                ).astype(BF)

            @pl.when(active & jnp.logical_not(relays))
            def _():
                stage[dest, cut, :] = x_ref[dest, cut, :]

            @pl.when(active)
            def _():
                hop(way, dest, i).start()

    out_ref[...] = x_ref[me].astype(F32)
    for way, came, has in ((0, from_left, has_left), (1, from_right, has_right)):

        @pl.when(has)
        def _():
            for i, cut in enumerate(cuts):
                hop(way, me, i).wait_recv()
                out_ref[cut, :] += came[me, cut, :].astype(F32)

    for way, dest, active, _ in flows:

        @pl.when(active)
        def _():
            for i in range(PIECES):
                hop(way, dest, i).wait_send()

    if swap:
        own_buf[...] = out_ref[...].astype(BF)
        copy = pltpu.make_async_remote_copy(
            src_ref=own_buf,
            dst_ref=peer_buf,
            send_sem=swap_sem.at[0],
            recv_sem=swap_sem.at[1],
            device_id={"dp": peer},
            device_id_type=mesh_id,
        )
        copy.start()
        copy.wait()
        out_ref[...] = own_buf[...].astype(F32) + peer_buf[...].astype(F32)


def scatter_row(value, rows, swap):
    count, wide = value.shape[0] // rows, value.shape[1]
    vmem = pl.BlockSpec(memory_space=pltpu.VMEM)
    return pl.pallas_call(
        functools.partial(scatter_row_kernel, rows, swap),
        name="scatter_row",
        out_shape=jax.ShapeDtypeStruct((count, wide), F32),
        in_specs=[vmem],
        out_specs=vmem,
        scratch_shapes=[pltpu.VMEM((rows, count, wide), BF)] * 4
        + [pltpu.VMEM((count, wide), BF)] * 2
        + [
            pltpu.SemaphoreType.DMA((2, rows, PIECES)),
            pltpu.SemaphoreType.DMA((2, rows, PIECES)),
            pltpu.SemaphoreType.DMA((2,)),
        ],
        compiler_params=comm_params(4),
    )(value.reshape(rows, count, wide))


def comm_params(ident):
    return pltpu.CompilerParams(
        collective_id=ident, has_side_effects=True, vmem_limit_bytes=32 << 20
    )


def comm_sems(kinds):
    return [pltpu.SemaphoreType.DMA((kinds, PIECES)), pltpu.SemaphoreType.DMA((kinds, PIECES))]


def gather_col(value, ident):
    count, wide = value.shape
    vmem = pl.BlockSpec(memory_space=pltpu.VMEM)
    return pl.pallas_call(
        gather_kernel,
        name="gather_col",
        out_shape=jax.ShapeDtypeStruct((4, count, wide), BF),
        in_specs=[vmem],
        out_specs=vmem,
        scratch_shapes=comm_sems(3),
        compiler_params=comm_params(ident),
    )(value)


def scatter_col(value):
    count, wide = value.shape[0] // 4, value.shape[1]
    vmem = pl.BlockSpec(memory_space=pltpu.VMEM)
    return pl.pallas_call(
        scatter_kernel,
        name="scatter_col",
        out_shape=jax.ShapeDtypeStruct((count, wide), F32),
        in_specs=[vmem],
        out_specs=vmem,
        scratch_shapes=[
            pltpu.VMEM((2, count, wide), BF),
            pltpu.VMEM((count, wide), BF),
            pltpu.VMEM((count, wide), BF),
        ]
        + comm_sems(3),
        compiler_params=comm_params(2),
    )(value.reshape(4, count, wide))


def norm(resid, gain, bias):
    mean = jnp.mean(resid, axis=1, keepdims=True)
    var = jnp.mean(resid * resid, axis=1, keepdims=True) - mean * mean
    rstd = lax.rsqrt(var + EPS)
    normed = (resid - mean) * rstd
    return normed * gain + bias, normed, rstd


def norm_grad(grad, normed, rstd, gain):
    scaled = grad * gain
    first = jnp.mean(scaled, axis=1, keepdims=True)
    second = jnp.mean(scaled * normed, axis=1, keepdims=True)
    return rstd * (scaled - first - normed * second)


def gelu(value):
    return jax.nn.gelu(value, approximate=True)


def on_device(
    inputs, w_query, w_key, w_value, w_out, w_up, w_down,
    ln1_gain, ln1_bias, ln2_gain, ln2_bias, segment_ids, pad_mask, rand_blocks, grad_out,
):
    rows, cols = lax.axis_size("row"), lax.axis_size("col")
    row, col = lax.axis_index("row"), lax.axis_index("col")
    feat, local = inputs.shape
    model = feat * rows
    hid = model // cols
    heads = hid // HW
    length = local * cols
    nb = length // BLOCK
    span = local // rows
    per = span // BLOCK
    dims = (heads, nb, per, rows)
    own = cols * span

    blk_q = w_query.reshape(feat, hid)
    blk_k = w_key.reshape(feat, hid)
    blk_v = w_value.reshape(feat, hid)
    blk_o = w_out.reshape(hid, feat)
    params = jnp.stack([ln1_gain, ln1_bias, ln2_gain, ln2_bias], axis=1)
    high = params.astype(BF)
    rest = params - high.astype(F32)
    middle = rest.astype(BF)
    low = (rest - middle.astype(F32)).astype(BF)
    w_qkv = jnp.concatenate([blk_q, blk_k, blk_v, high, middle, low], axis=1)
    w_own = lax.all_gather(w_qkv, "row", axis=0, tiled=True)
    x_parts = lax.all_gather(inputs, ("row", "col"), axis=0)
    w_rest = jnp.concatenate([w_up, w_down, blk_o.T], axis=1)
    x_parts, w_rest, grad_out = lax.optimization_barrier((x_parts, w_rest, grad_out))
    x_parts = x_parts.reshape(rows, cols, feat, local)
    w_rest = lax.all_gather(w_rest, "row", axis=0, tiled=True)
    ff = w_up.shape[1]
    up, down, w_o = w_rest[:, :ff], w_rest[:, ff : 2 * ff], w_rest[:, 2 * ff :]
    gains = w_own[:, 3 * hid :].astype(F32)
    gains = (gains[:, :4] + gains[:, 4:8]) + gains[:, 8:12]
    gains = gains.T.reshape(4, 1, model)
    w_own = w_own[:, : 3 * hid]
    grad_rows = lax.all_to_all(grad_out, "row", 1, 0, tiled=True).T.astype(F32)

    w_heads = w_own.reshape(model, 3, heads, HW)
    w_kv = jnp.concatenate([w_heads[:, 1], w_heads[:, 2]], axis=2).reshape(model, heads * LANES)
    w_q = jnp.pad(w_heads[:, 0], ((0, 0), (0, 0), (0, HW))).reshape(model, heads * LANES)
    row_arr = jnp.reshape(row, (1,)).astype(jnp.int32)
    q, kv, x_own, q_mask, k_mask = project(
        row_arr, x_parts, w_q, w_kv, span, segment_ids, pad_mask
    )
    x_res = lax.dynamic_slice_in_dim(x_own, col * span, span, axis=1).T.astype(F32)

    rand = rand_blocks.reshape(-1)
    o_wide, lse = attention_forward(dims, row_arr, rand, q, q_mask, kv, k_mask)
    o = o_wide.reshape(own, heads, 2, HW)[:, :, 1].reshape(own, hid)
    attn = scatter_col(mm_nt(o, w_o).astype(BF))

    gain1, bias1, gain2, bias2 = gains[0], gains[1], gains[2], gains[3]
    hidden, normed1, rstd1 = norm(x_res + attn, gain1, bias1)
    hidden_all = gather_col(hidden.astype(BF), 1).reshape(own, model)
    up_val = mm(hidden_all, up)
    act, gelu_back = jax.vjp(gelu, up_val)
    act = act.astype(BF)
    ffn = scatter_col(mm_nt(act, down).astype(BF))
    result, normed2, rstd2 = norm(hidden + ffn, gain2, bias2)
    output = lax.all_to_all(result.T.astype(BF), "row", 0, 1, tiled=True)

    grad2 = norm_grad(grad_rows, normed2, rstd2, gain2)
    df = gather_col(grad2.astype(BF), 1).reshape(own, model)
    g_down = mm_tn(df, act).astype(BF)
    du = gelu_back(mm(df, down))[0].astype(BF)
    g_up = mm_tn(hidden_all, du).astype(BF)
    g_ffn = jnp.concatenate(
        [g_up.reshape(rows, feat, ff), g_down.reshape(rows, feat, ff)], axis=1
    ).reshape(2 * model, ff)
    du, g_ffn = lax.optimization_barrier((du, g_ffn))
    g_ffn = lax.psum_scatter(g_ffn, "row", scatter_dimension=0, tiled=True)
    dh = scatter_col(mm_nt(du, up).astype(BF))
    dh = dh + grad2
    grad1 = norm_grad(dh, normed1, rstd1, gain1)
    sums = jnp.stack(
        [
            jnp.sum(dh * normed1, axis=0),
            jnp.sum(dh, axis=0),
            jnp.sum(grad_rows * normed2, axis=0),
            jnp.sum(grad_rows, axis=0),
        ]
    )
    extra = jnp.pad(sums, ((0, 28), (0, 0))).astype(BF)
    dattn = gather_col(jnp.concatenate([grad1.astype(BF), extra], axis=0), 3)
    sums = jnp.sum(dattn[:, span : span + 4].astype(F32), axis=0)
    dattn = dattn[:, :span].reshape(own, model)
    g_out = mm_tn(dattn, o).astype(BF)
    d_o = mm(dattn, w_o).astype(BF)
    d_o = jnp.pad(d_o.reshape(own, heads, HW), ((0, 0), (0, 0), (HW, 0))).reshape(own, -1)

    g_rest = jnp.concatenate([g_out, sums.T.astype(BF)], axis=1)

    dq, dkv = attention_backward(dims, row_arr, rand, q, q_mask, kv, k_mask, d_o, lse)
    dkv = lax.psum_scatter(dkv, "row", scatter_dimension=0, tiled=True)
    dkv, g_ffn, g_rest = lax.optimization_barrier((dkv, g_ffn, g_rest))
    g_rest = lax.psum_scatter(g_rest, "row", scatter_dimension=0, tiled=True)
    g_ffn, g_rest = lax.psum((g_ffn, g_rest), "dp")
    g_ffn, g_rest = g_ffn.astype(F32), g_rest.astype(F32)
    g_sums = g_rest[:, hid:].T
    dq = dq.reshape(own, heads, 2, HW)[:, :, 0].reshape(own, hid)
    dkv = dkv.reshape(own, heads, 2, HW)
    dqkv = jnp.concatenate(
        [dq, dkv[:, :, 0].reshape(own, hid), dkv[:, :, 1].reshape(own, hid)], axis=1
    )
    g_qkv = mm(x_own, dqkv).astype(BF)
    swap = lax.axis_size("dp") == 2
    g_qkv = scatter_row(g_qkv, rows, swap)
    if not swap:
        g_qkv = lax.psum(g_qkv.astype(BF), "dp").astype(F32)
    grad_in = scatter_col(mm_nt(dqkv, w_own).astype(BF)) + grad1
    grad_in = lax.all_to_all(grad_in.T.astype(BF), "row", 0, 1, tiled=True).astype(F32)

    return (
        output,
        grad_in,
        g_qkv[:, :hid].reshape(1, 1, -1),
        g_qkv[:, hid : 2 * hid].reshape(1, 1, -1),
        g_qkv[:, 2 * hid :].reshape(1, 1, -1),
        g_rest[:, :hid].T.reshape(1, 1, -1),
        g_ffn[:feat],
        g_ffn[feat:],
        g_sums[0],
        g_sums[1],
        g_sums[2],
        g_sums[3],
    )


def solution(mesh):
    tokens = P("row", ("dp", "col"))
    grid = P("row", "col", None)
    return jax.shard_map(
        on_device,
        mesh=mesh,
        in_specs=(
            tokens,
            grid,
            grid,
            grid,
            P("col", "row", None),
            P("row", "col"),
            P("row", "col"),
            P("row"),
            P("row"),
            P("row"),
            P("row"),
            P("dp"),
            P("dp"),
            P("dp", "col", None, None),
            tokens,
        ),
        out_specs=(
            tokens,
            tokens,
            grid,
            grid,
            grid,
            P("col", "row", None),
            P("row", "col"),
            P("row", "col"),
            P("row"),
            P("row"),
            P("row"),
            P("row"),
        ),
        check_vma=False,
    )
```

```python
import functools

import jax
import jax.numpy as jnp
from jax import lax
from jax.experimental import pallas as pl
from jax.experimental.pallas import tpu as pltpu
from jax.sharding import PartitionSpec as P


BLOCK = 64
HW = 64
LANES = 128
NEG = -1000000000.0
EPS = 1e-06
BF = jnp.bfloat16
F32 = jnp.float32


def mm(left, right):
    return lax.dot_general(left, right, (((1,), (0,)), ((), ())), preferred_element_type=F32)


def mm_nt(left, right):
    return lax.dot_general(left, right, (((1,), (1,)), ((), ())), preferred_element_type=F32)


def mm_tn(left, right):
    return lax.dot_general(left, right, (((0,), (0,)), ((), ())), preferred_element_type=F32)


def block_of(j, row, per, rows):
    return (j // per) * (per * rows) + row * per + j % per


def rows_at(ref, block, head):
    start = pl.multiple_of(block * BLOCK, BLOCK)
    return ref[pl.ds(start, BLOCK), head * LANES : (head + 1) * LANES]


def sparse_lists(rand_ref, head, pos, nb):
    before = jnp.maximum(pos - 1, 0)
    after = jnp.minimum(pos + 1, nb - 1)
    picks = [rand_ref[(head * nb + pos) * 3 + i] for i in range(3)]
    return [0, nb - 1, before, pos, after] + picks


def dense_list(group):
    return [group * 8 + i for i in range(8)]


def sparse_bar(pos, nb):
    entry = lax.broadcasted_iota(jnp.int32, (1, 8 * BLOCK), 1) // BLOCK
    no_before = jnp.where(pos < 2, 8.0, 0.0)
    no_after = jnp.where(pos > nb - 3, 8.0, 0.0)
    return 0.5 + jnp.where(entry == 2, no_before, 0.0) + jnp.where(entry == 4, no_after, 0.0)


def gather(ref, blocks, head):
    return jnp.concatenate([rows_at(ref, b, head) for b in blocks], axis=0)


def scores_of(query, query_mask, keys, key_mask, own, bar):
    shape = (query.shape[0], keys.shape[0])
    apart = lax.broadcasted_iota(jnp.int32, shape, 1) - lax.broadcasted_iota(jnp.int32, shape, 0)
    allowed = (mm_nt(query_mask, key_mask) > bar) | (apart == own * BLOCK)
    return jnp.where(allowed, mm_nt(query, keys), NEG)


def forward_kernel(heads, nb, per, rows, row_ref, rand_ref, q_ref, qm_ref, kv_ref, km_ref, o_ref, lse_ref):
    row = row_ref[0]

    def place(j, head):
        start = pl.multiple_of(j * BLOCK, BLOCK)
        return pl.ds(start, BLOCK), slice(head * LANES, (head + 1) * LANES)

    def step(j, carry):
        pos = block_of(j, row, per, rows)
        is_global = (pos == 0) | (pos == nb - 1)
        query_mask = qm_ref[pl.ds(pl.multiple_of(j * BLOCK, BLOCK), BLOCK), :]

        @pl.when(jnp.logical_not(is_global))
        def _():
            for head in range(heads):
                at = place(j, head)
                blocks = sparse_lists(rand_ref, head, pos, nb)
                keys = gather(kv_ref, blocks, head)
                score = scores_of(
                    q_ref[at], query_mask, keys, gather(km_ref, blocks, 0), 3, sparse_bar(pos, nb)
                )
                top = jnp.max(score, axis=1, keepdims=True)
                weight = jnp.exp(score - top)
                total = jnp.sum(weight, axis=1, keepdims=True)
                probs = (weight * (1.0 / total)).astype(BF)
                o_ref[at] = mm(probs, keys).astype(BF)
                lse_ref[at] = jnp.broadcast_to(top + jnp.log(total), (BLOCK, LANES))

        @pl.when(is_global)
        def _():
            def score_at(group, head):
                blocks = dense_list(group)
                keys = gather(kv_ref, blocks, head)
                score = scores_of(
                    q_ref[place(j, head)], query_mask, keys, gather(km_ref, blocks, 0),
                    pos - group * 8, 0.5,
                )
                return score, keys

            def stats(group, kept):
                new = []
                for head in range(heads):
                    top, total = kept[head]
                    score, _ = score_at(group, head)
                    above = jnp.maximum(top, jnp.max(score, axis=1, keepdims=True))
                    total = total * jnp.exp(top - above) + jnp.sum(
                        jnp.exp(score - above), axis=1, keepdims=True
                    )
                    new.append((above, total))
                return tuple(new)

            first = tuple(
                (jnp.full((BLOCK, 1), 2 * NEG, F32), jnp.zeros((BLOCK, 1), F32))
                for _ in range(heads)
            )
            found = lax.fori_loop(0, nb // 8, stats, first)
            lses = [top + jnp.log(total) for top, total in found]

            def outs(group, kept):
                new = []
                for head in range(heads):
                    score, keys = score_at(group, head)
                    new.append(kept[head] + mm(jnp.exp(score - lses[head]).astype(BF), keys))
                return tuple(new)

            done = lax.fori_loop(
                0, nb // 8, outs, tuple(jnp.zeros((BLOCK, LANES), F32) for _ in range(heads))
            )
            for head in range(heads):
                at = place(j, head)
                o_ref[at] = done[head].astype(BF)
                lse_ref[at] = jnp.broadcast_to(lses[head], (BLOCK, LANES))

        return carry

    lax.fori_loop(0, q_ref.shape[0] // BLOCK, step, 0)


def backward_kernel(
    heads, nb, per, rows, row_ref, rand_ref, q_ref, qm_ref, kv_ref, km_ref, do_ref, lse_ref,
    dq_ref, dkv_ref, acc_ref,
):
    row = row_ref[0]
    acc_ref[...] = jnp.zeros_like(acc_ref)

    def place(j, head):
        start = pl.multiple_of(j * BLOCK, BLOCK)
        return pl.ds(start, BLOCK), slice(head * LANES, (head + 1) * LANES)

    def parts(j, head, query_mask, blocks, mine, bar):
        at = place(j, head)
        keys = gather(kv_ref, blocks, head)
        score = scores_of(q_ref[at], query_mask, keys, gather(km_ref, blocks, 0), mine, bar)
        lse = lse_ref[at][:, :1]
        probs = jnp.exp(score - lse)
        return keys, probs, mm_nt(do_ref[at], keys)

    def finish(j, head, blocks, keys, probs, grad_probs, dot_row):
        at = place(j, head)
        low = (probs * (grad_probs - dot_row)).astype(BF)
        both = jnp.concatenate([low, probs.astype(BF)], axis=0)
        sides = jnp.concatenate([q_ref[at], do_ref[at]], axis=0)
        grad = mm_tn(both, sides)
        for i, block in enumerate(blocks):
            start = pl.multiple_of(block * BLOCK, BLOCK)
            acc_ref[pl.ds(start, BLOCK), at[1]] += grad[i * BLOCK : (i + 1) * BLOCK, :]
        return mm(low, keys)

    def step(j, carry):
        pos = block_of(j, row, per, rows)
        is_global = (pos == 0) | (pos == nb - 1)
        query_mask = qm_ref[pl.ds(pl.multiple_of(j * BLOCK, BLOCK), BLOCK), :]

        @pl.when(jnp.logical_not(is_global))
        def _():
            for head in range(heads):
                blocks = sparse_lists(rand_ref, head, pos, nb)
                keys, probs, grad_probs = parts(
                    j, head, query_mask, blocks, 3, sparse_bar(pos, nb)
                )
                dot_row = jnp.sum(probs * grad_probs, axis=1, keepdims=True)
                grad_q = finish(j, head, blocks, keys, probs, grad_probs, dot_row)
                dq_ref[place(j, head)] = (grad_q * 0.125).astype(BF)

        @pl.when(is_global)
        def _():
            def dots(group, kept):
                blocks = dense_list(group)
                mine = pos - group * 8
                new = []
                for head in range(heads):
                    _, probs, grad_probs = parts(j, head, query_mask, blocks, mine, 0.5)
                    new.append(kept[head] + jnp.sum(probs * grad_probs, axis=1, keepdims=True))
                return tuple(new)

            dot_rows = lax.fori_loop(
                0, nb // 8, dots, tuple(jnp.zeros((BLOCK, 1), F32) for _ in range(heads))
            )

            def grads(group, kept):
                blocks = dense_list(group)
                mine = pos - group * 8
                new = []
                for head in range(heads):
                    keys, probs, grad_probs = parts(j, head, query_mask, blocks, mine, 0.5)
                    new.append(
                        kept[head]
                        + finish(j, head, blocks, keys, probs, grad_probs, dot_rows[head])
                    )
                return tuple(new)

            done = lax.fori_loop(
                0, nb // 8, grads, tuple(jnp.zeros((BLOCK, LANES), F32) for _ in range(heads))
            )
            for head in range(heads):
                dq_ref[place(j, head)] = (done[head] * 0.125).astype(BF)

        return carry

    lax.fori_loop(0, q_ref.shape[0] // BLOCK, step, 0)
    span = per * BLOCK

    def out(i, carry):
        source = (i % rows) * (rows * span) + (i // rows) * span
        dkv_ref[pl.ds(pl.multiple_of(i * span, span), span), :] = acc_ref[
            pl.ds(pl.multiple_of(source, span), span), :
        ].astype(BF)
        return carry

    lax.fori_loop(0, kv_ref.shape[0] // span, out, 0)


def specs(count):
    return [pl.BlockSpec(memory_space=pltpu.SMEM)] * 2 + [
        pl.BlockSpec(memory_space=pltpu.VMEM)
    ] * count


def attention_forward(dims, row, rand, q, q_mask, kv, k_mask):
    own, wide = q.shape
    vmem = pl.BlockSpec(memory_space=pltpu.VMEM)
    return pl.pallas_call(
        functools.partial(forward_kernel, *dims),
        name="attn_fwd",
        out_shape=(
            jax.ShapeDtypeStruct((own, wide), BF),
            jax.ShapeDtypeStruct((own, wide), F32),
        ),
        in_specs=specs(4),
        out_specs=(vmem, vmem),
        cost_estimate=pl.CostEstimate(
            flops=own * 512 * wide * 6, bytes_accessed=12 << 20, transcendentals=own * 512 * 3
        ),
        compiler_params=pltpu.CompilerParams(vmem_limit_bytes=48 << 20),
    )(row, rand, q, q_mask, kv, k_mask)


def attention_backward(dims, row, rand, q, q_mask, kv, k_mask, d_o, lse):
    own, wide = q.shape
    vmem = pl.BlockSpec(memory_space=pltpu.VMEM)
    return pl.pallas_call(
        functools.partial(backward_kernel, *dims),
        name="attn_bwd",
        out_shape=(
            jax.ShapeDtypeStruct((own, wide), BF),
            jax.ShapeDtypeStruct(kv.shape, BF),
        ),
        in_specs=specs(6),
        out_specs=(vmem, vmem),
        scratch_shapes=[pltpu.VMEM(kv.shape, F32)],
        cost_estimate=pl.CostEstimate(
            flops=own * 512 * wide * 12, bytes_accessed=20 << 20, transcendentals=own * 512 * 3
        ),
        compiler_params=pltpu.CompilerParams(vmem_limit_bytes=48 << 20),
    )(row, rand, q, q_mask, kv, k_mask, d_o, lse)


def one_hot_rows(hot):
    kinds = hot.shape[0]
    shape = (kinds, LANES)
    eye = lax.broadcasted_iota(jnp.int32, shape, 0) == lax.broadcasted_iota(jnp.int32, shape, 1)
    return mm_tn(jnp.where(hot, 1.0, 0.0).astype(BF), jnp.where(eye, 1.0, 0.0).astype(BF)).astype(BF)


def project_kernel(
    rows, span, row_ref, x_ref, wq_ref, wkv_ref, seg_ref, pad_ref,
    q_ref, kv_ref, own_ref, qm_ref, km_ref,
):
    feat = x_ref.shape[2]
    start = pl.multiple_of(row_ref[0] * span, span)
    kv = q = None
    for part in range(rows):
        at = slice(part * feat, (part + 1) * feat)
        mine = x_ref[part, 0, :, pl.ds(start, span)]
        own_ref[at, :] = mine
        kv_part = mm_tn(x_ref[part, 0], wkv_ref[at, :])
        q_part = mm_tn(mine, wq_ref[at, :])
        kv = kv_part if kv is None else kv + kv_part
        q = q_part if q is None else q + q_part
    kv_ref[...] = kv.astype(BF)
    q_ref[...] = (q.astype(BF) * 0.125).astype(BF)
    segs = seg_ref[...]
    kinds = lax.broadcasted_iota(jnp.int32, (BLOCK, segs.shape[1]), 0)
    km_ref[...] = one_hot_rows((kinds == segs) & (pad_ref[...] == 1))
    mine = seg_ref[:, pl.ds(start, span)]
    kinds = lax.broadcasted_iota(jnp.int32, (BLOCK, span), 0)
    qm_ref[...] = one_hot_rows(kinds == mine)


def project(row, x_parts, w_q, w_kv, span, segs, pads):
    rows, cols, feat, local = x_parts.shape
    model, wide = w_q.shape
    return pl.pallas_call(
        functools.partial(project_kernel, rows, span),
        name="project",
        grid=(cols,),
        out_shape=(
            jax.ShapeDtypeStruct((cols * span, wide), BF),
            jax.ShapeDtypeStruct((cols * local, wide), BF),
            jax.ShapeDtypeStruct((model, cols * span), BF),
            jax.ShapeDtypeStruct((cols * span, LANES), BF),
            jax.ShapeDtypeStruct((cols * local, LANES), BF),
        ),
        in_specs=[
            pl.BlockSpec(memory_space=pltpu.SMEM),
            pl.BlockSpec((rows, 1, feat, local), lambda c: (0, c, 0, 0)),
            pl.BlockSpec((model, wide), lambda c: (0, 0)),
            pl.BlockSpec((model, wide), lambda c: (0, 0)),
            pl.BlockSpec((1, local), lambda c: (0, c)),
            pl.BlockSpec((1, local), lambda c: (0, c)),
        ],
        out_specs=(
            pl.BlockSpec((span, wide), lambda c: (c, 0)),
            pl.BlockSpec((local, wide), lambda c: (c, 0)),
            pl.BlockSpec((model, span), lambda c: (0, c)),
            pl.BlockSpec((span, LANES), lambda c: (c, 0)),
            pl.BlockSpec((local, LANES), lambda c: (c, 0)),
        ),
        cost_estimate=pl.CostEstimate(
            flops=cols * local * model * wide * 3, bytes_accessed=16 << 20, transcendentals=0
        ),
        compiler_params=pltpu.CompilerParams(vmem_limit_bytes=48 << 20),
    )(row, x_parts, w_q, w_kv, segs.reshape(1, -1), pads.reshape(1, -1))


PIECES = 2


def col_places():
    me = lax.axis_index("col")
    partner = me + 1 - 2 * lax.rem(me, 2)
    cross = lax.rem(me + 2, 4)
    diag = lax.rem(partner + 2, 4)
    barrier = pltpu.get_barrier_semaphore()
    for peer in (partner, cross):
        pl.semaphore_signal(
            barrier, inc=1, device_id={"col": peer}, device_id_type=pl.DeviceIdType.MESH
        )
    pl.semaphore_wait(barrier, 2)
    return me, partner, cross, diag


def send_to(source, target, sems, kind, piece, peer):
    copy = pltpu.make_async_remote_copy(
        src_ref=source,
        dst_ref=target,
        send_sem=sems[0].at[kind, piece],
        recv_sem=sems[1].at[kind, piece],
        device_id={"col": peer},
        device_id_type=pl.DeviceIdType.MESH,
    )
    copy.start()
    return copy


def gather_kernel(x_ref, out_ref, send_sem, recv_sem):
    me, partner, cross, _ = col_places()
    sems = (send_sem, recv_sem)
    size = x_ref.shape[0] // PIECES
    cuts = [pl.ds(i * size, size) for i in range(PIECES)]
    over = [
        send_to(x_ref.at[cut], out_ref.at[me, cut], sems, 0, i, cross)
        for i, cut in enumerate(cuts)
    ]
    near = [
        send_to(x_ref.at[cut], out_ref.at[me, cut], sems, 1, i, partner)
        for i, cut in enumerate(cuts)
    ]
    out_ref[me] = x_ref[...]
    relay = []
    for i, cut in enumerate(cuts):
        over[i].wait_recv()
        relay.append(
            send_to(out_ref.at[cross, cut], out_ref.at[cross, cut], sems, 2, i, partner)
        )
    for i in range(PIECES):
        over[i].wait_send()
        near[i].wait()
        relay[i].wait()


def scatter_kernel(x_ref, out_ref, near_buf, sum_buf, over_buf, send_sem, recv_sem):
    me, partner, cross, diag = col_places()
    sems = (send_sem, recv_sem)
    size = x_ref.shape[1] // PIECES
    cuts = [pl.ds(i * size, size) for i in range(PIECES)]
    first = [
        send_to(x_ref.at[diag, cut], near_buf.at[1, cut], sems, 0, i, partner)
        for i, cut in enumerate(cuts)
    ]
    second = [
        send_to(x_ref.at[partner, cut], near_buf.at[0, cut], sems, 1, i, partner)
        for i, cut in enumerate(cuts)
    ]
    over = []
    for i, cut in enumerate(cuts):
        first[i].wait_recv()
        sum_buf[cut, :] = (
            x_ref[cross, cut, :].astype(F32) + near_buf[1, cut, :].astype(F32)
        ).astype(BF)
        over.append(send_to(sum_buf.at[cut], over_buf.at[cut], sems, 2, i, cross))
    for i, cut in enumerate(cuts):
        second[i].wait_recv()
        out_ref[cut, :] = x_ref[me, cut, :].astype(F32) + near_buf[0, cut, :].astype(F32)
    for i, cut in enumerate(cuts):
        over[i].wait_recv()
        out_ref[cut, :] += over_buf[cut, :].astype(F32)
    for i in range(PIECES):
        first[i].wait_send()
        second[i].wait_send()
        over[i].wait_send()


def scatter_row_kernel(
    rows, swap, x_ref, out_ref, from_left, from_right, to_right, to_left, own_buf, peer_buf,
    send_sem, recv_sem, swap_sem,
):
    me = lax.axis_index("row")
    right, left = lax.rem(me + 1, rows), lax.rem(me + rows - 1, rows)
    has_left, has_right = me > 0, me < rows - 1
    mesh_id = pl.DeviceIdType.MESH
    barrier = pltpu.get_barrier_semaphore()

    @pl.when(has_left)
    def _():
        pl.semaphore_signal(barrier, inc=1, device_id={"row": left}, device_id_type=mesh_id)

    @pl.when(has_right)
    def _():
        pl.semaphore_signal(barrier, inc=1, device_id={"row": right}, device_id_type=mesh_id)

    if swap:
        peer = 1 - lax.axis_index("dp")
        pl.semaphore_signal(barrier, inc=1, device_id={"dp": peer}, device_id_type=mesh_id)

    peers = jnp.where(has_left, 1, 0) + jnp.where(has_right, 1, 0) + (1 if swap else 0)
    pl.semaphore_wait(barrier, peers)

    size = x_ref.shape[1] // PIECES
    cuts = [pl.ds(i * size, size) for i in range(PIECES)]

    def hop(way, dest, i):
        stage, target, to = ((to_right, from_left, right), (to_left, from_right, left))[way]
        return pltpu.make_async_remote_copy(
            src_ref=stage.at[dest, cuts[i]],
            dst_ref=target.at[dest, cuts[i]],
            send_sem=send_sem.at[way, dest, i],
            recv_sem=recv_sem.at[way, dest, i],
            device_id={"row": to},
            device_id_type=mesh_id,
        )

    flows = []
    for step in range(rows - 1):
        flows.append((0, rows - 1 - step, me < rows - 1 - step, has_left))
        flows.append((1, step, me > step, has_right))
    for way, dest, active, relays in flows:
        stage, came = ((to_right, from_left), (to_left, from_right))[way]
        for i, cut in enumerate(cuts):

            @pl.when(active & relays)
            def _():
                hop(way, dest, i).wait_recv()
                stage[dest, cut, :] = (
                    x_ref[dest, cut, :].astype(F32) + came[dest, cut, :].astype(F32)
                ).astype(BF)

            @pl.when(active & jnp.logical_not(relays))
            def _():
                stage[dest, cut, :] = x_ref[dest, cut, :]

            @pl.when(active)
            def _():
                hop(way, dest, i).start()

    out_ref[...] = x_ref[me].astype(F32)
    for way, came, has in ((0, from_left, has_left), (1, from_right, has_right)):

        @pl.when(has)
        def _():
            for i, cut in enumerate(cuts):
                hop(way, me, i).wait_recv()
                out_ref[cut, :] += came[me, cut, :].astype(F32)

    for way, dest, active, _ in flows:

        @pl.when(active)
        def _():
            for i in range(PIECES):
                hop(way, dest, i).wait_send()

    if swap:
        own_buf[...] = out_ref[...].astype(BF)
        copy = pltpu.make_async_remote_copy(
            src_ref=own_buf,
            dst_ref=peer_buf,
            send_sem=swap_sem.at[0],
            recv_sem=swap_sem.at[1],
            device_id={"dp": peer},
            device_id_type=mesh_id,
        )
        copy.start()
        copy.wait()
        out_ref[...] = own_buf[...].astype(F32) + peer_buf[...].astype(F32)


def scatter_row(value, rows, swap):
    count, wide = value.shape[0] // rows, value.shape[1]
    vmem = pl.BlockSpec(memory_space=pltpu.VMEM)
    return pl.pallas_call(
        functools.partial(scatter_row_kernel, rows, swap),
        name="scatter_row",
        out_shape=jax.ShapeDtypeStruct((count, wide), F32),
        in_specs=[vmem],
        out_specs=vmem,
        scratch_shapes=[pltpu.VMEM((rows, count, wide), BF)] * 4
        + [pltpu.VMEM((count, wide), BF)] * 2
        + [
            pltpu.SemaphoreType.DMA((2, rows, PIECES)),
            pltpu.SemaphoreType.DMA((2, rows, PIECES)),
            pltpu.SemaphoreType.DMA((2,)),
        ],
        compiler_params=comm_params(4),
    )(value.reshape(rows, count, wide))


def gather_in_kernel(rows, x_ref, w_ref, xs_ref, ws_ref, send_x, recv_x, send_w, recv_w):
    me, col = lax.axis_index("row"), lax.axis_index("col")
    right, left = lax.rem(me + 1, rows), lax.rem(me + rows - 1, rows)
    has_left, has_right = me > 0, me < rows - 1
    partner = col + 1 - 2 * lax.rem(col, 2)
    cross = lax.rem(col + 2, 4)
    diag = lax.rem(partner + 2, 4)
    mesh_id = pl.DeviceIdType.MESH
    barrier = pltpu.get_barrier_semaphore()

    @pl.when(has_left)
    def _():
        pl.semaphore_signal(barrier, inc=1, device_id={"row": left}, device_id_type=mesh_id)

    @pl.when(has_right)
    def _():
        pl.semaphore_signal(barrier, inc=1, device_id={"row": right}, device_id_type=mesh_id)

    for peer in (partner, cross):
        pl.semaphore_signal(barrier, inc=1, device_id={"col": peer}, device_id_type=mesh_id)
    pl.semaphore_wait(barrier, jnp.where(has_left, 1, 0) + jnp.where(has_right, 1, 0) + 2)

    def copy_x(source, kind, shard, slot, where):
        return pltpu.make_async_remote_copy(
            src_ref=source,
            dst_ref=xs_ref.at[shard, slot],
            send_sem=send_x.at[kind, shard],
            recv_sem=recv_x.at[kind, shard],
            device_id=where,
            device_id_type=mesh_id,
        )

    def copy_w(source, kind, shard, where):
        return pltpu.make_async_remote_copy(
            src_ref=source,
            dst_ref=ws_ref.at[shard],
            send_sem=send_w.at[kind, shard],
            recv_sem=recv_w.at[kind, shard],
            device_id=where,
            device_id_type=mesh_id,
        )

    to_right, to_left = {"row": right}, {"row": left}
    ways = ((0, has_right, to_right), (1, has_left, to_left))

    for kind, onward, where in ways:

        @pl.when(onward)
        def _():
            copy_x(x_ref, kind, me, col, where).start()

    copy_x(x_ref, 2, me, col, {"col": cross}).start()
    copy_x(x_ref, 3, me, col, {"col": partner}).start()
    for kind, onward, where in ways:

        @pl.when(onward)
        def _():
            copy_w(w_ref, kind, me, where).start()

    xs_ref[me, col] = x_ref[...]
    ws_ref[me] = w_ref[...]

    def relay(shard):
        copy_x(x_ref, 2, shard, cross, {"col": cross}).wait_recv()
        source = xs_ref.at[shard, cross]
        copy_x(source, 4, shard, cross, {"col": partner}).start()

    def shards_at(step):
        return (
            (0, me - step, me >= step, has_right, to_right),
            (1, me + step, me + step <= rows - 1, has_left, to_left),
        )

    for step in range(1, rows):
        for kind, shard, exists, onward, where in shards_at(step):

            @pl.when(exists)
            def _():
                copy_x(x_ref, kind, shard, col, where).wait_recv()

                @pl.when(onward)
                def _():
                    copy_x(xs_ref.at[shard, col], kind, shard, col, where).start()

                copy_x(xs_ref.at[shard, col], 2, shard, col, {"col": cross}).start()
                copy_x(xs_ref.at[shard, col], 3, shard, col, {"col": partner}).start()

        for kind, shard, exists, onward, where in shards_at(step):

            @pl.when(exists)
            def _():
                copy_w(w_ref, kind, shard, where).wait_recv()

                @pl.when(onward)
                def _():
                    copy_w(ws_ref.at[shard], kind, shard, where).start()

        if step == 1:
            relay(me)
        else:
            for _, shard, exists, _, _ in shards_at(step - 1):

                @pl.when(exists)
                def _():
                    relay(shard)

    for _, shard, exists, _, _ in shards_at(rows - 1):

        @pl.when(exists)
        def _():
            relay(shard)

    for shard in range(rows):
        copy_x(x_ref, 3, shard, partner, {"col": partner}).wait_recv()
        copy_x(x_ref, 4, shard, diag, {"col": partner}).wait_recv()
        for kind in (2, 3, 4):
            copy_x(x_ref, kind, shard, col, {"col": partner}).wait_send()
        for kind, sent, where in (
            (0, has_right & (me >= shard), to_right),
            (1, has_left & (me <= shard), to_left),
        ):

            @pl.when(sent)
            def _():
                copy_x(x_ref, kind, shard, col, where).wait_send()
                copy_w(w_ref, kind, shard, where).wait_send()


def gather_in(x, w, rows):
    vmem = pl.BlockSpec(memory_space=pltpu.VMEM)
    sems = pltpu.SemaphoreType.DMA
    return pl.pallas_call(
        functools.partial(gather_in_kernel, rows),
        name="gather_in",
        out_shape=(
            jax.ShapeDtypeStruct((rows, 4) + x.shape, BF),
            jax.ShapeDtypeStruct((rows,) + w.shape, BF),
        ),
        in_specs=[vmem, vmem],
        out_specs=(vmem, vmem),
        scratch_shapes=[sems((5, rows)), sems((5, rows)), sems((2, rows)), sems((2, rows))],
        compiler_params=comm_params(5),
    )(x, w)


def comm_params(ident):
    return pltpu.CompilerParams(
        collective_id=ident, has_side_effects=True, vmem_limit_bytes=32 << 20
    )


def comm_sems(kinds):
    return [pltpu.SemaphoreType.DMA((kinds, PIECES)), pltpu.SemaphoreType.DMA((kinds, PIECES))]


def gather_col(value, ident):
    count, wide = value.shape
    vmem = pl.BlockSpec(memory_space=pltpu.VMEM)
    return pl.pallas_call(
        gather_kernel,
        name="gather_col",
        out_shape=jax.ShapeDtypeStruct((4, count, wide), BF),
        in_specs=[vmem],
        out_specs=vmem,
        scratch_shapes=comm_sems(3),
        compiler_params=comm_params(ident),
    )(value)


def scatter_col(value):
    count, wide = value.shape[0] // 4, value.shape[1]
    vmem = pl.BlockSpec(memory_space=pltpu.VMEM)
    return pl.pallas_call(
        scatter_kernel,
        name="scatter_col",
        out_shape=jax.ShapeDtypeStruct((count, wide), F32),
        in_specs=[vmem],
        out_specs=vmem,
        scratch_shapes=[
            pltpu.VMEM((2, count, wide), BF),
            pltpu.VMEM((count, wide), BF),
            pltpu.VMEM((count, wide), BF),
        ]
        + comm_sems(3),
        compiler_params=comm_params(2),
    )(value.reshape(4, count, wide))


def norm(resid, gain, bias):
    mean = jnp.mean(resid, axis=1, keepdims=True)
    var = jnp.mean(resid * resid, axis=1, keepdims=True) - mean * mean
    rstd = lax.rsqrt(var + EPS)
    normed = (resid - mean) * rstd
    return normed * gain + bias, normed, rstd


def norm_grad(grad, normed, rstd, gain):
    scaled = grad * gain
    first = jnp.mean(scaled, axis=1, keepdims=True)
    second = jnp.mean(scaled * normed, axis=1, keepdims=True)
    return rstd * (scaled - first - normed * second)


def gelu(value):
    return jax.nn.gelu(value, approximate=True)


def on_device(
    inputs, w_query, w_key, w_value, w_out, w_up, w_down,
    ln1_gain, ln1_bias, ln2_gain, ln2_bias, segment_ids, pad_mask, rand_blocks, grad_out,
):
    rows, cols = lax.axis_size("row"), lax.axis_size("col")
    row, col = lax.axis_index("row"), lax.axis_index("col")
    feat, local = inputs.shape
    model = feat * rows
    hid = model // cols
    heads = hid // HW
    length = local * cols
    nb = length // BLOCK
    span = local // rows
    per = span // BLOCK
    dims = (heads, nb, per, rows)
    own = cols * span

    blk_q = w_query.reshape(feat, hid)
    blk_k = w_key.reshape(feat, hid)
    blk_v = w_value.reshape(feat, hid)
    blk_o = w_out.reshape(hid, feat)
    params = jnp.stack([ln1_gain, ln1_bias, ln2_gain, ln2_bias])
    high = params.astype(BF)
    rest = params - high.astype(F32)
    middle = rest.astype(BF)
    low = (rest - middle.astype(F32)).astype(BF)
    params = jnp.concatenate([high, middle, low], axis=0)
    params = jnp.pad(params, ((0, 4), (0, 4 * hid - feat)))
    w_small = jnp.concatenate([blk_q, blk_k, blk_v, blk_o.T], axis=1)
    w_small = jnp.concatenate([w_small, params], axis=0)
    x_parts, w_small = gather_in(inputs, w_small, rows)
    w_rest = jnp.concatenate([w_up, w_down], axis=1)
    x_parts, w_rest, grad_out = lax.optimization_barrier((x_parts, w_rest, grad_out))
    w_rest = lax.all_gather(w_rest, "row", axis=0, tiled=True)
    ff = w_up.shape[1]
    up, down = w_rest[:, :ff], w_rest[:, ff:]
    gains = w_small[:, feat : feat + 12, :feat].astype(F32).reshape(rows, 3, 4, feat)
    gains = (gains[:, 0] + gains[:, 1]) + gains[:, 2]
    gains = gains.transpose(1, 0, 2).reshape(4, 1, model)
    w_small = w_small[:, :feat].reshape(model, 4 * hid)
    w_own, w_o = w_small[:, : 3 * hid], w_small[:, 3 * hid :]
    grad_rows = lax.all_to_all(grad_out, "row", 1, 0, tiled=True).T.astype(F32)

    w_heads = w_own.reshape(model, 3, heads, HW)
    w_kv = jnp.concatenate([w_heads[:, 1], w_heads[:, 2]], axis=2).reshape(model, heads * LANES)
    w_q = jnp.pad(w_heads[:, 0], ((0, 0), (0, 0), (0, HW))).reshape(model, heads * LANES)
    row_arr = jnp.reshape(row, (1,)).astype(jnp.int32)
    q, kv, x_own, q_mask, k_mask = project(
        row_arr, x_parts, w_q, w_kv, span, segment_ids, pad_mask
    )
    x_res = lax.dynamic_slice_in_dim(x_own, col * span, span, axis=1).T.astype(F32)

    rand = rand_blocks.reshape(-1)
    o_wide, lse = attention_forward(dims, row_arr, rand, q, q_mask, kv, k_mask)
    o = o_wide.reshape(own, heads, 2, HW)[:, :, 1].reshape(own, hid)
    attn = scatter_col(mm_nt(o, w_o).astype(BF))

    gain1, bias1, gain2, bias2 = gains[0], gains[1], gains[2], gains[3]
    hidden, normed1, rstd1 = norm(x_res + attn, gain1, bias1)
    hidden_all = gather_col(hidden.astype(BF), 1).reshape(own, model)
    up_val = mm(hidden_all, up)
    act, gelu_back = jax.vjp(gelu, up_val)
    act = act.astype(BF)
    ffn = scatter_col(mm_nt(act, down).astype(BF))
    result, normed2, rstd2 = norm(hidden + ffn, gain2, bias2)
    output = lax.all_to_all(result.T.astype(BF), "row", 0, 1, tiled=True)

    grad2 = norm_grad(grad_rows, normed2, rstd2, gain2)
    df = gather_col(grad2.astype(BF), 1).reshape(own, model)
    g_down = mm_tn(df, act).astype(BF)
    du = gelu_back(mm(df, down))[0].astype(BF)
    g_up = mm_tn(hidden_all, du).astype(BF)
    g_ffn = jnp.concatenate(
        [g_up.reshape(rows, feat, ff), g_down.reshape(rows, feat, ff)], axis=1
    ).reshape(2 * model, ff)
    du, g_ffn = lax.optimization_barrier((du, g_ffn))
    g_ffn = lax.psum_scatter(g_ffn, "row", scatter_dimension=0, tiled=True)
    dh = scatter_col(mm_nt(du, up).astype(BF))
    dh = dh + grad2
    grad1 = norm_grad(dh, normed1, rstd1, gain1)
    sums = jnp.stack(
        [
            jnp.sum(dh * normed1, axis=0),
            jnp.sum(dh, axis=0),
            jnp.sum(grad_rows * normed2, axis=0),
            jnp.sum(grad_rows, axis=0),
        ]
    )
    extra = jnp.pad(sums, ((0, 28), (0, 0))).astype(BF)
    dattn = gather_col(jnp.concatenate([grad1.astype(BF), extra], axis=0), 3)
    sums = jnp.sum(dattn[:, span : span + 4].astype(F32), axis=0)
    dattn = dattn[:, :span].reshape(own, model)
    g_out = mm_tn(dattn, o).astype(BF)
    d_o = mm(dattn, w_o).astype(BF)
    d_o = jnp.pad(d_o.reshape(own, heads, HW), ((0, 0), (0, 0), (HW, 0))).reshape(own, -1)

    sums = sums.reshape(4, rows, feat).transpose(1, 0, 2).astype(BF)
    sums = jnp.pad(sums, ((0, 0), (0, 12), (0, hid - feat)))
    g_rest = jnp.concatenate([g_out.reshape(rows, feat, hid), sums], axis=1).reshape(-1, hid)
    d_o, g_rest = lax.optimization_barrier((d_o, g_rest))
    g_rest = lax.psum_scatter(g_rest, "row", scatter_dimension=0, tiled=True)
    dq, dkv = attention_backward(dims, row_arr, rand, q, q_mask, kv, k_mask, d_o, lse)
    dkv = lax.psum_scatter(dkv, "row", scatter_dimension=0, tiled=True)
    dkv, g_ffn, g_rest = lax.optimization_barrier((dkv, g_ffn, g_rest))
    g_ffn, g_rest = lax.psum((g_ffn, g_rest), "dp")
    g_ffn, g_rest = g_ffn.astype(F32), g_rest.astype(F32)
    g_sums = g_rest[feat : feat + 4, :feat]
    dq = dq.reshape(own, heads, 2, HW)[:, :, 0].reshape(own, hid)
    dkv = dkv.reshape(own, heads, 2, HW)
    dqkv = jnp.concatenate(
        [dq, dkv[:, :, 0].reshape(own, hid), dkv[:, :, 1].reshape(own, hid)], axis=1
    )
    g_qkv = mm(x_own, dqkv).astype(BF)
    swap = lax.axis_size("dp") == 2
    g_qkv = scatter_row(g_qkv, rows, swap)
    if not swap:
        g_qkv = lax.psum(g_qkv.astype(BF), "dp").astype(F32)
    grad_in = scatter_col(mm_nt(dqkv, w_own).astype(BF)) + grad1
    grad_in = lax.all_to_all(grad_in.T.astype(BF), "row", 0, 1, tiled=True).astype(F32)

    return (
        output,
        grad_in,
        g_qkv[:, :hid].reshape(1, 1, -1),
        g_qkv[:, hid : 2 * hid].reshape(1, 1, -1),
        g_qkv[:, 2 * hid :].reshape(1, 1, -1),
        g_rest[:feat].T.reshape(1, 1, -1),
        g_ffn[:feat],
        g_ffn[feat:],
        g_sums[0],
        g_sums[1],
        g_sums[2],
        g_sums[3],
    )


def solution(mesh):
    tokens = P("row", ("dp", "col"))
    grid = P("row", "col", None)
    return jax.shard_map(
        on_device,
        mesh=mesh,
        in_specs=(
            tokens,
            grid,
            grid,
            grid,
            P("col", "row", None),
            P("row", "col"),
            P("row", "col"),
            P("row"),
            P("row"),
            P("row"),
            P("row"),
            P("dp"),
            P("dp"),
            P("dp", "col", None, None),
            tokens,
        ),
        out_specs=(
            tokens,
            tokens,
            grid,
            grid,
            grid,
            P("col", "row", None),
            P("row", "col"),
            P("row", "col"),
            P("row"),
            P("row"),
            P("row"),
            P("row"),
        ),
        check_vma=False,
    )
```

```python
import functools

import jax
import jax.numpy as jnp
from jax import lax
from jax.experimental import pallas as pl
from jax.experimental.pallas import tpu as pltpu
from jax.sharding import PartitionSpec as P


BLOCK = 64
HW = 64
LANES = 128
NEG = -1000000000.0
EPS = 1e-06
BF = jnp.bfloat16
F32 = jnp.float32


def mm(left, right):
    return lax.dot_general(left, right, (((1,), (0,)), ((), ())), preferred_element_type=F32)


def mm_nt(left, right):
    return lax.dot_general(left, right, (((1,), (1,)), ((), ())), preferred_element_type=F32)


def mm_tn(left, right):
    return lax.dot_general(left, right, (((0,), (0,)), ((), ())), preferred_element_type=F32)


def block_of(j, row, per, rows):
    return (j // per) * (per * rows) + row * per + j % per


def rows_at(ref, block, head):
    start = pl.multiple_of(block * BLOCK, BLOCK)
    return ref[pl.ds(start, BLOCK), head * LANES : (head + 1) * LANES]


def sparse_list(rand_ref, head, pos, nb):
    before = jnp.maximum(pos - 1, 0)
    after = jnp.minimum(pos + 1, nb - 1)
    picks = [rand_ref[(head * nb + pos) * 3 + i] for i in range(3)]
    return [0, nb - 1, before, pos, after] + picks


def dense_list(group):
    return [group * 8 + i for i in range(8)]


def gather(ref, blocks, head):
    return jnp.concatenate([rows_at(ref, b, head) for b in blocks], axis=0)


def allowed_of(query_segs, sk_ref, blocks, own, drop):
    def segs_of(i):
        segs = sk_ref[pl.ds(blocks[i], 1), :]
        if i in drop:
            keep = jnp.where(drop[i], 0, 1)
            segs = segs * keep - 2 * (1 - keep)
        return segs

    low = lax.broadcasted_iota(jnp.int32, (1, LANES), 1) < BLOCK
    segs = jnp.concatenate(
        [jnp.where(low, segs_of(i), segs_of(i + 1)) for i in range(0, len(blocks), 2)], axis=1
    )
    shape = (query_segs.shape[0], segs.shape[1])
    apart = lax.broadcasted_iota(jnp.int32, shape, 1) - lax.broadcasted_iota(jnp.int32, shape, 0)
    query = jnp.concatenate([query_segs] * (len(blocks) // 2), axis=1)
    return (query == segs) | (apart == own * BLOCK)


def forward_kernel(
    heads, nb, per, rows, row_ref, rand_ref, q_ref, qs_ref, kv_ref, sk_ref, o_ref, lse_ref
):
    row = row_ref[0]

    def place(j, head):
        start = pl.multiple_of(j * BLOCK, BLOCK)
        return pl.ds(start, BLOCK), slice(head * LANES, (head + 1) * LANES)

    def store(at, top, total, summed):
        o_ref[at] = (summed * (1.0 / total)).astype(BF)
        lse_ref[at] = jnp.broadcast_to(top + jnp.log(total), (BLOCK, LANES))

    def step(j, carry):
        pos = block_of(j, row, per, rows)
        is_global = (pos == 0) | (pos == nb - 1)
        query_segs = qs_ref[pl.ds(pl.multiple_of(j * BLOCK, BLOCK), BLOCK), :]

        @pl.when(jnp.logical_not(is_global))
        def _():
            for head in range(heads):
                at = place(j, head)
                blocks = sparse_list(rand_ref, head, pos, nb)
                allowed = allowed_of(query_segs, sk_ref, blocks, 3, {2: pos < 2, 4: pos > nb - 3})
                keys = gather(kv_ref, blocks, head)
                score = jnp.where(allowed, mm_nt(q_ref[at], keys), NEG)
                top = jnp.max(score, axis=1, keepdims=True)
                weight = jnp.exp(score - top)
                total = jnp.sum(weight, axis=1, keepdims=True)
                store(at, top, total, mm(weight.astype(BF), keys))

        @pl.when(is_global)
        def _():
            def online(group, kept):
                blocks = dense_list(group)
                allowed = allowed_of(query_segs, sk_ref, blocks, pos - group * 8, {})
                new = []
                for head in range(heads):
                    top, total, summed = kept[head]
                    keys = gather(kv_ref, blocks, head)
                    score = jnp.where(allowed, mm_nt(q_ref[place(j, head)], keys), NEG)
                    above = jnp.maximum(top, jnp.max(score, axis=1, keepdims=True))
                    fade = jnp.exp(top - above)
                    weight = jnp.exp(score - above)
                    total = total * fade + jnp.sum(weight, axis=1, keepdims=True)
                    new.append((above, total, summed * fade + mm(weight.astype(BF), keys)))
                return tuple(new)

            first = (
                jnp.full((BLOCK, 1), 2 * NEG, F32),
                jnp.zeros((BLOCK, 1), F32),
                jnp.zeros((BLOCK, LANES), F32),
            )
            found = lax.fori_loop(0, nb // 8, online, (first,) * heads)
            for head in range(heads):
                store(place(j, head), *found[head])

        return carry

    lax.fori_loop(0, q_ref.shape[0] // BLOCK, step, 0)


def backward_kernel(
    heads, nb, per, rows, row_ref, rand_ref, q_ref, qs_ref, kv_ref, sk_ref, do_ref, lse_ref, o_ref,
    dq_ref, dkv_ref, acc_ref,
):
    row = row_ref[0]
    acc_ref[...] = jnp.zeros_like(acc_ref)

    def place(j, head):
        start = pl.multiple_of(j * BLOCK, BLOCK)
        return pl.ds(start, BLOCK), slice(head * LANES, (head + 1) * LANES)

    def work(j, head, blocks, allowed):
        at = place(j, head)
        keys = gather(kv_ref, blocks, head)
        grad_o = do_ref[at]
        sides = jnp.concatenate([q_ref[at], grad_o], axis=0)
        both = mm_nt(sides, keys)
        dot_row = jnp.sum(grad_o.astype(F32) * o_ref[at].astype(F32), axis=1, keepdims=True)
        probs = jnp.exp(jnp.where(allowed, both[:BLOCK], NEG) - lse_ref[at][:, :1])
        low = (probs * (both[BLOCK:] - dot_row)).astype(BF)
        grad = mm_tn(jnp.concatenate([low, probs.astype(BF)], axis=0), sides)
        for i, block in enumerate(blocks):
            start = pl.multiple_of(block * BLOCK, BLOCK)
            acc_ref[pl.ds(start, BLOCK), at[1]] += grad[i * BLOCK : (i + 1) * BLOCK, :]
        return mm(low, keys)

    def step(j, carry):
        pos = block_of(j, row, per, rows)
        is_global = (pos == 0) | (pos == nb - 1)
        query_segs = qs_ref[pl.ds(pl.multiple_of(j * BLOCK, BLOCK), BLOCK), :]

        @pl.when(jnp.logical_not(is_global))
        def _():
            for head in range(heads):
                blocks = sparse_list(rand_ref, head, pos, nb)
                allowed = allowed_of(query_segs, sk_ref, blocks, 3, {2: pos < 2, 4: pos > nb - 3})
                grad_q = work(j, head, blocks, allowed)
                dq_ref[place(j, head)] = (grad_q * 0.125).astype(BF)

        @pl.when(is_global)
        def _():
            def grads(group, kept):
                blocks = dense_list(group)
                allowed = allowed_of(query_segs, sk_ref, blocks, pos - group * 8, {})
                return tuple(
                    kept[head] + work(j, head, blocks, allowed) for head in range(heads)
                )

            done = lax.fori_loop(
                0, nb // 8, grads, tuple(jnp.zeros((BLOCK, LANES), F32) for _ in range(heads))
            )
            for head in range(heads):
                dq_ref[place(j, head)] = (done[head] * 0.125).astype(BF)

        return carry

    lax.fori_loop(0, q_ref.shape[0] // BLOCK, step, 0)
    span = per * BLOCK

    def out(i, carry):
        source = (i % rows) * (rows * span) + (i // rows) * span
        dkv_ref[pl.ds(pl.multiple_of(i * span, span), span), :] = acc_ref[
            pl.ds(pl.multiple_of(source, span), span), :
        ].astype(BF)
        return carry

    lax.fori_loop(0, kv_ref.shape[0] // span, out, 0)


def specs(count):
    return [pl.BlockSpec(memory_space=pltpu.SMEM)] * 2 + [
        pl.BlockSpec(memory_space=pltpu.VMEM)
    ] * count


def attention_forward(dims, row, rand, q, q_segs, kv, k_segs):
    own, wide = q.shape
    vmem = pl.BlockSpec(memory_space=pltpu.VMEM)
    return pl.pallas_call(
        functools.partial(forward_kernel, *dims),
        name="attn_fwd",
        out_shape=(
            jax.ShapeDtypeStruct((own, wide), BF),
            jax.ShapeDtypeStruct((own, wide), F32),
        ),
        in_specs=specs(4),
        out_specs=(vmem, vmem),
        cost_estimate=pl.CostEstimate(
            flops=own * 512 * wide * 6, bytes_accessed=12 << 20, transcendentals=own * 512 * 3
        ),
        compiler_params=pltpu.CompilerParams(vmem_limit_bytes=48 << 20),
    )(row, rand, q, q_segs, kv, k_segs)


def attention_backward(dims, row, rand, q, q_segs, kv, k_segs, d_o, lse, o):
    own, wide = q.shape
    vmem = pl.BlockSpec(memory_space=pltpu.VMEM)
    return pl.pallas_call(
        functools.partial(backward_kernel, *dims),
        name="attn_bwd",
        out_shape=(
            jax.ShapeDtypeStruct((own, wide), BF),
            jax.ShapeDtypeStruct(kv.shape, BF),
        ),
        in_specs=specs(7),
        out_specs=(vmem, vmem),
        scratch_shapes=[pltpu.VMEM(kv.shape, F32)],
        cost_estimate=pl.CostEstimate(
            flops=own * 512 * wide * 12, bytes_accessed=20 << 20, transcendentals=own * 512 * 3
        ),
        compiler_params=pltpu.CompilerParams(vmem_limit_bytes=48 << 20),
    )(row, rand, q, q_segs, kv, k_segs, d_o, lse, o)


def project_kernel(
    rows, span, row_ref, x_ref, wq_ref, wkv_ref, q_ref, kv_ref, own_ref
):
    feat = x_ref.shape[2]
    start = pl.multiple_of(row_ref[0] * span, span)
    kv = q = None
    for part in range(rows):
        at = slice(part * feat, (part + 1) * feat)
        mine = x_ref[part, 0, :, pl.ds(start, span)]
        own_ref[at, :] = mine
        kv_part = mm_tn(x_ref[part, 0], wkv_ref[at, :])
        q_part = mm_tn(mine, wq_ref[at, :])
        kv = kv_part if kv is None else kv + kv_part
        q = q_part if q is None else q + q_part
    kv_ref[...] = kv.astype(BF)
    q_ref[...] = (q.astype(BF) * 0.125).astype(BF)


def project(row, x_parts, w_q, w_kv, span):
    rows, cols, feat, local = x_parts.shape
    model, wide = w_q.shape
    return pl.pallas_call(
        functools.partial(project_kernel, rows, span),
        name="project",
        grid=(cols,),
        out_shape=(
            jax.ShapeDtypeStruct((cols * span, wide), BF),
            jax.ShapeDtypeStruct((cols * local, wide), BF),
            jax.ShapeDtypeStruct((model, cols * span), BF),
        ),
        in_specs=[
            pl.BlockSpec(memory_space=pltpu.SMEM),
            pl.BlockSpec((rows, 1, feat, local), lambda c: (0, c, 0, 0)),
            pl.BlockSpec((model, wide), lambda c: (0, 0)),
            pl.BlockSpec((model, wide), lambda c: (0, 0)),
        ],
        out_specs=(
            pl.BlockSpec((span, wide), lambda c: (c, 0)),
            pl.BlockSpec((local, wide), lambda c: (c, 0)),
            pl.BlockSpec((model, span), lambda c: (0, c)),
        ),
        cost_estimate=pl.CostEstimate(
            flops=cols * local * model * wide * 3, bytes_accessed=16 << 20, transcendentals=0
        ),
        compiler_params=pltpu.CompilerParams(vmem_limit_bytes=48 << 20),
    )(row, x_parts, w_q, w_kv)


PIECES = 2


def col_places():
    me = lax.axis_index("col")
    partner = me + 1 - 2 * lax.rem(me, 2)
    cross = lax.rem(me + 2, 4)
    diag = lax.rem(partner + 2, 4)
    barrier = pltpu.get_barrier_semaphore()
    for peer in (partner, cross):
        pl.semaphore_signal(
            barrier, inc=1, device_id={"col": peer}, device_id_type=pl.DeviceIdType.MESH
        )
    pl.semaphore_wait(barrier, 2)
    return me, partner, cross, diag


def send_to(source, target, sems, kind, piece, peer):
    copy = pltpu.make_async_remote_copy(
        src_ref=source,
        dst_ref=target,
        send_sem=sems[0].at[kind, piece],
        recv_sem=sems[1].at[kind, piece],
        device_id={"col": peer},
        device_id_type=pl.DeviceIdType.MESH,
    )
    copy.start()
    return copy


def gather_kernel(x_ref, out_ref, send_sem, recv_sem):
    me, partner, cross, _ = col_places()
    sems = (send_sem, recv_sem)
    size = x_ref.shape[0] // PIECES
    cuts = [pl.ds(i * size, size) for i in range(PIECES)]
    over = [
        send_to(x_ref.at[cut], out_ref.at[me, cut], sems, 0, i, cross)
        for i, cut in enumerate(cuts)
    ]
    near = [
        send_to(x_ref.at[cut], out_ref.at[me, cut], sems, 1, i, partner)
        for i, cut in enumerate(cuts)
    ]
    out_ref[me] = x_ref[...]
    relay = []
    for i, cut in enumerate(cuts):
        over[i].wait_recv()
        relay.append(
            send_to(out_ref.at[cross, cut], out_ref.at[cross, cut], sems, 2, i, partner)
        )
    for i in range(PIECES):
        over[i].wait_send()
        near[i].wait()
        relay[i].wait()


def scatter_kernel(x_ref, out_ref, near_buf, sum_buf, over_buf, send_sem, recv_sem):
    me, partner, cross, diag = col_places()
    sems = (send_sem, recv_sem)
    size = x_ref.shape[1] // PIECES
    cuts = [pl.ds(i * size, size) for i in range(PIECES)]
    first = [
        send_to(x_ref.at[diag, cut], near_buf.at[1, cut], sems, 0, i, partner)
        for i, cut in enumerate(cuts)
    ]
    second = [
        send_to(x_ref.at[partner, cut], near_buf.at[0, cut], sems, 1, i, partner)
        for i, cut in enumerate(cuts)
    ]
    over = []
    for i, cut in enumerate(cuts):
        first[i].wait_recv()
        sum_buf[cut, :] = (
            x_ref[cross, cut, :].astype(F32) + near_buf[1, cut, :].astype(F32)
        ).astype(BF)
        over.append(send_to(sum_buf.at[cut], over_buf.at[cut], sems, 2, i, cross))
    for i, cut in enumerate(cuts):
        second[i].wait_recv()
        out_ref[cut, :] = x_ref[me, cut, :].astype(F32) + near_buf[0, cut, :].astype(F32)
    for i, cut in enumerate(cuts):
        over[i].wait_recv()
        out_ref[cut, :] += over_buf[cut, :].astype(F32)
    for i in range(PIECES):
        first[i].wait_send()
        second[i].wait_send()
        over[i].wait_send()


def scatter_row_kernel(
    rows, swap, x_ref, out_ref, from_left, from_right, to_right, to_left, own_buf, peer_buf,
    send_sem, recv_sem, swap_sem,
):
    me = lax.axis_index("row")
    right, left = lax.rem(me + 1, rows), lax.rem(me + rows - 1, rows)
    has_left, has_right = me > 0, me < rows - 1
    mesh_id = pl.DeviceIdType.MESH
    barrier = pltpu.get_barrier_semaphore()

    @pl.when(has_left)
    def _():
        pl.semaphore_signal(barrier, inc=1, device_id={"row": left}, device_id_type=mesh_id)

    @pl.when(has_right)
    def _():
        pl.semaphore_signal(barrier, inc=1, device_id={"row": right}, device_id_type=mesh_id)

    if swap:
        peer = 1 - lax.axis_index("dp")
        pl.semaphore_signal(barrier, inc=1, device_id={"dp": peer}, device_id_type=mesh_id)

    peers = jnp.where(has_left, 1, 0) + jnp.where(has_right, 1, 0) + (1 if swap else 0)
    pl.semaphore_wait(barrier, peers)

    size = x_ref.shape[1] // PIECES
    cuts = [pl.ds(i * size, size) for i in range(PIECES)]

    def hop(way, dest, i):
        stage, target, to = ((to_right, from_left, right), (to_left, from_right, left))[way]
        return pltpu.make_async_remote_copy(
            src_ref=stage.at[dest, cuts[i]],
            dst_ref=target.at[dest, cuts[i]],
            send_sem=send_sem.at[way, dest, i],
            recv_sem=recv_sem.at[way, dest, i],
            device_id={"row": to},
            device_id_type=mesh_id,
        )

    flows = []
    for step in range(rows - 1):
        flows.append((0, rows - 1 - step, me < rows - 1 - step, has_left))
        flows.append((1, step, me > step, has_right))
    for way, dest, active, relays in flows:
        stage, came = ((to_right, from_left), (to_left, from_right))[way]
        for i, cut in enumerate(cuts):

            @pl.when(active & relays)
            def _():
                hop(way, dest, i).wait_recv()
                stage[dest, cut, :] = (
                    x_ref[dest, cut, :].astype(F32) + came[dest, cut, :].astype(F32)
                ).astype(BF)

            @pl.when(active & jnp.logical_not(relays))
            def _():
                stage[dest, cut, :] = x_ref[dest, cut, :]

            @pl.when(active)
            def _():
                hop(way, dest, i).start()

    out_ref[...] = x_ref[me].astype(F32)
    for way, came, has in ((0, from_left, has_left), (1, from_right, has_right)):

        @pl.when(has)
        def _():
            for i, cut in enumerate(cuts):
                hop(way, me, i).wait_recv()
                out_ref[cut, :] += came[me, cut, :].astype(F32)

    for way, dest, active, _ in flows:

        @pl.when(active)
        def _():
            for i in range(PIECES):
                hop(way, dest, i).wait_send()

    if swap:
        own_buf[...] = out_ref[...].astype(BF)
        copy = pltpu.make_async_remote_copy(
            src_ref=own_buf,
            dst_ref=peer_buf,
            send_sem=swap_sem.at[0],
            recv_sem=swap_sem.at[1],
            device_id={"dp": peer},
            device_id_type=mesh_id,
        )
        copy.start()
        copy.wait()
        out_ref[...] = own_buf[...].astype(F32) + peer_buf[...].astype(F32)


def scatter_row(value, rows, swap):
    count, wide = value.shape[0] // rows, value.shape[1]
    vmem = pl.BlockSpec(memory_space=pltpu.VMEM)
    return pl.pallas_call(
        functools.partial(scatter_row_kernel, rows, swap),
        name="scatter_row",
        out_shape=jax.ShapeDtypeStruct((count, wide), F32),
        in_specs=[vmem],
        out_specs=vmem,
        scratch_shapes=[pltpu.VMEM((rows, count, wide), BF)] * 4
        + [pltpu.VMEM((count, wide), BF)] * 2
        + [
            pltpu.SemaphoreType.DMA((2, rows, PIECES)),
            pltpu.SemaphoreType.DMA((2, rows, PIECES)),
            pltpu.SemaphoreType.DMA((2,)),
        ],
        compiler_params=comm_params(4),
    )(value.reshape(rows, count, wide))


def gather_in_kernel(rows, x_ref, w_ref, xs_ref, ws_ref, send_x, recv_x, send_w, recv_w):
    me, col = lax.axis_index("row"), lax.axis_index("col")
    right, left = lax.rem(me + 1, rows), lax.rem(me + rows - 1, rows)
    has_left, has_right = me > 0, me < rows - 1
    partner = col + 1 - 2 * lax.rem(col, 2)
    cross = lax.rem(col + 2, 4)
    diag = lax.rem(partner + 2, 4)
    mesh_id = pl.DeviceIdType.MESH
    barrier = pltpu.get_barrier_semaphore()

    @pl.when(has_left)
    def _():
        pl.semaphore_signal(barrier, inc=1, device_id={"row": left}, device_id_type=mesh_id)

    @pl.when(has_right)
    def _():
        pl.semaphore_signal(barrier, inc=1, device_id={"row": right}, device_id_type=mesh_id)

    for peer in (partner, cross):
        pl.semaphore_signal(barrier, inc=1, device_id={"col": peer}, device_id_type=mesh_id)
    pl.semaphore_wait(barrier, jnp.where(has_left, 1, 0) + jnp.where(has_right, 1, 0) + 2)

    def copy_x(source, kind, shard, slot, where):
        return pltpu.make_async_remote_copy(
            src_ref=source,
            dst_ref=xs_ref.at[shard, slot],
            send_sem=send_x.at[kind, shard],
            recv_sem=recv_x.at[kind, shard],
            device_id=where,
            device_id_type=mesh_id,
        )

    def copy_w(source, kind, shard, where):
        return pltpu.make_async_remote_copy(
            src_ref=source,
            dst_ref=ws_ref.at[shard],
            send_sem=send_w.at[kind, shard],
            recv_sem=recv_w.at[kind, shard],
            device_id=where,
            device_id_type=mesh_id,
        )

    to_right, to_left = {"row": right}, {"row": left}
    ways = ((0, has_right, to_right), (1, has_left, to_left))

    for kind, onward, where in ways:

        @pl.when(onward)
        def _():
            copy_x(x_ref, kind, me, col, where).start()

    copy_x(x_ref, 2, me, col, {"col": cross}).start()
    copy_x(x_ref, 3, me, col, {"col": partner}).start()
    for kind, onward, where in ways:

        @pl.when(onward)
        def _():
            copy_w(w_ref, kind, me, where).start()

    xs_ref[me, col] = x_ref[...]
    ws_ref[me] = w_ref[...]

    def relay(shard):
        copy_x(x_ref, 2, shard, cross, {"col": cross}).wait_recv()
        source = xs_ref.at[shard, cross]
        copy_x(source, 4, shard, cross, {"col": partner}).start()

    def shards_at(step):
        return (
            (0, me - step, me >= step, has_right, to_right),
            (1, me + step, me + step <= rows - 1, has_left, to_left),
        )

    for step in range(1, rows):
        for kind, shard, exists, onward, where in shards_at(step):

            @pl.when(exists)
            def _():
                copy_x(x_ref, kind, shard, col, where).wait_recv()

                @pl.when(onward)
                def _():
                    copy_x(xs_ref.at[shard, col], kind, shard, col, where).start()

                copy_x(xs_ref.at[shard, col], 2, shard, col, {"col": cross}).start()
                copy_x(xs_ref.at[shard, col], 3, shard, col, {"col": partner}).start()

        for kind, shard, exists, onward, where in shards_at(step):

            @pl.when(exists)
            def _():
                copy_w(w_ref, kind, shard, where).wait_recv()

                @pl.when(onward)
                def _():
                    copy_w(ws_ref.at[shard], kind, shard, where).start()

        if step == 1:
            relay(me)
        else:
            for _, shard, exists, _, _ in shards_at(step - 1):

                @pl.when(exists)
                def _():
                    relay(shard)

    for _, shard, exists, _, _ in shards_at(rows - 1):

        @pl.when(exists)
        def _():
            relay(shard)

    for shard in range(rows):
        copy_x(x_ref, 3, shard, partner, {"col": partner}).wait_recv()
        copy_x(x_ref, 4, shard, diag, {"col": partner}).wait_recv()
        for kind in (2, 3, 4):
            copy_x(x_ref, kind, shard, col, {"col": partner}).wait_send()
        for kind, sent, where in (
            (0, has_right & (me >= shard), to_right),
            (1, has_left & (me <= shard), to_left),
        ):

            @pl.when(sent)
            def _():
                copy_x(x_ref, kind, shard, col, where).wait_send()
                copy_w(w_ref, kind, shard, where).wait_send()


def gather_in(x, w, rows):
    vmem = pl.BlockSpec(memory_space=pltpu.VMEM)
    sems = pltpu.SemaphoreType.DMA
    return pl.pallas_call(
        functools.partial(gather_in_kernel, rows),
        name="gather_in",
        out_shape=(
            jax.ShapeDtypeStruct((rows, 4) + x.shape, BF),
            jax.ShapeDtypeStruct((rows,) + w.shape, BF),
        ),
        in_specs=[vmem, vmem],
        out_specs=(vmem, vmem),
        scratch_shapes=[sems((5, rows)), sems((5, rows)), sems((2, rows)), sems((2, rows))],
        compiler_params=comm_params(5),
    )(x, w)


def comm_params(ident):
    return pltpu.CompilerParams(
        collective_id=ident, has_side_effects=True, vmem_limit_bytes=32 << 20
    )


def comm_sems(kinds):
    return [pltpu.SemaphoreType.DMA((kinds, PIECES)), pltpu.SemaphoreType.DMA((kinds, PIECES))]


def gather_col(value, ident):
    count, wide = value.shape
    vmem = pl.BlockSpec(memory_space=pltpu.VMEM)
    return pl.pallas_call(
        gather_kernel,
        name="gather_col",
        out_shape=jax.ShapeDtypeStruct((4, count, wide), BF),
        in_specs=[vmem],
        out_specs=vmem,
        scratch_shapes=comm_sems(3),
        compiler_params=comm_params(ident),
    )(value)


def scatter_col(value):
    count, wide = value.shape[0] // 4, value.shape[1]
    vmem = pl.BlockSpec(memory_space=pltpu.VMEM)
    return pl.pallas_call(
        scatter_kernel,
        name="scatter_col",
        out_shape=jax.ShapeDtypeStruct((count, wide), F32),
        in_specs=[vmem],
        out_specs=vmem,
        scratch_shapes=[
            pltpu.VMEM((2, count, wide), BF),
            pltpu.VMEM((count, wide), BF),
            pltpu.VMEM((count, wide), BF),
        ]
        + comm_sems(3),
        compiler_params=comm_params(2),
    )(value.reshape(4, count, wide))


def norm(resid, gain, bias):
    mean = jnp.mean(resid, axis=1, keepdims=True)
    var = jnp.mean(resid * resid, axis=1, keepdims=True) - mean * mean
    rstd = lax.rsqrt(var + EPS)
    normed = (resid - mean) * rstd
    return normed * gain + bias, normed, rstd


def norm_grad(grad, normed, rstd, gain):
    scaled = grad * gain
    first = jnp.mean(scaled, axis=1, keepdims=True)
    second = jnp.mean(scaled * normed, axis=1, keepdims=True)
    return rstd * (scaled - first - normed * second)


def gelu(value):
    return jax.nn.gelu(value, approximate=True)


def on_device(
    inputs, w_query, w_key, w_value, w_out, w_up, w_down,
    ln1_gain, ln1_bias, ln2_gain, ln2_bias, segment_ids, pad_mask, rand_blocks, grad_out,
):
    rows, cols = lax.axis_size("row"), lax.axis_size("col")
    row, col = lax.axis_index("row"), lax.axis_index("col")
    feat, local = inputs.shape
    model = feat * rows
    hid = model // cols
    heads = hid // HW
    length = local * cols
    nb = length // BLOCK
    span = local // rows
    per = span // BLOCK
    dims = (heads, nb, per, rows)
    own = cols * span

    blk_q = w_query.reshape(feat, hid)
    blk_k = w_key.reshape(feat, hid)
    blk_v = w_value.reshape(feat, hid)
    blk_o = w_out.reshape(hid, feat)
    params = jnp.stack([ln1_gain, ln1_bias, ln2_gain, ln2_bias])
    high = params.astype(BF)
    rest = params - high.astype(F32)
    middle = rest.astype(BF)
    low = (rest - middle.astype(F32)).astype(BF)
    params = jnp.concatenate([high, middle, low], axis=0)
    params = jnp.pad(params, ((0, 4), (0, 4 * hid - feat)))
    w_small = jnp.concatenate([blk_q, blk_k, blk_v, blk_o.T], axis=1)
    w_small = jnp.concatenate([w_small, params], axis=0)
    x_parts, w_small = gather_in(inputs, w_small, rows)
    w_rest = jnp.concatenate([w_up, w_down], axis=1)
    x_parts, w_rest, grad_out = lax.optimization_barrier((x_parts, w_rest, grad_out))
    w_rest = lax.all_gather(w_rest, "row", axis=0, tiled=True)
    ff = w_up.shape[1]
    up, down = w_rest[:, :ff], w_rest[:, ff:]
    gains = w_small[:, feat : feat + 12, :feat].astype(F32).reshape(rows, 3, 4, feat)
    gains = (gains[:, 0] + gains[:, 1]) + gains[:, 2]
    gains = gains.transpose(1, 0, 2).reshape(4, 1, model)
    w_small = w_small[:, :feat].reshape(model, 4 * hid)
    w_own, w_o = w_small[:, : 3 * hid], w_small[:, 3 * hid :]
    grad_rows = lax.all_to_all(grad_out, "row", 1, 0, tiled=True).T.astype(F32)

    w_heads = w_own.reshape(model, 3, heads, HW)
    w_kv = jnp.concatenate([w_heads[:, 1], w_heads[:, 2]], axis=2).reshape(model, heads * LANES)
    w_q = jnp.pad(w_heads[:, 0], ((0, 0), (0, 0), (0, HW))).reshape(model, heads * LANES)
    row_arr = jnp.reshape(row, (1,)).astype(jnp.int32)
    q, kv, x_own = project(row_arr, x_parts, w_q, w_kv, span)
    x_res = lax.dynamic_slice_in_dim(x_own, col * span, span, axis=1).T.astype(F32)

    rand = rand_blocks.reshape(-1)
    k_segs = jnp.where(pad_mask == 1, segment_ids, -1).reshape(nb, BLOCK)
    k_segs = jnp.concatenate([k_segs, k_segs], axis=1)
    q_segs = lax.dynamic_index_in_dim(
        segment_ids.reshape(cols, rows, span), row, axis=1, keepdims=False
    )
    q_segs = jnp.broadcast_to(q_segs.reshape(own, 1), (own, LANES))
    o_wide, lse = attention_forward(dims, row_arr, rand, q, q_segs, kv, k_segs)
    o = o_wide.reshape(own, heads, 2, HW)[:, :, 1].reshape(own, hid)
    attn = scatter_col(mm_nt(o, w_o).astype(BF))

    gain1, bias1, gain2, bias2 = gains[0], gains[1], gains[2], gains[3]
    hidden, normed1, rstd1 = norm(x_res + attn, gain1, bias1)
    hidden_all = gather_col(hidden.astype(BF), 1).reshape(own, model)
    up_val = mm(hidden_all, up)
    act, gelu_back = jax.vjp(gelu, up_val)
    act = act.astype(BF)
    ffn = scatter_col(mm_nt(act, down).astype(BF))
    result, normed2, rstd2 = norm(hidden + ffn, gain2, bias2)
    output = lax.all_to_all(result.T.astype(BF), "row", 0, 1, tiled=True)

    grad2 = norm_grad(grad_rows, normed2, rstd2, gain2)
    df = gather_col(grad2.astype(BF), 1).reshape(own, model)
    g_down = mm_tn(df, act).astype(BF)
    du = gelu_back(mm(df, down))[0].astype(BF)
    g_up = mm_tn(hidden_all, du).astype(BF)
    g_ffn = jnp.concatenate(
        [g_up.reshape(rows, feat, ff), g_down.reshape(rows, feat, ff)], axis=1
    ).reshape(2 * model, ff)
    du, g_ffn = lax.optimization_barrier((du, g_ffn))
    g_ffn = lax.psum_scatter(g_ffn, "row", scatter_dimension=0, tiled=True)
    dh = scatter_col(mm_nt(du, up).astype(BF))
    dh = dh + grad2
    grad1 = norm_grad(dh, normed1, rstd1, gain1)
    sums = jnp.stack(
        [
            jnp.sum(dh * normed1, axis=0),
            jnp.sum(dh, axis=0),
            jnp.sum(grad_rows * normed2, axis=0),
            jnp.sum(grad_rows, axis=0),
        ]
    )
    extra = jnp.pad(sums, ((0, 28), (0, 0))).astype(BF)
    dattn = gather_col(jnp.concatenate([grad1.astype(BF), extra], axis=0), 3)
    sums = jnp.sum(dattn[:, span : span + 4].astype(F32), axis=0)
    dattn = dattn[:, :span].reshape(own, model)
    g_out = mm_tn(dattn, o).astype(BF)
    d_o = mm(dattn, w_o).astype(BF)
    d_o = jnp.pad(d_o.reshape(own, heads, HW), ((0, 0), (0, 0), (HW, 0))).reshape(own, -1)

    sums = sums.reshape(4, rows, feat).transpose(1, 0, 2).astype(BF)
    sums = jnp.pad(sums, ((0, 0), (0, 12), (0, hid - feat)))
    g_rest = jnp.concatenate([g_out.reshape(rows, feat, hid), sums], axis=1).reshape(-1, hid)
    d_o, g_rest = lax.optimization_barrier((d_o, g_rest))
    g_rest = lax.psum_scatter(g_rest, "row", scatter_dimension=0, tiled=True)
    dq, dkv = attention_backward(dims, row_arr, rand, q, q_segs, kv, k_segs, d_o, lse, o_wide)
    dkv = lax.psum_scatter(dkv, "row", scatter_dimension=0, tiled=True)
    dkv, g_ffn, g_rest = lax.optimization_barrier((dkv, g_ffn, g_rest))
    g_ffn, g_rest = lax.psum((g_ffn, g_rest), "dp")
    g_ffn, g_rest = g_ffn.astype(F32), g_rest.astype(F32)
    g_sums = g_rest[feat : feat + 4, :feat]
    dq = dq.reshape(own, heads, 2, HW)[:, :, 0].reshape(own, hid)
    dkv = dkv.reshape(own, heads, 2, HW)
    dqkv = jnp.concatenate(
        [dq, dkv[:, :, 0].reshape(own, hid), dkv[:, :, 1].reshape(own, hid)], axis=1
    )
    g_qkv = mm(x_own, dqkv).astype(BF)
    swap = lax.axis_size("dp") == 2
    g_qkv = scatter_row(g_qkv, rows, swap)
    if not swap:
        g_qkv = lax.psum(g_qkv.astype(BF), "dp").astype(F32)
    grad_in = scatter_col(mm_nt(dqkv, w_own).astype(BF))
    grad_in = grad_in + grad1
    grad_in = lax.all_to_all(grad_in.T.astype(BF), "row", 0, 1, tiled=True).astype(F32)

    return (
        output,
        grad_in,
        g_qkv[:, :hid].reshape(1, 1, -1),
        g_qkv[:, hid : 2 * hid].reshape(1, 1, -1),
        g_qkv[:, 2 * hid :].reshape(1, 1, -1),
        g_rest[:feat].T.reshape(1, 1, -1),
        g_ffn[:feat],
        g_ffn[feat:],
        g_sums[0],
        g_sums[1],
        g_sums[2],
        g_sums[3],
    )


def solution(mesh):
    tokens = P("row", ("dp", "col"))
    grid = P("row", "col", None)
    return jax.shard_map(
        on_device,
        mesh=mesh,
        in_specs=(
            tokens,
            grid,
            grid,
            grid,
            P("col", "row", None),
            P("row", "col"),
            P("row", "col"),
            P("row"),
            P("row"),
            P("row"),
            P("row"),
            P("dp"),
            P("dp"),
            P("dp", "col", None, None),
            tokens,
        ),
        out_specs=(
            tokens,
            tokens,
            grid,
            grid,
            grid,
            P("col", "row", None),
            P("row", "col"),
            P("row", "col"),
            P("row"),
            P("row"),
            P("row"),
            P("row"),
        ),
        check_vma=False,
    )
```

```python
import functools

import jax
import jax.numpy as jnp
from jax import lax
from jax.experimental import pallas as pl
from jax.experimental.pallas import tpu as pltpu
from jax.sharding import PartitionSpec as P


BLOCK = 64
HW = 64
LANES = 128
NEG = -1000000000.0
EPS = 1e-06
BF = jnp.bfloat16
F32 = jnp.float32


def mm(left, right):
    return lax.dot_general(left, right, (((1,), (0,)), ((), ())), preferred_element_type=F32)


def mm_nt(left, right):
    return lax.dot_general(left, right, (((1,), (1,)), ((), ())), preferred_element_type=F32)


def mm_tn(left, right):
    return lax.dot_general(left, right, (((0,), (0,)), ((), ())), preferred_element_type=F32)


def block_of(j, row, per, rows):
    return (j // per) * (per * rows) + row * per + j % per


def rows_at(ref, block, head):
    start = pl.multiple_of(block * BLOCK, BLOCK)
    return ref[pl.ds(start, BLOCK), head * LANES : (head + 1) * LANES]


def sparse_list(rand_ref, head, pos, nb):
    before = jnp.maximum(pos - 1, 0)
    after = jnp.minimum(pos + 1, nb - 1)
    picks = [rand_ref[(head * nb + pos) * 3 + i] for i in range(3)]
    return [0, nb - 1, before, pos, after] + picks


def dense_list(group):
    return [group * 8 + i for i in range(8)]


def gather(ref, blocks, head):
    return jnp.concatenate([rows_at(ref, b, head) for b in blocks], axis=0)


def allowed_of(query_segs, sk_ref, blocks, own, drop):
    def segs_of(i):
        segs = sk_ref[pl.ds(blocks[i], 1), :]
        if i in drop:
            keep = jnp.where(drop[i], 0, 1)
            segs = segs * keep - 2 * (1 - keep)
        return segs

    low = lax.broadcasted_iota(jnp.int32, (1, LANES), 1) < BLOCK
    segs = jnp.concatenate(
        [jnp.where(low, segs_of(i), segs_of(i + 1)) for i in range(0, len(blocks), 2)], axis=1
    )
    shape = (query_segs.shape[0], segs.shape[1])
    apart = lax.broadcasted_iota(jnp.int32, shape, 1) - lax.broadcasted_iota(jnp.int32, shape, 0)
    query = jnp.concatenate([query_segs] * (len(blocks) // 2), axis=1)
    return (query == segs) | (apart == own * BLOCK)


def forward_kernel(
    heads, nb, per, rows, row_ref, rand_ref, q_ref, qs_ref, kv_ref, sk_ref, o_ref, lse_ref
):
    row = row_ref[0]

    def place(j, head):
        start = pl.multiple_of(j * BLOCK, BLOCK)
        return pl.ds(start, BLOCK), slice(head * LANES, (head + 1) * LANES)

    def store(at, top, total, summed):
        o_ref[at] = (summed * (1.0 / total)).astype(BF)
        lse_ref[at] = jnp.broadcast_to(top + jnp.log(total), (BLOCK, LANES))

    def step(j, carry):
        pos = block_of(j, row, per, rows)
        is_global = (pos == 0) | (pos == nb - 1)
        query_segs = qs_ref[pl.ds(pl.multiple_of(j * BLOCK, BLOCK), BLOCK), :]

        @pl.when(jnp.logical_not(is_global))
        def _():
            for head in range(heads):
                at = place(j, head)
                blocks = sparse_list(rand_ref, head, pos, nb)
                allowed = allowed_of(query_segs, sk_ref, blocks, 3, {2: pos < 2, 4: pos > nb - 3})
                keys = gather(kv_ref, blocks, head)
                score = jnp.where(allowed, mm_nt(q_ref[at], keys), NEG)
                top = jnp.max(score, axis=1, keepdims=True)
                weight = jnp.exp(score - top)
                total = jnp.sum(weight, axis=1, keepdims=True)
                store(at, top, total, mm(weight.astype(BF), keys))

        @pl.when(is_global)
        def _():
            def online(group, kept):
                blocks = dense_list(group)
                allowed = allowed_of(query_segs, sk_ref, blocks, pos - group * 8, {})
                new = []
                for head in range(heads):
                    top, total, summed = kept[head]
                    keys = gather(kv_ref, blocks, head)
                    score = jnp.where(allowed, mm_nt(q_ref[place(j, head)], keys), NEG)
                    above = jnp.maximum(top, jnp.max(score, axis=1, keepdims=True))
                    fade = jnp.exp(top - above)
                    weight = jnp.exp(score - above)
                    total = total * fade + jnp.sum(weight, axis=1, keepdims=True)
                    new.append((above, total, summed * fade + mm(weight.astype(BF), keys)))
                return tuple(new)

            first = (
                jnp.full((BLOCK, 1), 2 * NEG, F32),
                jnp.zeros((BLOCK, 1), F32),
                jnp.zeros((BLOCK, LANES), F32),
            )
            found = lax.fori_loop(0, nb // 8, online, (first,) * heads)
            for head in range(heads):
                store(place(j, head), *found[head])

        return carry

    lax.fori_loop(0, q_ref.shape[0] // BLOCK, step, 0)


def backward_kernel(
    heads, nb, per, rows, row_ref, rand_ref, q_ref, qs_ref, kv_ref, sk_ref, do_ref, lse_ref, o_ref,
    dq_ref, dkv_ref, acc_ref,
):
    row = row_ref[0]
    acc_ref[...] = jnp.zeros_like(acc_ref)

    def place(j, head):
        start = pl.multiple_of(j * BLOCK, BLOCK)
        return pl.ds(start, BLOCK), slice(head * LANES, (head + 1) * LANES)

    def work(j, head, blocks, allowed):
        at = place(j, head)
        keys = gather(kv_ref, blocks, head)
        grad_o = do_ref[at]
        sides = jnp.concatenate([q_ref[at], grad_o], axis=0)
        both = mm_nt(sides, keys)
        dot_row = jnp.sum(grad_o.astype(F32) * o_ref[at].astype(F32), axis=1, keepdims=True)
        probs = jnp.exp(jnp.where(allowed, both[:BLOCK], NEG) - lse_ref[at][:, :1])
        low = (probs * (both[BLOCK:] - dot_row)).astype(BF)
        grad = mm_tn(jnp.concatenate([low, probs.astype(BF)], axis=0), sides)
        for i, block in enumerate(blocks):
            start = pl.multiple_of(block * BLOCK, BLOCK)
            acc_ref[pl.ds(start, BLOCK), at[1]] += grad[i * BLOCK : (i + 1) * BLOCK, :]
        return mm(low, keys)

    def step(j, carry):
        pos = block_of(j, row, per, rows)
        is_global = (pos == 0) | (pos == nb - 1)
        query_segs = qs_ref[pl.ds(pl.multiple_of(j * BLOCK, BLOCK), BLOCK), :]

        @pl.when(jnp.logical_not(is_global))
        def _():
            for head in range(heads):
                blocks = sparse_list(rand_ref, head, pos, nb)
                allowed = allowed_of(query_segs, sk_ref, blocks, 3, {2: pos < 2, 4: pos > nb - 3})
                grad_q = work(j, head, blocks, allowed)
                dq_ref[place(j, head)] = (grad_q * 0.125).astype(BF)

        @pl.when(is_global)
        def _():
            def grads(group, kept):
                blocks = dense_list(group)
                allowed = allowed_of(query_segs, sk_ref, blocks, pos - group * 8, {})
                return tuple(
                    kept[head] + work(j, head, blocks, allowed) for head in range(heads)
                )

            done = lax.fori_loop(
                0, nb // 8, grads, tuple(jnp.zeros((BLOCK, LANES), F32) for _ in range(heads))
            )
            for head in range(heads):
                dq_ref[place(j, head)] = (done[head] * 0.125).astype(BF)

        return carry

    lax.fori_loop(0, q_ref.shape[0] // BLOCK, step, 0)
    span = per * BLOCK

    def out(i, carry):
        source = (i % rows) * (rows * span) + (i // rows) * span
        dkv_ref[pl.ds(pl.multiple_of(i * span, span), span), :] = acc_ref[
            pl.ds(pl.multiple_of(source, span), span), :
        ].astype(BF)
        return carry

    lax.fori_loop(0, kv_ref.shape[0] // span, out, 0)


def specs(count):
    return [pl.BlockSpec(memory_space=pltpu.SMEM)] * 2 + [
        pl.BlockSpec(memory_space=pltpu.VMEM)
    ] * count


def attention_forward(dims, row, rand, q, q_segs, kv, k_segs):
    own, wide = q.shape
    vmem = pl.BlockSpec(memory_space=pltpu.VMEM)
    return pl.pallas_call(
        functools.partial(forward_kernel, *dims),
        name="attn_fwd",
        out_shape=(
            jax.ShapeDtypeStruct((own, wide), BF),
            jax.ShapeDtypeStruct((own, wide), F32),
        ),
        in_specs=specs(4),
        out_specs=(vmem, vmem),
        cost_estimate=pl.CostEstimate(
            flops=own * 512 * wide * 6, bytes_accessed=12 << 20, transcendentals=own * 512 * 3
        ),
        compiler_params=pltpu.CompilerParams(vmem_limit_bytes=48 << 20),
    )(row, rand, q, q_segs, kv, k_segs)


def attention_backward(dims, row, rand, q, q_segs, kv, k_segs, d_o, lse, o):
    own, wide = q.shape
    vmem = pl.BlockSpec(memory_space=pltpu.VMEM)
    return pl.pallas_call(
        functools.partial(backward_kernel, *dims),
        name="attn_bwd",
        out_shape=(
            jax.ShapeDtypeStruct((own, wide), BF),
            jax.ShapeDtypeStruct(kv.shape, BF),
        ),
        in_specs=specs(7),
        out_specs=(vmem, vmem),
        scratch_shapes=[pltpu.VMEM(kv.shape, F32)],
        cost_estimate=pl.CostEstimate(
            flops=own * 512 * wide * 12, bytes_accessed=20 << 20, transcendentals=own * 512 * 3
        ),
        compiler_params=pltpu.CompilerParams(vmem_limit_bytes=48 << 20),
    )(row, rand, q, q_segs, kv, k_segs, d_o, lse, o)


def project_kernel(
    rows, span, row_ref, x_ref, wq_ref, wkv_ref, q_ref, kv_ref, own_ref
):
    feat = x_ref.shape[2]
    start = pl.multiple_of(row_ref[0] * span, span)
    kv = q = None
    for part in range(rows):
        at = slice(part * feat, (part + 1) * feat)
        mine = x_ref[part, 0, :, pl.ds(start, span)]
        own_ref[at, :] = mine
        kv_part = mm_tn(x_ref[part, 0], wkv_ref[at, :])
        q_part = mm_tn(mine, wq_ref[at, :])
        kv = kv_part if kv is None else kv + kv_part
        q = q_part if q is None else q + q_part
    kv_ref[...] = kv.astype(BF)
    q_ref[...] = (q.astype(BF) * 0.125).astype(BF)


def project(row, x_parts, w_q, w_kv, span):
    rows, cols, feat, local = x_parts.shape
    model, wide = w_q.shape
    return pl.pallas_call(
        functools.partial(project_kernel, rows, span),
        name="project",
        grid=(cols,),
        out_shape=(
            jax.ShapeDtypeStruct((cols * span, wide), BF),
            jax.ShapeDtypeStruct((cols * local, wide), BF),
            jax.ShapeDtypeStruct((model, cols * span), BF),
        ),
        in_specs=[
            pl.BlockSpec(memory_space=pltpu.SMEM),
            pl.BlockSpec((rows, 1, feat, local), lambda c: (0, c, 0, 0)),
            pl.BlockSpec((model, wide), lambda c: (0, 0)),
            pl.BlockSpec((model, wide), lambda c: (0, 0)),
        ],
        out_specs=(
            pl.BlockSpec((span, wide), lambda c: (c, 0)),
            pl.BlockSpec((local, wide), lambda c: (c, 0)),
            pl.BlockSpec((model, span), lambda c: (0, c)),
        ),
        cost_estimate=pl.CostEstimate(
            flops=cols * local * model * wide * 3, bytes_accessed=16 << 20, transcendentals=0
        ),
        compiler_params=pltpu.CompilerParams(vmem_limit_bytes=48 << 20),
    )(row, x_parts, w_q, w_kv)


PIECES = 2


def col_places():
    me = lax.axis_index("col")
    partner = me + 1 - 2 * lax.rem(me, 2)
    cross = lax.rem(me + 2, 4)
    diag = lax.rem(partner + 2, 4)
    barrier = pltpu.get_barrier_semaphore()
    for peer in (partner, cross):
        pl.semaphore_signal(
            barrier, inc=1, device_id={"col": peer}, device_id_type=pl.DeviceIdType.MESH
        )
    pl.semaphore_wait(barrier, 2)
    return me, partner, cross, diag


def send_to(source, target, sems, kind, piece, peer):
    copy = pltpu.make_async_remote_copy(
        src_ref=source,
        dst_ref=target,
        send_sem=sems[0].at[kind, piece],
        recv_sem=sems[1].at[kind, piece],
        device_id={"col": peer},
        device_id_type=pl.DeviceIdType.MESH,
    )
    copy.start()
    return copy


def gather_kernel(x_ref, out_ref, send_sem, recv_sem):
    me, partner, cross, _ = col_places()
    sems = (send_sem, recv_sem)
    size = x_ref.shape[0] // PIECES
    cuts = [pl.ds(i * size, size) for i in range(PIECES)]
    over = [
        send_to(x_ref.at[cut], out_ref.at[me, cut], sems, 0, i, cross)
        for i, cut in enumerate(cuts)
    ]
    near = [
        send_to(x_ref.at[cut], out_ref.at[me, cut], sems, 1, i, partner)
        for i, cut in enumerate(cuts)
    ]
    out_ref[me] = x_ref[...]
    relay = []
    for i, cut in enumerate(cuts):
        over[i].wait_recv()
        relay.append(
            send_to(out_ref.at[cross, cut], out_ref.at[cross, cut], sems, 2, i, partner)
        )
    for i in range(PIECES):
        over[i].wait_send()
        near[i].wait()
        relay[i].wait()


def scatter_kernel(x_ref, out_ref, near_buf, sum_buf, over_buf, send_sem, recv_sem):
    me, partner, cross, diag = col_places()
    sems = (send_sem, recv_sem)
    size = x_ref.shape[1] // PIECES
    cuts = [pl.ds(i * size, size) for i in range(PIECES)]
    first = [
        send_to(x_ref.at[diag, cut], near_buf.at[1, cut], sems, 0, i, partner)
        for i, cut in enumerate(cuts)
    ]
    second = [
        send_to(x_ref.at[partner, cut], near_buf.at[0, cut], sems, 1, i, partner)
        for i, cut in enumerate(cuts)
    ]
    over = []
    for i, cut in enumerate(cuts):
        first[i].wait_recv()
        sum_buf[cut, :] = (
            x_ref[cross, cut, :].astype(F32) + near_buf[1, cut, :].astype(F32)
        ).astype(BF)
        over.append(send_to(sum_buf.at[cut], over_buf.at[cut], sems, 2, i, cross))
    for i, cut in enumerate(cuts):
        second[i].wait_recv()
        out_ref[cut, :] = x_ref[me, cut, :].astype(F32) + near_buf[0, cut, :].astype(F32)
    for i, cut in enumerate(cuts):
        over[i].wait_recv()
        out_ref[cut, :] += over_buf[cut, :].astype(F32)
    for i in range(PIECES):
        first[i].wait_send()
        second[i].wait_send()
        over[i].wait_send()


def scatter_both_kernel(
    rows, swap, x_ref, g_ref, out_ref, grad_ref, near_buf, sum_buf, over_buf,
    from_left, from_right, to_right, to_left, own_buf, peer_buf,
    col_send, col_recv, send_sem, recv_sem, swap_sem,
):
    me, col = lax.axis_index("row"), lax.axis_index("col")
    right, left = lax.rem(me + 1, rows), lax.rem(me + rows - 1, rows)
    has_left, has_right = me > 0, me < rows - 1
    partner = col + 1 - 2 * lax.rem(col, 2)
    cross = lax.rem(col + 2, 4)
    diag = lax.rem(partner + 2, 4)
    mesh_id = pl.DeviceIdType.MESH
    barrier = pltpu.get_barrier_semaphore()

    @pl.when(has_left)
    def _():
        pl.semaphore_signal(barrier, inc=1, device_id={"row": left}, device_id_type=mesh_id)

    @pl.when(has_right)
    def _():
        pl.semaphore_signal(barrier, inc=1, device_id={"row": right}, device_id_type=mesh_id)

    for peer in (partner, cross):
        pl.semaphore_signal(barrier, inc=1, device_id={"col": peer}, device_id_type=mesh_id)
    if swap:
        other = 1 - lax.axis_index("dp")
        pl.semaphore_signal(barrier, inc=1, device_id={"dp": other}, device_id_type=mesh_id)
    peers = jnp.where(has_left, 1, 0) + jnp.where(has_right, 1, 0) + (3 if swap else 2)
    pl.semaphore_wait(barrier, peers)

    size = g_ref.shape[1] // PIECES
    cuts = [pl.ds(i * size, size) for i in range(PIECES)]
    deep = x_ref.shape[1] // PIECES
    slabs = [pl.ds(i * deep, deep) for i in range(PIECES)]
    sems = (col_send, col_recv)

    def hop(way, dest, i):
        stage, target, to = ((to_right, from_left, right), (to_left, from_right, left))[way]
        return pltpu.make_async_remote_copy(
            src_ref=stage.at[dest, cuts[i]],
            dst_ref=target.at[dest, cuts[i]],
            send_sem=send_sem.at[way, dest, i],
            recv_sem=recv_sem.at[way, dest, i],
            device_id={"row": to},
            device_id_type=mesh_id,
        )

    flows = []
    for step in range(rows - 1):
        flows.append((0, rows - 1 - step, me < rows - 1 - step, has_left))
        flows.append((1, step, me > step, has_right))

    first = [
        send_to(x_ref.at[diag, cut], near_buf.at[1, cut], sems, 0, i, partner)
        for i, cut in enumerate(slabs)
    ]
    for way, dest, active, relays in flows:
        stage = (to_right, to_left)[way]

        @pl.when(active & jnp.logical_not(relays))
        def _():
            for i, cut in enumerate(cuts):
                stage[dest, cut, :] = g_ref[dest, cut, :]
                hop(way, dest, i).start()

    second = [
        send_to(x_ref.at[partner, cut], near_buf.at[0, cut], sems, 1, i, partner)
        for i, cut in enumerate(slabs)
    ]
    over = []
    for i, cut in enumerate(slabs):
        first[i].wait_recv()
        sum_buf[cut, :] = (
            x_ref[cross, cut, :].astype(F32) + near_buf[1, cut, :].astype(F32)
        ).astype(BF)
        over.append(send_to(sum_buf.at[cut], over_buf.at[cut], sems, 2, i, cross))
    for way, dest, active, relays in flows:
        stage, came = ((to_right, from_left), (to_left, from_right))[way]

        @pl.when(active & relays)
        def _():
            for i, cut in enumerate(cuts):
                hop(way, dest, i).wait_recv()
                stage[dest, cut, :] = (
                    g_ref[dest, cut, :].astype(F32) + came[dest, cut, :].astype(F32)
                ).astype(BF)
                hop(way, dest, i).start()

    for i, cut in enumerate(slabs):
        second[i].wait_recv()
        out_ref[cut, :] = x_ref[col, cut, :].astype(F32) + near_buf[0, cut, :].astype(F32)
    for i, cut in enumerate(slabs):
        over[i].wait_recv()
        out_ref[cut, :] += over_buf[cut, :].astype(F32)

    grad_ref[...] = g_ref[me].astype(F32)
    for way, came, has in ((0, from_left, has_left), (1, from_right, has_right)):

        @pl.when(has)
        def _():
            for i, cut in enumerate(cuts):
                hop(way, me, i).wait_recv()
                grad_ref[cut, :] += came[me, cut, :].astype(F32)

    if swap:
        own_buf[...] = grad_ref[...].astype(BF)
        copy = pltpu.make_async_remote_copy(
            src_ref=own_buf,
            dst_ref=peer_buf,
            send_sem=swap_sem.at[0],
            recv_sem=swap_sem.at[1],
            device_id={"dp": other},
            device_id_type=mesh_id,
        )
        copy.start()
        copy.wait()
        grad_ref[...] = own_buf[...].astype(F32) + peer_buf[...].astype(F32)

    for way, dest, active, _ in flows:

        @pl.when(active)
        def _():
            for i in range(PIECES):
                hop(way, dest, i).wait_send()

    for i in range(PIECES):
        first[i].wait_send()
        second[i].wait_send()
        over[i].wait_send()


def scatter_both(value, grad, rows, swap):
    count, wide = value.shape[0] // 4, value.shape[1]
    deep, span = grad.shape[0] // rows, grad.shape[1]
    vmem = pl.BlockSpec(memory_space=pltpu.VMEM)
    return pl.pallas_call(
        functools.partial(scatter_both_kernel, rows, swap),
        name="scatter_both",
        out_shape=(
            jax.ShapeDtypeStruct((count, wide), F32),
            jax.ShapeDtypeStruct((deep, span), F32),
        ),
        in_specs=[vmem, vmem],
        out_specs=(vmem, vmem),
        scratch_shapes=[
            pltpu.VMEM((2, count, wide), BF),
            pltpu.VMEM((count, wide), BF),
            pltpu.VMEM((count, wide), BF),
        ]
        + [pltpu.VMEM((rows, deep, span), BF)] * 4
        + [pltpu.VMEM((deep, span), BF)] * 2
        + comm_sems(3)
        + [
            pltpu.SemaphoreType.DMA((2, rows, PIECES)),
            pltpu.SemaphoreType.DMA((2, rows, PIECES)),
            pltpu.SemaphoreType.DMA((2,)),
        ],
        compiler_params=comm_params(4),
    )(value.reshape(4, count, wide), grad.reshape(rows, deep, span))


def gather_in_kernel(rows, swap, x_ref, w_ref, xs_ref, ws_ref, send_x, recv_x, send_w, recv_w):
    me, col = lax.axis_index("row"), lax.axis_index("col")
    right, left = lax.rem(me + 1, rows), lax.rem(me + rows - 1, rows)
    has_left, has_right = me > 0, me < rows - 1
    partner = col + 1 - 2 * lax.rem(col, 2)
    cross = lax.rem(col + 2, 4)
    diag = lax.rem(partner + 2, 4)
    mesh_id = pl.DeviceIdType.MESH
    barrier = pltpu.get_barrier_semaphore()

    @pl.when(has_left)
    def _():
        pl.semaphore_signal(barrier, inc=1, device_id={"row": left}, device_id_type=mesh_id)

    @pl.when(has_right)
    def _():
        pl.semaphore_signal(barrier, inc=1, device_id={"row": right}, device_id_type=mesh_id)

    for peer in (partner, cross):
        pl.semaphore_signal(barrier, inc=1, device_id={"col": peer}, device_id_type=mesh_id)
    half = w_ref.shape[0] // 2
    cut = far = pl.ds(0, w_ref.shape[0])
    if swap:
        dp = lax.axis_index("dp")
        pl.semaphore_signal(barrier, inc=1, device_id={"dp": 1 - dp}, device_id_type=mesh_id)
        cut = pl.ds(pl.multiple_of(dp * half, half), half)
        far = pl.ds(pl.multiple_of((1 - dp) * half, half), half)
    peers = jnp.where(has_left, 1, 0) + jnp.where(has_right, 1, 0) + (3 if swap else 2)
    pl.semaphore_wait(barrier, peers)

    def copy_x(source, kind, shard, slot, where):
        return pltpu.make_async_remote_copy(
            src_ref=source,
            dst_ref=xs_ref.at[shard, slot],
            send_sem=send_x.at[kind, shard],
            recv_sem=recv_x.at[kind, shard],
            device_id=where,
            device_id_type=mesh_id,
        )

    def copy_w(source, kind, shard, where, cut=cut):
        return pltpu.make_async_remote_copy(
            src_ref=source.at[cut],
            dst_ref=ws_ref.at[shard, cut],
            send_sem=send_w.at[kind, shard],
            recv_sem=recv_w.at[kind, shard],
            device_id=where,
            device_id_type=mesh_id,
        )

    to_right, to_left = {"row": right}, {"row": left}
    ways = ((0, has_right, to_right), (1, has_left, to_left))

    for kind, onward, where in ways:

        @pl.when(onward)
        def _():
            copy_x(x_ref, kind, me, col, where).start()

    copy_x(x_ref, 2, me, col, {"col": cross}).start()
    copy_x(x_ref, 3, me, col, {"col": partner}).start()
    for kind, onward, where in ways:

        @pl.when(onward)
        def _():
            copy_w(w_ref, kind, me, where).start()

    xs_ref[me, col] = x_ref[...]
    ws_ref[me] = w_ref[...]

    def relay(shard):
        copy_x(x_ref, 2, shard, cross, {"col": cross}).wait_recv()
        source = xs_ref.at[shard, cross]
        copy_x(source, 4, shard, cross, {"col": partner}).start()

    def shards_at(step):
        return (
            (0, me - step, me >= step, has_right, to_right),
            (1, me + step, me + step <= rows - 1, has_left, to_left),
        )

    for step in range(1, rows):
        for kind, shard, exists, onward, where in shards_at(step):

            @pl.when(exists)
            def _():
                copy_x(x_ref, kind, shard, col, where).wait_recv()

                @pl.when(onward)
                def _():
                    copy_x(xs_ref.at[shard, col], kind, shard, col, where).start()

                copy_x(xs_ref.at[shard, col], 2, shard, col, {"col": cross}).start()
                copy_x(xs_ref.at[shard, col], 3, shard, col, {"col": partner}).start()

        for kind, shard, exists, onward, where in shards_at(step):

            @pl.when(exists)
            def _():
                copy_w(w_ref, kind, shard, where).wait_recv()

                @pl.when(onward)
                def _():
                    copy_w(ws_ref.at[shard], kind, shard, where).start()

                if swap:
                    copy_w(ws_ref.at[shard], 2, shard, {"dp": 1 - dp}).start()

        if step == 1:
            relay(me)
        else:
            for _, shard, exists, _, _ in shards_at(step - 1):

                @pl.when(exists)
                def _():
                    relay(shard)

    for _, shard, exists, _, _ in shards_at(rows - 1):

        @pl.when(exists)
        def _():
            relay(shard)

    for shard in range(rows):
        copy_x(x_ref, 3, shard, partner, {"col": partner}).wait_recv()
        copy_x(x_ref, 4, shard, diag, {"col": partner}).wait_recv()
        for kind in (2, 3, 4):
            copy_x(x_ref, kind, shard, col, {"col": partner}).wait_send()
        for kind, sent, where in (
            (0, has_right & (me >= shard), to_right),
            (1, has_left & (me <= shard), to_left),
        ):

            @pl.when(sent)
            def _():
                copy_x(x_ref, kind, shard, col, where).wait_send()
                copy_w(w_ref, kind, shard, where).wait_send()

        if swap:

            @pl.when(me != shard)
            def _():
                copy_w(w_ref, 2, shard, {"dp": 1 - dp}).wait_send()
                copy_w(w_ref, 2, shard, {"dp": 1 - dp}, far).wait_recv()


def gather_in(x, w, rows, swap):
    vmem = pl.BlockSpec(memory_space=pltpu.VMEM)
    sems = pltpu.SemaphoreType.DMA
    return pl.pallas_call(
        functools.partial(gather_in_kernel, rows, swap),
        name="gather_in",
        out_shape=(
            jax.ShapeDtypeStruct((rows, 4) + x.shape, BF),
            jax.ShapeDtypeStruct((rows,) + w.shape, BF),
        ),
        in_specs=[vmem, vmem],
        out_specs=(vmem, vmem),
        scratch_shapes=[sems((5, rows)), sems((5, rows)), sems((3, rows)), sems((3, rows))],
        compiler_params=comm_params(5),
    )(x, w)


def comm_params(ident):
    return pltpu.CompilerParams(
        collective_id=ident, has_side_effects=True, vmem_limit_bytes=32 << 20
    )


def comm_sems(kinds):
    return [pltpu.SemaphoreType.DMA((kinds, PIECES)), pltpu.SemaphoreType.DMA((kinds, PIECES))]


def gather_col(value, ident):
    count, wide = value.shape
    vmem = pl.BlockSpec(memory_space=pltpu.VMEM)
    return pl.pallas_call(
        gather_kernel,
        name="gather_col",
        out_shape=jax.ShapeDtypeStruct((4, count, wide), BF),
        in_specs=[vmem],
        out_specs=vmem,
        scratch_shapes=comm_sems(3),
        compiler_params=comm_params(ident),
    )(value)


def scatter_col(value):
    count, wide = value.shape[0] // 4, value.shape[1]
    vmem = pl.BlockSpec(memory_space=pltpu.VMEM)
    return pl.pallas_call(
        scatter_kernel,
        name="scatter_col",
        out_shape=jax.ShapeDtypeStruct((count, wide), F32),
        in_specs=[vmem],
        out_specs=vmem,
        scratch_shapes=[
            pltpu.VMEM((2, count, wide), BF),
            pltpu.VMEM((count, wide), BF),
            pltpu.VMEM((count, wide), BF),
        ]
        + comm_sems(3),
        compiler_params=comm_params(2),
    )(value.reshape(4, count, wide))


def norm(resid, gain, bias):
    mean = jnp.mean(resid, axis=1, keepdims=True)
    var = jnp.mean(resid * resid, axis=1, keepdims=True) - mean * mean
    rstd = lax.rsqrt(var + EPS)
    normed = (resid - mean) * rstd
    return normed * gain + bias, normed, rstd


def norm_grad(grad, normed, rstd, gain):
    scaled = grad * gain
    first = jnp.mean(scaled, axis=1, keepdims=True)
    second = jnp.mean(scaled * normed, axis=1, keepdims=True)
    return rstd * (scaled - first - normed * second)


def gelu(value):
    return jax.nn.gelu(value, approximate=True)


def on_device(
    inputs, w_query, w_key, w_value, w_out, w_up, w_down,
    ln1_gain, ln1_bias, ln2_gain, ln2_bias, segment_ids, pad_mask, rand_blocks, grad_out,
):
    rows, cols = lax.axis_size("row"), lax.axis_size("col")
    row, col = lax.axis_index("row"), lax.axis_index("col")
    feat, local = inputs.shape
    model = feat * rows
    hid = model // cols
    heads = hid // HW
    length = local * cols
    nb = length // BLOCK
    span = local // rows
    per = span // BLOCK
    dims = (heads, nb, per, rows)
    own = cols * span

    blk_q = w_query.reshape(feat, hid)
    blk_k = w_key.reshape(feat, hid)
    blk_v = w_value.reshape(feat, hid)
    blk_o = w_out.reshape(hid, feat)
    params = jnp.stack([ln1_gain, ln1_bias, ln2_gain, ln2_bias])
    high = params.astype(BF)
    rest = params - high.astype(F32)
    middle = rest.astype(BF)
    low = (rest - middle.astype(F32)).astype(BF)
    params = jnp.concatenate([high, middle, low], axis=0)
    params = jnp.pad(params, ((0, 20), (0, 4 * hid - feat)))
    w_small = jnp.concatenate([blk_q, blk_k, blk_v, blk_o.T], axis=1)
    w_small = jnp.concatenate([w_small, params], axis=0)
    swap = lax.axis_size("dp") == 2
    x_parts, w_small = gather_in(inputs, w_small, rows, swap)
    w_rest = jnp.concatenate([w_up, w_down], axis=1)
    x_parts, w_rest, grad_out = lax.optimization_barrier((x_parts, w_rest, grad_out))
    w_rest = lax.all_gather(w_rest, "row", axis=0, tiled=True)
    ff = w_up.shape[1]
    up, down = w_rest[:, :ff], w_rest[:, ff:]
    gains = w_small[:, feat : feat + 12, :feat].astype(F32).reshape(rows, 3, 4, feat)
    gains = (gains[:, 0] + gains[:, 1]) + gains[:, 2]
    gains = gains.transpose(1, 0, 2).reshape(4, 1, model)
    w_small = w_small[:, :feat].reshape(model, 4 * hid)
    w_own, w_o = w_small[:, : 3 * hid], w_small[:, 3 * hid :]
    grad_rows = lax.all_to_all(grad_out, "row", 1, 0, tiled=True).T.astype(F32)

    w_heads = w_own.reshape(model, 3, heads, HW)
    w_kv = jnp.concatenate([w_heads[:, 1], w_heads[:, 2]], axis=2).reshape(model, heads * LANES)
    w_q = jnp.pad(w_heads[:, 0], ((0, 0), (0, 0), (0, HW))).reshape(model, heads * LANES)
    row_arr = jnp.reshape(row, (1,)).astype(jnp.int32)
    q, kv, x_own = project(row_arr, x_parts, w_q, w_kv, span)
    x_res = lax.dynamic_slice_in_dim(x_own, col * span, span, axis=1).T.astype(F32)

    rand = rand_blocks.reshape(-1)
    k_segs = jnp.where(pad_mask == 1, segment_ids, -1).reshape(nb, BLOCK)
    k_segs = jnp.concatenate([k_segs, k_segs], axis=1)
    q_segs = lax.dynamic_index_in_dim(
        segment_ids.reshape(cols, rows, span), row, axis=1, keepdims=False
    )
    q_segs = jnp.broadcast_to(q_segs.reshape(own, 1), (own, LANES))
    o_wide, lse = attention_forward(dims, row_arr, rand, q, q_segs, kv, k_segs)
    o = o_wide.reshape(own, heads, 2, HW)[:, :, 1].reshape(own, hid)
    attn = scatter_col(mm_nt(o, w_o).astype(BF))

    gain1, bias1, gain2, bias2 = gains[0], gains[1], gains[2], gains[3]
    hidden, normed1, rstd1 = norm(x_res + attn, gain1, bias1)
    hidden_all = gather_col(hidden.astype(BF), 1).reshape(own, model)
    up_val = mm(hidden_all, up)
    act, gelu_back = jax.vjp(gelu, up_val)
    act = act.astype(BF)
    ffn = scatter_col(mm_nt(act, down).astype(BF))
    result, normed2, rstd2 = norm(hidden + ffn, gain2, bias2)
    output = lax.all_to_all(result.T.astype(BF), "row", 0, 1, tiled=True)

    grad2 = norm_grad(grad_rows, normed2, rstd2, gain2)
    df = gather_col(grad2.astype(BF), 1).reshape(own, model)
    g_down = mm_tn(df, act).astype(BF)
    du = gelu_back(mm(df, down))[0].astype(BF)
    g_up = mm_tn(hidden_all, du).astype(BF)
    g_ffn = jnp.concatenate(
        [g_up.reshape(rows, feat, ff), g_down.reshape(rows, feat, ff)], axis=1
    ).reshape(2 * model, ff)
    du, g_ffn = lax.optimization_barrier((du, g_ffn))
    g_ffn = lax.psum_scatter(g_ffn, "row", scatter_dimension=0, tiled=True)
    dh = scatter_col(mm_nt(du, up).astype(BF))
    dh = dh + grad2
    grad1 = norm_grad(dh, normed1, rstd1, gain1)
    sums = jnp.stack(
        [
            jnp.sum(dh * normed1, axis=0),
            jnp.sum(dh, axis=0),
            jnp.sum(grad_rows * normed2, axis=0),
            jnp.sum(grad_rows, axis=0),
        ]
    )
    extra = jnp.pad(sums, ((0, 28), (0, 0))).astype(BF)
    dattn = gather_col(jnp.concatenate([grad1.astype(BF), extra], axis=0), 3)
    sums = jnp.sum(dattn[:, span : span + 4].astype(F32), axis=0)
    dattn = dattn[:, :span].reshape(own, model)
    g_out = mm_tn(dattn, o).astype(BF)
    d_o = mm(dattn, w_o).astype(BF)
    d_o = jnp.pad(d_o.reshape(own, heads, HW), ((0, 0), (0, 0), (HW, 0))).reshape(own, -1)

    sums = sums.reshape(4, rows, feat).transpose(1, 0, 2).astype(BF)
    sums = jnp.pad(sums, ((0, 0), (0, 12), (0, hid - feat)))
    g_rest = jnp.concatenate([g_out.reshape(rows, feat, hid), sums], axis=1).reshape(-1, hid)
    d_o, g_rest = lax.optimization_barrier((d_o, g_rest))
    g_rest = lax.psum_scatter(g_rest, "row", scatter_dimension=0, tiled=True)
    dq, dkv = attention_backward(dims, row_arr, rand, q, q_segs, kv, k_segs, d_o, lse, o_wide)
    dkv = lax.psum_scatter(dkv, "row", scatter_dimension=0, tiled=True)
    dkv, g_ffn, g_rest = lax.optimization_barrier((dkv, g_ffn, g_rest))
    g_ffn, g_rest = lax.psum((g_ffn, g_rest), "dp")
    g_ffn, g_rest = g_ffn.astype(F32), g_rest.astype(F32)
    g_sums = g_rest[feat : feat + 4, :feat]
    dq = dq.reshape(own, heads, 2, HW)[:, :, 0].reshape(own, hid)
    dkv = dkv.reshape(own, heads, 2, HW)
    dqkv = jnp.concatenate(
        [dq, dkv[:, :, 0].reshape(own, hid), dkv[:, :, 1].reshape(own, hid)], axis=1
    )
    g_qkv = mm(x_own, dqkv).astype(BF)
    grad_in, g_qkv = scatter_both(mm_nt(dqkv, w_own).astype(BF), g_qkv, rows, swap)
    if not swap:
        g_qkv = lax.psum(g_qkv.astype(BF), "dp").astype(F32)
    grad_in = grad_in + grad1
    grad_in = lax.all_to_all(grad_in.T.astype(BF), "row", 0, 1, tiled=True).astype(F32)

    return (
        output,
        grad_in,
        g_qkv[:, :hid].reshape(1, 1, -1),
        g_qkv[:, hid : 2 * hid].reshape(1, 1, -1),
        g_qkv[:, 2 * hid :].reshape(1, 1, -1),
        g_rest[:feat].T.reshape(1, 1, -1),
        g_ffn[:feat],
        g_ffn[feat:],
        g_sums[0],
        g_sums[1],
        g_sums[2],
        g_sums[3],
    )


def solution(mesh):
    tokens = P("row", ("dp", "col"))
    grid = P("row", "col", None)
    return jax.shard_map(
        on_device,
        mesh=mesh,
        in_specs=(
            tokens,
            grid,
            grid,
            grid,
            P("col", "row", None),
            P("row", "col"),
            P("row", "col"),
            P("row"),
            P("row"),
            P("row"),
            P("row"),
            P("dp"),
            P("dp"),
            P("dp", "col", None, None),
            tokens,
        ),
        out_specs=(
            tokens,
            tokens,
            grid,
            grid,
            grid,
            P("col", "row", None),
            P("row", "col"),
            P("row", "col"),
            P("row"),
            P("row"),
            P("row"),
            P("row"),
        ),
        check_vma=False,
    )
```
